32 devices in a mesh: shard: 2 (over core), ctx: 8 (over z, x), tp: 2 (over y).
Axes of the slice: x: 2, y: 2, z: 4, core: 2. Of those that a mesh axis runs over, the one named last changes fastest.
Arguments:
- tokens: bfloat16 [2, 4096, 1024], P('shard', ('ctx', 'tp')), may hold values from -6 to 6
- value_first: bfloat16 [2, 4096, 1024], P('shard', ('ctx', 'tp')), may hold values from -6 to 6
- teacher: bfloat16 [2, 4096, 1024], P('shard', ('ctx', 'tp')), may hold values from -13 to 13
- valid: int32 [2, 4096], P('shard', ('ctx', 'tp')), may hold values from 0 to 1, as said below
- blocks: int32 [2, 4096], P('shard'), may hold values from 0 to 31, never falling along the last dimension, each value on 1 to 256 neighbouring positions
- gain_attn: float32 [1024], replicated, may hold values from 0.1 to 1.9
- gain_ffn: float32 [1024], replicated, may hold values from 0.1 to 1.9
- w_query: bfloat16 [1024, 1024], P('shard', 'tp'), may hold values from -0.375 to 0.375
- w_key: bfloat16 [1024, 1024], P('shard', 'tp'), may hold values from -0.1875 to 0.1875
- w_value: bfloat16 [1024, 1024], P('shard', 'tp'), may hold values from -0.1875 to 0.1875
- w_out: bfloat16 [1024, 1024], P('tp', 'shard'), may hold values from -0.75 to 0.75
- w_gate: bfloat16 [1024, 2816], P('shard', 'tp'), may hold values from -0.1875 to 0.1875
- w_up: bfloat16 [1024, 2816], P('shard', 'tp'), may hold values from -0.1875 to 0.1875
- w_down: bfloat16 [2816, 1024], P('tp', 'shard'), may hold values from -0.109375 to 0.109375
Outputs:
- output: bfloat16 [2, 4096, 1024], P('shard', ('ctx', 'tp'))
- loss: float32 [], replicated
- tokens_grad: float32 [2, 4096, 1024], P('shard', ('ctx', 'tp'))
- value_first_grad: float32 [2, 4096, 1024], P('shard', ('ctx', 'tp'))
- gain_attn_grad: float32 [1024], replicated
- gain_ffn_grad: float32 [1024], replicated
- w_query_grad: float32 [1024, 1024], P('shard', 'tp')
- w_key_grad: float32 [1024, 1024], P('shard', 'tp')
- w_value_grad: float32 [1024, 1024], P('shard', 'tp')
- w_out_grad: float32 [1024, 1024], P('tp', 'shard')
- w_gate_grad: float32 [1024, 2816], P('shard', 'tp')
- w_up_grad: float32 [1024, 2816], P('shard', 'tp')
- w_down_grad: float32 [2816, 1024], P('tp', 'shard')
The draws below stay inside these ranges and needn't reach their ends.
Inputs may be any that keep to these rules, and one draw needn't show every extreme that they name: `blocks`: block numbers count from 0 and never fall along a sequence; each block holds 1 to 256 tokens, one exactly 256. The first token of every sequence is valid.
All inputs are finite; a program needn't handle non-finite values.
Results may differ from the reference program's by a relative error of at most 0.019.
Values may be sent and summed in bfloat16 or wider, within the bound.
No kernel may reach another device: no remote copies, remote signals or barrier semaphores. Data moves between devices by JAX's collectives and lax.ppermute only.
A program may use at most 256 MiB of HBM per device.

```python
import math
import jax
import jax.numpy as jnp
import numpy as np
from jax import lax

D = 1024
HEADS = 16
HEAD_DIM = 64
FF = 2816
BLOCK = 256
SEQS = 2
LEN = 4096
TOKENS = 8192


def draw_teacher(key, part):
    position = jnp.arange(LEN, dtype=jnp.float32)[None, :, None] / LEN
    sequence = jnp.arange(SEQS, dtype=jnp.float32)[:, None, None] / SEQS
    rising = (0.4 + 0.9 * position) * (0.7 + 0.6 * sequence)
    base = jax.random.truncated_normal(key, -4.0, 4.0, (SEQS, LEN, D), jnp.float32)
    return (base * rising).astype(jnp.bfloat16)


def draw_valid(key, part):
    position = jnp.arange(LEN, dtype=jnp.int32)[None, :]
    ticket = jax.random.randint(key, (SEQS, LEN), 0, 4 * LEN)
    chosen = (ticket < LEN + 2 * position) | (position == 0)
    return jnp.where(chosen, 1, 0).astype(jnp.int32)


def shard_levels(rng, shape, cuts, low, top_value):
    def one(axis_at, parts):
        steps = jax.random.uniform(jax.random.fold_in(jax.random.fold_in(rng, 6), axis_at), (parts,), jnp.float32, low / len(cuts), top_value / len(cuts))
        return jnp.repeat(jnp.exp(steps), shape[axis_at] // parts).reshape((-1,) + (1,) * (len(shape) - axis_at - 1))

    factor_of = one(*cuts[0])
    for cut in cuts[1:]:
        factor_of = factor_of * one(*cut)
    return factor_of


def split_up(amount, total, most, slope):
    loads = [(1 << 20) // math.isqrt(grade ** slope) + 1 for grade in range(2, amount + 1)]
    spare, holding = total - most - (amount - 1), [1] * (amount - 1)
    while spare > 0:
        free = [i for i in range(amount - 1) if holding[i] < most]
        pool, budget = sum([loads[i] for i in free]), spare
        for i in free:
            more = min(most - holding[i], max(1, budget * loads[i] // pool), spare)
            holding[i] = holding[i] + more
            spare = spare - more
    return np.array([most] + holding)


def ragged(key, count, total, limit, skew):
    if count == 2:
        one = jax.random.randint(key, (), max(1, total - limit), min(limit, total - 1) + 1)
        return jnp.stack([one, total - one])
    sizes = jnp.asarray(split_up(count, total, limit, skew), jnp.int32)
    twos = (count - 1) // 2
    giver, sink = sizes[1:1 + 2 * twos:2], sizes[2:2 + 2 * twos:2]
    slack = jnp.minimum(giver - 1, limit - sink)
    passed = jax.random.randint(jax.random.fold_in(key, 1), (twos,), 0, 1 << 20) % (slack + 1)
    sizes = sizes.at[1:1 + 2 * twos:2].set(giver - passed).at[2:2 + 2 * twos:2].set(sink + passed)
    return sizes[jax.random.permutation(jax.random.fold_in(key, 2), count)]


def noise(stream_key, extent, scale, bound, pieces=(), held_as=jnp.bfloat16):
    level = shard_levels(stream_key, extent, pieces, -0.22, 0.18) if pieces else 1.0
    result = jax.random.normal(stream_key, extent, jnp.float32) * scale * level
    return jnp.minimum(jnp.maximum(result, -bound), bound).astype(held_as)


def setup_inputs(seed: int = 0) -> dict:
    seeds = jax.random.split(jax.random.key(seed), 15)
    tokens = noise(seeds[0], (SEQS, LEN, D), 1.0, 6.0, ((0, 2), (1, 16)))
    value_first = noise(seeds[1], (SEQS, LEN, D), 1.0, 6.0, ((0, 2), (1, 16)))
    teacher = draw_teacher(jax.random.fold_in(seeds[14], 71), 0)
    valid = draw_valid(jax.random.fold_in(seeds[14], 71), 0)
    blocks = jax.vmap(lambda own: jnp.searchsorted(jnp.cumsum(ragged(own, 2 * LEN // BLOCK, LEN, BLOCK, 1)), jnp.arange(LEN), side="right"))(jax.random.split(seeds[4], SEQS)).reshape((SEQS, LEN)).astype(jnp.int32)
    gain_attn = jnp.clip(1.0 + 0.18 * jax.random.normal(seeds[5], (D,), jnp.float32), 0.1, 1.9)
    gain_ffn = jnp.clip(1.0 + 0.18 * jax.random.normal(seeds[6], (D,), jnp.float32), 0.1, 1.9)
    w_query = noise(seeds[7], (D, D), (D // 4) ** -0.5, 0.375, ((0, 2), (1, 2)))
    w_key = noise(seeds[8], (D, D), D ** -0.5, 0.1875, ((0, 2), (1, 2)))
    w_value = noise(seeds[9], (D, D), D ** -0.5, 0.1875, ((0, 2), (1, 2)))
    w_out = noise(seeds[10], (D, D), (D // 16) ** -0.5, 0.75, ((0, 2), (1, 2)))
    w_gate = noise(seeds[11], (D, FF), D ** -0.5, 0.1875, ((0, 2), (1, 2)))
    w_up = noise(seeds[12], (D, FF), D ** -0.5, 0.1875, ((0, 2), (1, 2)))
    w_down = noise(seeds[13], (FF, D), FF ** -0.5, 0.109375, ((0, 2), (1, 2)))
    return {"tokens": tokens, "value_first": value_first, "teacher": teacher, "valid": valid, "blocks": blocks, "gain_attn": gain_attn, "gain_ffn": gain_ffn, "w_query": w_query, "w_key": w_key, "w_value": w_value, "w_out": w_out, "w_gate": w_gate, "w_up": w_up, "w_down": w_down}


precise = lax.Precision.HIGHEST
epsilon = 1e-06

@jax.custom_vjp
def low(v):
    return lax.optimization_barrier(v.astype(jnp.bfloat16)).astype(jnp.float32)

@jax.custom_vjp
def low_back(v):
    return v

def low_keep(v):
    return (low(v), None)

def low_pass(kept, grad):
    return (grad,)

def back_keep(v):
    return (v, None)

def back_low(kept, grad):
    return (low(grad),)
low.defvjp(low_keep, low_pass)
low_back.defvjp(back_keep, back_low)

def rms_norm(values, gain):
    return values * lax.rsqrt(lax.optimization_barrier(jnp.mean(values * values, axis=-1, keepdims=True)) + epsilon) * gain

def matmul(left, right):
    return jnp.dot(left, right, precision=precise, preferred_element_type=jnp.float32)

def attention(queries, keys, values, marks):
    length = queries.shape[0]
    block_size = min(512, length)
    block_count = length // block_size
    score_scale = HEAD_DIM ** (-0.5)
    query_blocks = queries.reshape(block_count, block_size, HEADS, HEAD_DIM)
    mark_blocks = marks.reshape(block_count, block_size)
    key_heads = keys.reshape(length, HEADS, HEAD_DIM)
    value_heads = values.reshape(length, HEADS, HEAD_DIM)

    def one_block(item):
        query_part, mark_part = item
        scores = jnp.einsum('qhd,khd->hqk', query_part, key_heads, precision=precise) * score_scale
        scores = low_back(scores)
        allowed = marks[None, None, :] <= mark_part[None, :, None]
        scores = jnp.where(allowed, scores, -1e+30)
        weights = low(jax.nn.softmax(scores, axis=-1))
        return jnp.einsum('hqk,khd->qhd', weights, value_heads, precision=precise)
    outcome = lax.map(jax.checkpoint(one_block), (query_blocks, mark_blocks))
    return outcome.reshape(length, HEADS * HEAD_DIM)

def layer(inputs, first_values, target, keep, marks, gain_attn, gain_ffn, w_query, w_key, w_value, w_out, w_gate, w_up, w_down):
    normed_one = low(rms_norm(inputs, gain_attn))
    queries = low_back(low(matmul(normed_one, w_query)))
    keys = low_back(low(matmul(normed_one, w_key)))
    mixed = low_back(low(0.5 * matmul(normed_one, w_value) + 0.5 * first_values))
    attended = low_back(low(attention(queries, keys, mixed, marks)))
    hidden = inputs + low_back(matmul(attended, w_out))
    normed_two = low(rms_norm(hidden, gain_ffn))
    gate_value = low_back(matmul(normed_two, w_gate))
    up_value = low_back(matmul(normed_two, w_up))
    activated = low(jax.nn.silu(gate_value) * up_value)
    final = hidden + low_back(matmul(activated, w_down))
    difference = final - target
    return (final, jnp.sum(lax.optimization_barrier(jnp.mean(difference * difference, axis=-1)) * keep))

def reference(tokens, value_first, teacher, valid, blocks, gain_attn, gain_ffn, w_query, w_key, w_value, w_out, w_gate, w_up, w_down):
    keep = valid.astype(jnp.float32)
    valid_count = jnp.sum(keep)
    target = teacher.astype(jnp.float32)
    params = tuple((item.astype(jnp.float32) for item in (gain_attn, gain_ffn, w_query, w_key, w_value, w_out, w_gate, w_up, w_down)))

    def forward(inputs_all, first_all, *weights):

        def one_sequence(item):
            inputs, first_values, target_seq, keep_seq, marks = item
            return layer(inputs, first_values, target_seq, keep_seq, marks, *weights)
        finals, errors = lax.map(one_sequence, (inputs_all, first_all, target, keep, blocks))
        return (jnp.sum(errors) / valid_count, finals)
    loss, pullback, finals = jax.vjp(forward, tokens.astype(jnp.float32), value_first.astype(jnp.float32), *params, has_aux=True)
    grads = pullback(jnp.asarray(TOKENS * D / 2, loss.dtype))
    return (finals.astype(jnp.bfloat16), loss, grads[0], grads[1], grads[2], grads[3], grads[4], grads[5], grads[6], grads[7], grads[8], grads[9], grads[10])
```

```python
import functools

import jax
import jax.numpy as jnp
from jax import lax
from jax.experimental import pallas as pl
from jax.experimental.pallas import tpu as pltpu
from jax.sharding import PartitionSpec as P

HEAD_DIM = 64
PAIR = 2 * HEAD_DIM
LN2 = 0.6931471805599453
QUERY_SCALE = HEAD_DIM ** (-0.5) / LN2
F32 = jnp.float32
BF16 = jnp.bfloat16
BOUNDARY = 256

epsilon = 1e-06


def rms_norm(values, gain):
    return values * lax.rsqrt(jnp.mean(values * values, axis=-1, keepdims=True) + epsilon) * gain


def dot(left, right, left_dim, right_dim):
    return lax.dot_general(
        left, right, (((left_dim,), (right_dim,)), ((), ())), preferred_element_type=F32
    )


def nn(left, right):
    return dot(left, right, 1, 0)


def nt(left, right):
    return dot(left, right, 1, 1)


def tn(left, right):
    return dot(left, right, 0, 0)


def split_heads(pair):
    lane = lax.broadcasted_iota(jnp.int32, (1, PAIR), 1)
    zero = jnp.zeros_like(pair)
    return [jnp.where(lane < HEAD_DIM, pair, zero), jnp.where(lane >= HEAD_DIM, pair, zero)]


def forward_kernel(
    step_keys, index_ref, q_ref, k_ref, v_ref, qmark_ref, kmark_ref, out_ref, lse_ref, vt_ref
):
    rows, length = q_ref.shape[0], k_ref.shape[0]
    index = index_ref[0]
    queries = split_heads(q_ref[...])
    vt_ref[...] = v_ref[...].T

    def step(masked):
        def body(at, state):
            start = pl.multiple_of(at * step_keys, step_keys)
            keys = k_ref[pl.ds(start, step_keys), :]
            if masked:
                allowed = kmark_ref[pl.ds(start, step_keys), :] <= qmark_ref[...]
            scores = [nt(keys, queries[h]) for h in range(2)]
            new = []
            for h in range(2):
                highest, total, out = state[3 * h : 3 * h + 3]
                score = scores[h]
                if masked:
                    score = jnp.where(allowed, score, -1e30)
                top = jnp.maximum(highest, jnp.max(score, axis=0, keepdims=True))
                power = jnp.exp2(score - top)
                shrink = jnp.exp2(highest - top)
                total = total * shrink + jnp.sum(power, axis=0, keepdims=True)
                values = vt_ref[pl.ds(HEAD_DIM * h, HEAD_DIM), pl.ds(start, step_keys)]
                new += [top, total, out * shrink + nn(values, power.astype(BF16))]
            return tuple(new)

        return body

    empty = (
        jnp.full((1, rows), -1e30, F32),
        jnp.zeros((1, rows), F32),
        jnp.zeros((HEAD_DIM, rows), F32),
    )
    full = (index * rows) // step_keys
    end = jnp.minimum(
        ((index + 1) * rows + BOUNDARY + step_keys - 1) // step_keys, length // step_keys
    )
    state = lax.fori_loop(full, end, step(True), empty + empty)
    state = lax.fori_loop(0, full, step(False), state)
    out = jnp.concatenate([state[2] / state[1], state[5] / state[4]], axis=0)
    out_ref[...] = out.T.astype(out_ref.dtype)
    lse_ref[0] = jnp.concatenate(
        [state[0] + jnp.log2(state[1]), state[3] + jnp.log2(state[4])], axis=0
    )


def attend_forward(index, queries, kv_all, qmark, kmark, step_keys=1024):
    rows, width = queries.shape
    length = kv_all.shape[0]
    pairs = width // PAIR
    return pl.pallas_call(
        functools.partial(forward_kernel, step_keys),
        grid_spec=pltpu.PrefetchScalarGridSpec(
            num_scalar_prefetch=1,
            grid=(pairs,),
            in_specs=[
                pl.BlockSpec((rows, PAIR), lambda h, s: (0, h)),
                pl.BlockSpec((length, PAIR), lambda h, s: (0, h)),
                pl.BlockSpec((length, PAIR), lambda h, s: (0, pairs + h)),
                pl.BlockSpec((1, rows), lambda h, s: (0, 0)),
                pl.BlockSpec((length, 1), lambda h, s: (0, 0)),
            ],
            out_specs=[
                pl.BlockSpec((rows, PAIR), lambda h, s: (0, h)),
                pl.BlockSpec((1, 2, rows), lambda h, s: (h, 0, 0)),
            ],
            scratch_shapes=[pltpu.VMEM((PAIR, length), BF16)],
        ),
        out_shape=[
            jax.ShapeDtypeStruct((rows, width), BF16),
            jax.ShapeDtypeStruct((pairs, 2, rows), F32),
        ],
        compiler_params=pltpu.CompilerParams(vmem_limit_bytes=56 << 20),
        cost_estimate=pl.CostEstimate(
            flops=4 * rows * length * width,
            bytes_accessed=4 * length * width,
            transcendentals=rows * length * width // HEAD_DIM,
        ),
    )(index, queries, kv_all, kv_all, qmark, kmark)


def delta_kernel(grad_ref, out_ref, delta_ref):
    terms = (grad_ref[...].astype(F32) * out_ref[...].astype(F32)).T
    delta_ref[0] = jnp.concatenate(
        [
            jnp.sum(terms[:HEAD_DIM], axis=0, keepdims=True),
            jnp.sum(terms[HEAD_DIM:], axis=0, keepdims=True),
        ],
        axis=0,
    )


def attend_delta(grad, out):
    rows, width = grad.shape
    pairs = width // PAIR
    return pl.pallas_call(
        delta_kernel,
        grid=(pairs,),
        in_specs=[pl.BlockSpec((rows, PAIR), lambda h: (0, h))] * 2,
        out_specs=pl.BlockSpec((1, 2, rows), lambda h: (h, 0, 0)),
        out_shape=jax.ShapeDtypeStruct((pairs, 2, rows), F32),
    )(grad, out)


def query_kernel(
    step_keys,
    index_ref,
    q_ref,
    grad_ref,
    k_ref,
    v_ref,
    lse_ref,
    delta_ref,
    qmark_ref,
    kmark_ref,
    out_ref,
    kt_ref,
):
    rows, length = q_ref.shape[0], k_ref.shape[0]
    index = index_ref[0]
    queries, grads = split_heads(q_ref[...]), split_heads(grad_ref[...])
    kt_ref[...] = k_ref[...].T

    def step(masked):
        def body(at, state):
            start = pl.multiple_of(at * step_keys, step_keys)
            keys = k_ref[pl.ds(start, step_keys), :]
            values = v_ref[pl.ds(start, step_keys), :]
            if masked:
                allowed = kmark_ref[pl.ds(start, step_keys), :] <= qmark_ref[...]
            new = []
            for h in range(2):
                score = nt(keys, queries[h])
                slope = nt(values, grads[h])
                prob = jnp.exp2(score - lse_ref[0, h : h + 1, :])
                if masked:
                    prob = jnp.where(allowed, prob, 0.0)
                grad = (prob * (slope - delta_ref[0, h : h + 1, :])).astype(BF16)
                turned = kt_ref[pl.ds(HEAD_DIM * h, HEAD_DIM), pl.ds(start, step_keys)]
                new.append(state[h] + nn(turned, grad))
            return tuple(new)

        return body

    empty = jnp.zeros((HEAD_DIM, rows), F32)
    full = (index * rows) // step_keys
    end = jnp.minimum(
        ((index + 1) * rows + BOUNDARY + step_keys - 1) // step_keys, length // step_keys
    )
    state = lax.fori_loop(full, end, step(True), (empty, empty))
    state = lax.fori_loop(0, full, step(False), state)
    out_ref[...] = (jnp.concatenate(state, axis=0).T * HEAD_DIM ** (-0.5)).astype(out_ref.dtype)


def query_gradient(index, queries, grad, kv_all, lse, delta, qmark, kmark, step_keys=1024):
    rows, width = queries.shape
    length = kv_all.shape[0]
    pairs = width // PAIR
    return pl.pallas_call(
        functools.partial(query_kernel, step_keys),
        grid_spec=pltpu.PrefetchScalarGridSpec(
            num_scalar_prefetch=1,
            grid=(pairs,),
            in_specs=[
                pl.BlockSpec((rows, PAIR), lambda h, s: (0, h)),
                pl.BlockSpec((rows, PAIR), lambda h, s: (0, h)),
                pl.BlockSpec((length, PAIR), lambda h, s: (0, h)),
                pl.BlockSpec((length, PAIR), lambda h, s: (0, pairs + h)),
                pl.BlockSpec((1, 2, rows), lambda h, s: (h, 0, 0)),
                pl.BlockSpec((1, 2, rows), lambda h, s: (h, 0, 0)),
                pl.BlockSpec((1, rows), lambda h, s: (0, 0)),
                pl.BlockSpec((length, 1), lambda h, s: (0, 0)),
            ],
            out_specs=pl.BlockSpec((rows, PAIR), lambda h, s: (0, h)),
            scratch_shapes=[pltpu.VMEM((PAIR, length), BF16)],
        ),
        out_shape=jax.ShapeDtypeStruct((rows, width), BF16),
        compiler_params=pltpu.CompilerParams(vmem_limit_bytes=56 << 20),
        cost_estimate=pl.CostEstimate(
            flops=6 * rows * length * width,
            bytes_accessed=4 * length * width,
            transcendentals=rows * length * width // HEAD_DIM,
        ),
    )(index, queries, grad, kv_all, kv_all, lse, delta, qmark, kmark)


def key_kernel(
    step_queries,
    index_ref,
    k_ref,
    v_ref,
    q_ref,
    grad_ref,
    lse_ref,
    delta_ref,
    qmark_ref,
    kmark_ref,
    dk_ref,
    dv_ref,
):
    rows, length = k_ref.shape[0], q_ref.shape[0]
    index = index_ref[0]
    keys, values = split_heads(k_ref[...]), split_heads(v_ref[...])

    def step(masked):
        def body(at, state):
            start = pl.multiple_of(at * step_queries, step_queries)
            queries = q_ref[pl.ds(start, step_queries), :]
            grads = grad_ref[pl.ds(start, step_queries), :]
            if masked:
                allowed = kmark_ref[...] <= qmark_ref[:, pl.ds(start, step_queries)]
            new = []
            for h in range(2):
                score = nt(keys[h], queries)
                slope = nt(values[h], grads)
                prob = jnp.exp2(score - lse_ref[0, h : h + 1, pl.ds(start, step_queries)])
                if masked:
                    prob = jnp.where(allowed, prob, 0.0)
                grad = prob * (slope - delta_ref[0, h : h + 1, pl.ds(start, step_queries)])
                new += [
                    state[2 * h] + nn(grad.astype(BF16), queries),
                    state[2 * h + 1] + nn(prob.astype(BF16), grads),
                ]
            return tuple(new)

        return body

    empty = jnp.zeros((rows, PAIR), F32)
    first = jnp.maximum((index * rows - BOUNDARY) // step_queries, 0)
    own = ((index + 1) * rows + step_queries - 1) // step_queries
    state = lax.fori_loop(first, own, step(True), (empty,) * 4)
    state = lax.fori_loop(own, length // step_queries, step(False), state)
    lane = lax.broadcasted_iota(jnp.int32, (1, PAIR), 1)
    dk_ref[...] = (jnp.where(lane < HEAD_DIM, state[0], state[2]) * LN2).astype(dk_ref.dtype)
    dv_ref[...] = jnp.where(lane < HEAD_DIM, state[1], state[3]).astype(dv_ref.dtype)


def key_gradient(index, kv, q_all, grad_all, lse, delta, qmark, kmark, step_queries=512):
    rows = kv.shape[0]
    length, width = q_all.shape
    pairs = width // PAIR
    return pl.pallas_call(
        functools.partial(key_kernel, step_queries),
        grid_spec=pltpu.PrefetchScalarGridSpec(
            num_scalar_prefetch=1,
            grid=(pairs,),
            in_specs=[
                pl.BlockSpec((rows, PAIR), lambda h, s: (0, h)),
                pl.BlockSpec((rows, PAIR), lambda h, s: (0, pairs + h)),
                pl.BlockSpec((length, PAIR), lambda h, s: (0, h)),
                pl.BlockSpec((length, PAIR), lambda h, s: (0, h)),
                pl.BlockSpec((1, 2, length), lambda h, s: (h, 0, 0)),
                pl.BlockSpec((1, 2, length), lambda h, s: (h, 0, 0)),
                pl.BlockSpec((1, length), lambda h, s: (0, 0)),
                pl.BlockSpec((rows, 1), lambda h, s: (0, 0)),
            ],
            out_specs=[pl.BlockSpec((rows, PAIR), lambda h, s: (0, h))] * 2,
        ),
        out_shape=[jax.ShapeDtypeStruct((rows, width), BF16)] * 2,
        compiler_params=pltpu.CompilerParams(vmem_limit_bytes=56 << 20),
        cost_estimate=pl.CostEstimate(
            flops=8 * rows * length * width,
            bytes_accessed=4 * length * width,
            transcendentals=rows * length * width // HEAD_DIM,
        ),
    )(index, kv, kv, q_all, grad_all, lse, delta, qmark, kmark)


def on_device(
    tokens,
    value_first,
    teacher,
    valid,
    blocks,
    gain_attn,
    gain_ffn,
    w_query,
    w_key,
    w_value,
    w_out,
    w_gate,
    w_up,
    w_down,
):
    width = tokens.shape[2]
    own_rows = tokens.shape[1]
    sizes = {axis: lax.axis_size(axis) for axis in ("shard", "ctx", "tp")}
    shard, ctx, tp = (lax.axis_index(axis) for axis in ("shard", "ctx", "tp"))
    group_rows = own_rows * sizes["tp"]
    half = w_query.shape[1]
    part = w_query.shape[0]

    def flip(values, axis, bit=1):
        return lax.ppermute(values, axis, [(i, i ^ bit) for i in range(sizes[axis])])

    def tree_sum(values):
        for axis, size in sizes.items():
            bit = 1
            while bit < size:
                values = values + flip(values, axis, bit)
                bit *= 2
        return values

    def in_order(position, mine, other, axis):
        first = position == 0
        return jnp.concatenate(
            [jnp.where(first, mine, other), jnp.where(first, other, mine)], axis=axis
        )

    def shard_gather(values, axis):
        if sizes["shard"] == 2:
            return in_order(shard, values, flip(values, "shard"), axis)
        return lax.all_gather(values, "shard", axis=axis, tiled=True)

    def rows_of(values, position):
        return lax.dynamic_slice_in_dim(values, position * own_rows, own_rows, 0)

    def cols_of(values, position, size):
        return lax.dynamic_slice_in_dim(values, position * size, size, 1)

    mine = tokens.reshape(own_rows, width)
    first_own = value_first.reshape(own_rows, width)
    key_marks = blocks.reshape(-1)
    query_marks = lax.dynamic_slice_in_dim(key_marks, ctx * group_rows, group_rows, 0)
    keep = valid.reshape(own_rows).astype(F32)
    index = ctx.reshape(1).astype(jnp.int32)

    theirs = flip(mine, "tp")
    first_theirs = flip(cols_of(first_own, 1 - tp, half), "tp")
    weight_qkv = shard_gather(jnp.concatenate([w_query, w_key, w_value], axis=1), 0)
    count = tree_sum(jnp.broadcast_to(jnp.sum(keep), (1, 128)))[0, 0]

    theirs, w_gate, w_up, w_down, w_out = lax.optimization_barrier(
        (theirs, w_gate, w_up, w_down, w_out)
    )
    gates = [shard_gather(w_gate, 0), shard_gather(flip(w_gate, "tp"), 0)]
    ups = [shard_gather(w_up, 0), shard_gather(flip(w_up, "tp"), 0)]
    downs = [shard_gather(w_down, 1), shard_gather(flip(w_down, "tp"), 1)]
    outs = [shard_gather(w_out, 1), shard_gather(flip(w_out, "tp"), 1)]

    group = in_order(tp, mine, theirs, 0).astype(F32)
    normed_one = rms_norm(group, gain_attn).astype(BF16)
    first_group = in_order(tp, cols_of(first_own, tp, half), first_theirs, 0).astype(F32)
    qkv = nn(normed_one, weight_qkv)
    queries = (qkv[:, :half] * QUERY_SCALE).astype(BF16)
    kv = jnp.concatenate(
        [qkv[:, half : 2 * half], 0.5 * qkv[:, 2 * half :] + 0.5 * first_group], axis=1
    ).astype(BF16)
    kv_all = lax.all_gather(kv, "ctx", axis=0, tiled=True)
    qmark, kmark = query_marks.reshape(1, -1), key_marks.reshape(-1, 1)
    attended, lse = attend_forward(index, queries, kv_all, qmark, kmark)

    q_all = lax.all_gather(queries, "ctx", axis=0, tiled=True)
    att = [rows_of(attended, tp), flip(rows_of(attended, 1 - tp), "tp")]
    inputs = mine.astype(F32)
    hidden = inputs + (nn(att[0], outs[0]) + nn(att[1], outs[1]))
    normed_two = rms_norm(hidden, gain_ffn).astype(BF16)
    gate = [nn(normed_two, w) for w in gates]
    up = [nn(normed_two, w) for w in ups]
    logistic = [jax.nn.sigmoid(g) for g in gate]
    act = [(g * s * u).astype(BF16) for g, s, u in zip(gate, logistic, up)]
    final = hidden + (nn(act[0], downs[0]) + nn(act[1], downs[1]))
    difference = final - teacher.reshape(own_rows, width).astype(F32)
    local_error = jnp.sum(jnp.mean(difference * difference, axis=1) * keep)
    token_total = group_rows * sizes["ctx"] * sizes["shard"]
    grad_final = token_total / count * keep[:, None] * difference
    grad_round = grad_final.astype(BF16)
    grad_act = [nt(grad_round, w) for w in downs]
    grad_gate = [
        (a * u * s * (1.0 + g * (1.0 - s))).astype(BF16)
        for a, u, s, g in zip(grad_act, up, logistic, gate)
    ]
    grad_up = [(a * g * s).astype(BF16) for a, g, s in zip(grad_act, gate, logistic)]
    grad_two = (
        nt(grad_gate[0], gates[0])
        + nt(grad_gate[1], gates[1])
        + nt(grad_up[0], ups[0])
        + nt(grad_up[1], ups[1])
    )
    hidden_part, gain_ffn_term = jax.vjp(rms_norm, hidden, gain_ffn)[1](grad_two)
    grad_hidden = grad_final + hidden_part
    hidden_round = grad_hidden.astype(BF16)
    grad_att = [nt(hidden_round, w).astype(BF16) for w in outs]
    grad_attended = in_order(tp, grad_att[0], flip(grad_att[1], "tp"), 0)
    delta = attend_delta(grad_attended, attended)
    grad_all = lax.all_gather(grad_attended, "ctx", axis=0, tiled=True)
    stats = lax.all_gather(jnp.stack([lse, delta]), "ctx", axis=3, tiled=True)

    def reduce_shard(left, right, slice_left):
        if sizes["shard"] != 2:
            return lax.psum_scatter(
                tn(left, right).astype(BF16),
                "shard",
                scatter_dimension=0 if slice_left else 1,
                tiled=True,
            ).astype(F32)
        if slice_left:
            kept, sent = (
                tn(cols_of(left, shard, part), right),
                tn(cols_of(left, 1 - shard, part), right),
            )
        else:
            kept, sent = (
                tn(left, cols_of(right, shard, part)),
                tn(left, cols_of(right, 1 - shard, part)),
            )
        return kept + flip(sent.astype(BF16), "shard").astype(F32)

    def reduce_pair(lefts, rights, slice_left):
        other = flip(reduce_shard(lefts[1], rights[1], slice_left).astype(BF16), "tp")
        own = reduce_shard(lefts[0], rights[0], slice_left)
        return (own + other.astype(F32)).astype(BF16)

    down_part = reduce_pair(act, [grad_round] * 2, False)
    gate_part = reduce_pair([normed_two] * 2, grad_gate, True)
    up_part = reduce_pair([normed_two] * 2, grad_up, True)
    out_part = reduce_pair(att, [hidden_round] * 2, False)
    w_down_grad, w_gate_grad, w_up_grad, w_out_grad = lax.psum(
        (down_part, gate_part, up_part, out_part), "ctx"
    )

    query_grad = query_gradient(
        index, queries, grad_attended, kv_all, lse, delta, qmark, kmark
    )
    key_grad, value_grad = key_gradient(
        index,
        kv,
        q_all,
        grad_all,
        stats[0],
        stats[1],
        key_marks.reshape(1, -1),
        query_marks.reshape(-1, 1),
    )
    value_half = (0.5 * value_grad.astype(F32)).astype(BF16)
    grads = jnp.concatenate([query_grad, key_grad, value_half], axis=1)
    grad_one_theirs = flip(nt(rows_of(grads, 1 - tp), weight_qkv).astype(BF16), "tp")
    grad_one = nt(rows_of(grads, tp), weight_qkv) + grad_one_theirs.astype(F32)
    input_part, gain_attn_term = jax.vjp(rms_norm, inputs, gain_attn)[1](grad_one)
    tokens_grad = grad_hidden + input_part
    first_grad = in_order(
        tp, rows_of(value_half, tp), flip(rows_of(value_half, 1 - tp), "tp"), 1
    ).astype(F32)
    qkv_part = reduce_shard(normed_one, grads, True).astype(BF16)
    qkv_grad = lax.psum(qkv_part, "ctx").astype(F32)

    small = jnp.concatenate(
        [gain_attn_term, gain_ffn_term, jnp.broadcast_to(local_error, (128,))]
    )
    small = tree_sum(small.reshape(1, -1)).reshape(-1)
    return (
        final.astype(BF16).reshape(1, own_rows, width),
        small[2 * width] / count,
        tokens_grad.reshape(1, own_rows, width),
        first_grad.reshape(1, own_rows, width),
        small[:width],
        small[width : 2 * width],
        qkv_grad[:, :half],
        qkv_grad[:, half : 2 * half],
        qkv_grad[:, 2 * half :],
        w_out_grad.astype(F32),
        w_gate_grad.astype(F32),
        w_up_grad.astype(F32),
        w_down_grad.astype(F32),
    )


def solution(mesh):
    rows = P("shard", ("ctx", "tp"), None)
    wide, tall = P("shard", "tp"), P("tp", "shard")
    return jax.shard_map(
        on_device,
        mesh=mesh,
        in_specs=(
            rows,
            rows,
            rows,
            P("shard", ("ctx", "tp")),
            P("shard", None),
            P(),
            P(),
            wide,
            wide,
            wide,
            tall,
            wide,
            wide,
            tall,
        ),
        out_specs=(rows, P(), rows, rows, P(), P(), wide, wide, wide, tall, wide, wide, tall),
        check_vma=False,
    )
```

```python
import functools

import jax
import jax.numpy as jnp
from jax import lax
from jax.experimental import pallas as pl
from jax.experimental.pallas import tpu as pltpu
from jax.sharding import PartitionSpec as P

HEAD_DIM = 64
PAIR = 2 * HEAD_DIM
LN2 = 0.6931471805599453
QUERY_SCALE = HEAD_DIM ** (-0.5) / LN2
F32 = jnp.float32
BF16 = jnp.bfloat16
BOUNDARY = 256
STAT_ROWS = 3

epsilon = 1e-06


def rms_norm(values, gain):
    return values * lax.rsqrt(jnp.mean(values * values, axis=-1, keepdims=True) + epsilon) * gain


def dot(left, right, left_dim, right_dim):
    return lax.dot_general(
        left, right, (((left_dim,), (right_dim,)), ((), ())), preferred_element_type=F32
    )


def nn(left, right):
    return dot(left, right, 1, 0)


def nt(left, right):
    return dot(left, right, 1, 1)


def tn(left, right):
    return dot(left, right, 0, 0)


def split_heads(pair):
    lane = lax.broadcasted_iota(jnp.int32, (1, PAIR), 1)
    zero = jnp.zeros_like(pair)
    return [jnp.where(lane < HEAD_DIM, pair, zero), jnp.where(lane >= HEAD_DIM, pair, zero)]


def forward_kernel(pieces, first, last, flag_ref, q_ref, *refs):
    refs = list(refs)
    qmark_ref = refs.pop(0)
    arrays = []
    for masked in pieces:
        count = 3 if masked else 2
        arrays.append(refs[:count])
        refs = refs[count:]
    if not first:
        old_high, old_total, old_out = refs[:3]
        refs = refs[3:]
    if last:
        result_ref, lse_ref = refs[:2]
        refs = refs[2:]
    high_ref, total_ref, out_ref = refs
    rows = q_ref.shape[0]
    if first:
        high_ref[0] = jnp.full((2, rows), -1e30, F32)
        total_ref[0] = jnp.zeros((2, rows), F32)
        out_ref[...] = jnp.zeros((PAIR, rows), F32)
    else:
        high_ref[0] = old_high[0]
        total_ref[0] = old_total[0]
        out_ref[...] = old_out[...]
    queries = split_heads(q_ref[...])

    def add_piece(piece, masked):
        keys = piece[0][...]
        turned = piece[1][...].T
        scores = [nt(keys, queries[h]) for h in range(2)]
        if masked:
            allowed = piece[2][...] <= qmark_ref[...]
        for h in range(2):
            score = scores[h]
            if masked:
                score = jnp.where(allowed, score, -1e30)
            highest = high_ref[0, h : h + 1, :]
            top = jnp.maximum(highest, jnp.max(score, axis=0, keepdims=True))
            power = jnp.exp2(score - top)
            shrink = jnp.exp2(highest - top)
            high_ref[0, h : h + 1, :] = top
            total_ref[0, h : h + 1, :] = total_ref[0, h : h + 1, :] * shrink + jnp.sum(
                power, axis=0, keepdims=True
            )
            columns = pl.ds(HEAD_DIM * h, HEAD_DIM)
            out_ref[columns, :] = out_ref[columns, :] * shrink + nn(
                turned[HEAD_DIM * h : HEAD_DIM * (h + 1)], power.astype(BF16)
            )

    for at, masked in enumerate(pieces):
        if masked:
            add_piece(arrays[at], True)
        else:
            pl.when(flag_ref[at] >= 0)(functools.partial(add_piece, arrays[at], False))
    if last:
        for h in range(2):
            columns = pl.ds(HEAD_DIM * h, HEAD_DIM)
            out_ref[columns, :] = out_ref[columns, :] / total_ref[0, h : h + 1, :]
        result_ref[...] = out_ref[...].T.astype(BF16)
        lse_ref[0] = high_ref[0] + jnp.log2(total_ref[0])


def forward_stage(queries, qmark, pieces, state, last):
    rows, width = queries.shape
    pairs = width // PAIR
    flags = jnp.stack([jnp.asarray(place, jnp.int32) for _, place, _ in pieces])
    args = [queries, qmark]
    in_specs = [
        pl.BlockSpec((rows, PAIR), lambda h, s: (0, h)),
        pl.BlockSpec((1, rows), lambda h, s: (0, 0)),
    ]
    keys = 0
    for kv, _, marks in pieces:
        count = kv.shape[0]
        keys += count
        args += [kv, kv]
        in_specs += [
            pl.BlockSpec((count, PAIR), lambda h, s: (0, h)),
            pl.BlockSpec((count, PAIR), lambda h, s: (0, pairs + h)),
        ]
        if marks is not None:
            args.append(marks)
            in_specs.append(pl.BlockSpec((count, 1), lambda h, s: (0, 0)))
    stat = jax.ShapeDtypeStruct((pairs, 2, rows), F32)
    stat_spec = pl.BlockSpec((1, 2, rows), lambda h, s: (h, 0, 0))
    state_specs = [stat_spec, stat_spec, pl.BlockSpec((PAIR, rows), lambda h, s: (h, 0))]
    state_shapes = [stat, stat, jax.ShapeDtypeStruct((width, rows), F32)]
    if state is not None:
        args += list(state)
        in_specs += state_specs
    if last:
        out_specs = [pl.BlockSpec((rows, PAIR), lambda h, s: (0, h)), stat_spec]
        out_shape = [jax.ShapeDtypeStruct((rows, width), BF16), stat]
        scratch = [
            pltpu.VMEM((1, 2, rows), F32),
            pltpu.VMEM((1, 2, rows), F32),
            pltpu.VMEM((PAIR, rows), F32),
        ]
    else:
        out_specs, out_shape, scratch = state_specs, state_shapes, []
    return pl.pallas_call(
        functools.partial(
            forward_kernel, [m is not None for _, _, m in pieces], state is None, last
        ),
        grid_spec=pltpu.PrefetchScalarGridSpec(
            num_scalar_prefetch=1,
            grid=(pairs,),
            in_specs=in_specs,
            out_specs=out_specs,
            scratch_shapes=scratch,
        ),
        out_shape=out_shape,
        compiler_params=pltpu.CompilerParams(vmem_limit_bytes=40 << 20),
        cost_estimate=pl.CostEstimate(
            flops=16 * rows * keys * width,
            bytes_accessed=8 * keys * width,
            transcendentals=rows * keys * width // HEAD_DIM,
        ),
    )(flags, *args)


def stats_kernel(rows, place_ref, mine_ref, other_ref, out_ref, lse_ref, sent_ref, stat_ref):
    half = mine_ref.shape[0]
    place = place_ref[0]
    sent_ref[pl.ds(pl.multiple_of(place * half, half), half), :] = mine_ref[...]
    sent_ref[pl.ds(pl.multiple_of((1 - place) * half, half), half), :] = other_ref[...]
    width = mine_ref.shape[1]
    heads = width // HEAD_DIM
    deltas = []
    for pair in range(width // PAIR):
        columns = pl.ds(pair * PAIR, PAIR)
        grad = sent_ref[pl.ds(0, rows), columns]
        terms = (grad.astype(F32) * out_ref[:, columns].astype(F32)).T
        deltas += [
            jnp.sum(terms[:HEAD_DIM], axis=0, keepdims=True),
            jnp.sum(terms[HEAD_DIM:], axis=0, keepdims=True),
        ]
    stat = jnp.concatenate(
        [lse_ref[pair] for pair in range(width // PAIR)] + deltas, axis=0
    )
    stat_ref[...] = stat
    for at in range(STAT_ROWS):
        piece = stat.astype(BF16)
        sent_ref[pl.ds(rows + at * 2 * heads, 2 * heads), :] = piece
        stat = stat - piece.astype(F32)


def pack_gradient(place, mine, other, attended, lse):
    rows, width = attended.shape
    stat_rows = 2 * width // HEAD_DIM
    return pl.pallas_call(
        functools.partial(stats_kernel, rows),
        in_specs=[pl.BlockSpec(memory_space=pltpu.SMEM)]
        + [pl.BlockSpec(memory_space=pltpu.VMEM)] * 4,
        out_specs=[pl.BlockSpec(memory_space=pltpu.VMEM)] * 2,
        out_shape=[
            jax.ShapeDtypeStruct((rows + STAT_ROWS * stat_rows, width), BF16),
            jax.ShapeDtypeStruct((stat_rows, rows), F32),
        ],
    )(place, mine, other, attended, lse)


def query_kernel(
    sizes, step_keys, place_ref, q_ref, grad_ref, stat_ref, qmark_ref, kmark_ref, *refs
):
    count = len(sizes)
    pieces, out_ref, kv_ref, kt_ref, sems = refs[:count], *refs[count:]
    rows, length = q_ref.shape[0], kv_ref.shape[0]
    width = kv_ref.shape[1] // 2
    pair = pl.program_id(0)
    index = place_ref[0]
    full = (index * rows) // step_keys
    end = jnp.minimum(
        ((index + 1) * rows + BOUNDARY + step_keys - 1) // step_keys, length // step_keys
    )

    def copy(at):
        start = pl.multiple_of(place_ref[at] * rows, rows)
        return pltpu.make_async_copy(
            pieces[at], kv_ref.at[pl.ds(start, sizes[at]), :], sems.at[at]
        )

    @pl.when(pair == 0)
    def _():
        for at in range(count):
            pl.when(place_ref[at] >= 0)(lambda at=at: copy(at).start())

        def clear(at, _):
            start = pl.multiple_of(at * BOUNDARY, BOUNDARY)
            kv_ref[pl.ds(start, BOUNDARY), :] = jnp.zeros((BOUNDARY, 2 * width), BF16)
            return 0

        ratio = rows // BOUNDARY
        lax.fori_loop((index + 1) * ratio + 1, end * (step_keys // BOUNDARY), clear, 0)
        for at in range(count):
            pl.when(place_ref[at] >= 0)(lambda at=at: copy(at).wait())

    queries, grads = split_heads(q_ref[...]), split_heads(grad_ref[...])
    k_columns = pl.ds(pl.multiple_of(pair * PAIR, PAIR), PAIR)
    v_columns = pl.ds(pl.multiple_of(width + pair * PAIR, PAIR), PAIR)
    lse = [stat_ref[pl.ds(2 * pair + h, 1), :] for h in range(2)]
    delta = [
        stat_ref[pl.ds(stat_ref.shape[0] // 2 + 2 * pair + h, 1), :] for h in range(2)
    ]

    def turn(at, _):
        start = pl.multiple_of(at * step_keys, step_keys)
        kt_ref[:, pl.ds(start, step_keys)] = kv_ref[pl.ds(start, step_keys), k_columns].T
        return 0

    lax.fori_loop(0, end, turn, 0)

    def step(masked):
        def body(at, state):
            start = pl.multiple_of(at * step_keys, step_keys)
            keys = kv_ref[pl.ds(start, step_keys), k_columns]
            values = kv_ref[pl.ds(start, step_keys), v_columns]
            if masked:
                allowed = kmark_ref[pl.ds(start, step_keys), :] <= qmark_ref[...]
            new = []
            for h in range(2):
                score = nt(keys, queries[h])
                slope = nt(values, grads[h])
                prob = jnp.exp2(score - lse[h])
                if masked:
                    prob = jnp.where(allowed, prob, 0.0)
                grad = (prob * (slope - delta[h])).astype(BF16)
                turned = kt_ref[pl.ds(HEAD_DIM * h, HEAD_DIM), pl.ds(start, step_keys)]
                new.append(state[h] + nn(turned, grad))
            return tuple(new)

        return body

    empty = jnp.zeros((HEAD_DIM, rows), F32)
    state = lax.fori_loop(full, end, step(True), (empty, empty))
    state = lax.fori_loop(0, full, step(False), state)
    out_ref[...] = (jnp.concatenate(state, axis=0).T * HEAD_DIM ** (-0.5)).astype(out_ref.dtype)


def query_gradient(queries, sent, stat, pieces, qmark, kmark, step_keys=1024):
    rows, width = queries.shape
    length = kmark.shape[0]
    pairs = width // PAIR
    places = jnp.stack([jnp.asarray(place, jnp.int32) for _, place in pieces])
    sizes = [kv.shape[0] for kv, _ in pieces]
    return pl.pallas_call(
        functools.partial(query_kernel, sizes, step_keys),
        grid_spec=pltpu.PrefetchScalarGridSpec(
            num_scalar_prefetch=1,
            grid=(pairs,),
            in_specs=[
                pl.BlockSpec((rows, PAIR), lambda h, s: (0, h)),
                pl.BlockSpec((rows, PAIR), lambda h, s: (0, h)),
                pl.BlockSpec(stat.shape, lambda h, s: (0, 0)),
                pl.BlockSpec((1, rows), lambda h, s: (0, 0)),
                pl.BlockSpec((length, 1), lambda h, s: (0, 0)),
            ]
            + [pl.BlockSpec(memory_space=pl.ANY)] * len(pieces),
            out_specs=pl.BlockSpec((rows, PAIR), lambda h, s: (0, h)),
            scratch_shapes=[
                pltpu.VMEM((length, 2 * width), BF16),
                pltpu.VMEM((PAIR, length), BF16),
                pltpu.SemaphoreType.DMA((len(pieces),)),
            ],
        ),
        out_shape=jax.ShapeDtypeStruct((rows, width), BF16),
        compiler_params=pltpu.CompilerParams(vmem_limit_bytes=56 << 20),
        cost_estimate=pl.CostEstimate(
            flops=16 * rows * length * width,
            bytes_accessed=4 * length * width,
            transcendentals=rows * length * width // HEAD_DIM,
        ),
    )(places, queries, sent, stat, qmark, kmark, *[kv for kv, _ in pieces])


def key_kernel(
    sizes, step_queries, place_ref, k_ref, v_ref, q_ref, qmark_ref, kmark_ref, *refs
):
    count = len(sizes)
    pieces = refs[:count]
    dk_ref, dv_ref, grad_ref, raw_ref, stat_ref, sems = refs[count:]
    rows, length = k_ref.shape[0], q_ref.shape[0]
    width = grad_ref.shape[1]
    stat_rows = stat_ref.shape[0]
    packed = STAT_ROWS * stat_rows
    pair = pl.program_id(0)
    index = place_ref[0]

    def copies(at):
        size = sizes[at]
        start = pl.multiple_of(place_ref[at] * rows + rows - size, BOUNDARY)
        return (
            pltpu.make_async_copy(
                pieces[at].at[pl.ds(0, size), :],
                grad_ref.at[pl.ds(start, size), :],
                sems.at[2 * at],
            ),
            pltpu.make_async_copy(
                pieces[at].at[pl.ds(size, packed), :],
                raw_ref.at[at],
                sems.at[2 * at + 1],
            ),
        )

    @pl.when(pair == 0)
    def _():
        for at in range(count):

            @pl.when(place_ref[at] >= 0)
            def _(at=at):
                for one in copies(at):
                    one.start()

        @pl.when(index > 0)
        def _():
            start = pl.multiple_of((index - 1) * rows, rows)
            grad_ref[pl.ds(start, rows - BOUNDARY), :] = jnp.zeros(
                (rows - BOUNDARY, width), BF16
            )

        for at in range(count):

            @pl.when(place_ref[at] >= 0)
            def _(at=at):
                for one in copies(at):
                    one.wait()
                stat = raw_ref[at, :stat_rows].astype(F32)
                for part in range(1, STAT_ROWS):
                    stat = stat + raw_ref[
                        at, part * stat_rows : (part + 1) * stat_rows
                    ].astype(F32)
                start = pl.multiple_of(place_ref[at] * rows, rows)
                stat_ref[:, pl.ds(start, rows)] = stat

    keys, values = split_heads(k_ref[...]), split_heads(v_ref[...])
    columns = pl.ds(pl.multiple_of(pair * PAIR, PAIR), PAIR)

    def step(masked):
        def body(at, state):
            start = pl.multiple_of(at * step_queries, step_queries)
            span = pl.ds(start, step_queries)
            queries = q_ref[span, :]
            grads = grad_ref[span, columns]
            if masked:
                allowed = kmark_ref[...] <= qmark_ref[:, span]
            new = []
            for h in range(2):
                lse = stat_ref[pl.ds(2 * pair + h, 1), span]
                delta = stat_ref[pl.ds(stat_rows // 2 + 2 * pair + h, 1), span]
                score = nt(keys[h], queries)
                slope = nt(values[h], grads)
                prob = jnp.exp2(score - lse)
                if masked:
                    prob = jnp.where(allowed, prob, 0.0)
                grad = prob * (slope - delta)
                new += [
                    state[2 * h] + nn(grad.astype(BF16), queries),
                    state[2 * h + 1] + nn(prob.astype(BF16), grads),
                ]
            return tuple(new)

        return body

    empty = jnp.zeros((rows, PAIR), F32)
    first = jnp.maximum((index * rows - BOUNDARY) // step_queries, 0)
    own = ((index + 1) * rows + step_queries - 1) // step_queries
    state = lax.fori_loop(first, own, step(True), (empty,) * 4)
    state = lax.fori_loop(own, length // step_queries, step(False), state)
    lane = lax.broadcasted_iota(jnp.int32, (1, PAIR), 1)
    dk_ref[...] = (jnp.where(lane < HEAD_DIM, state[0], state[2]) * LN2).astype(dk_ref.dtype)
    dv_ref[...] = (0.5 * jnp.where(lane < HEAD_DIM, state[1], state[3])).astype(dv_ref.dtype)


def key_gradient(kv, q_all, pieces, qmark, kmark, step_queries=512):
    rows = kv.shape[0]
    length, width = q_all.shape
    pairs = width // PAIR
    stat_rows = 2 * width // HEAD_DIM
    packed = STAT_ROWS * stat_rows
    places = jnp.stack([jnp.asarray(place, jnp.int32) for _, place in pieces])
    sizes = [sent.shape[0] - packed for sent, _ in pieces]
    return pl.pallas_call(
        functools.partial(key_kernel, sizes, step_queries),
        grid_spec=pltpu.PrefetchScalarGridSpec(
            num_scalar_prefetch=1,
            grid=(pairs,),
            in_specs=[
                pl.BlockSpec((rows, PAIR), lambda h, s: (0, h)),
                pl.BlockSpec((rows, PAIR), lambda h, s: (0, pairs + h)),
                pl.BlockSpec((length, PAIR), lambda h, s: (0, h)),
                pl.BlockSpec((1, length), lambda h, s: (0, 0)),
                pl.BlockSpec((rows, 1), lambda h, s: (0, 0)),
            ]
            + [pl.BlockSpec(memory_space=pl.ANY)] * len(pieces),
            out_specs=[pl.BlockSpec((rows, PAIR), lambda h, s: (0, h))] * 2,
            scratch_shapes=[
                pltpu.VMEM((length, width), BF16),
                pltpu.VMEM((len(pieces), packed, rows), BF16),
                pltpu.VMEM((stat_rows, length), F32),
                pltpu.SemaphoreType.DMA((2 * len(pieces),)),
            ],
        ),
        out_shape=[jax.ShapeDtypeStruct((rows, width), BF16)] * 2,
        compiler_params=pltpu.CompilerParams(vmem_limit_bytes=56 << 20),
        cost_estimate=pl.CostEstimate(
            flops=rows * length * width,
            bytes_accessed=4 * length * width,
            transcendentals=rows * length * width // HEAD_DIM,
        ),
    )(places, kv, kv, q_all, qmark, kmark, *[sent for sent, _ in pieces])


def on_device(
    tokens,
    value_first,
    teacher,
    valid,
    blocks,
    gain_attn,
    gain_ffn,
    w_query,
    w_key,
    w_value,
    w_out,
    w_gate,
    w_up,
    w_down,
):
    width = tokens.shape[2]
    own_rows = tokens.shape[1]
    sizes = {axis: lax.axis_size(axis) for axis in ("shard", "ctx", "tp")}
    shard, ctx, tp = (lax.axis_index(axis) for axis in ("shard", "ctx", "tp"))
    group_rows = own_rows * sizes["tp"]
    half = w_query.shape[1]
    part = w_query.shape[0]
    line = sizes["ctx"] // 2

    def flip(values, axis, bit=1):
        return lax.ppermute(values, axis, [(i, i ^ bit) for i in range(sizes[axis])])

    def tree_sum(values):
        for axis, size in sizes.items():
            bit = 1
            while bit < size:
                values = values + flip(values, axis, bit)
                bit *= 2
        return values

    def in_order(position, mine, other, axis):
        first = position == 0
        return jnp.concatenate(
            [jnp.where(first, mine, other), jnp.where(first, other, mine)], axis=axis
        )

    def shard_gather(values, axis):
        if sizes["shard"] == 2:
            return in_order(shard, values, flip(values, "shard"), axis)
        return lax.all_gather(values, "shard", axis=axis, tiled=True)

    def rows_of(values, position):
        return lax.dynamic_slice_in_dim(values, position * own_rows, own_rows, 0)

    def cols_of(values, position, size):
        return lax.dynamic_slice_in_dim(values, position * size, size, 1)

    level, column = ctx // 2, ctx % 2

    def spread(own, step, edge, between):
        if line != 4:
            gathered = lax.all_gather(own, "ctx", axis=0, tiled=False)
            below = [(place < ctx) if step == 1 else (place > ctx) for place in range(2 * line)]
            pieces = [
                (gathered[place], jnp.where(below[place], place, -1)) for place in range(2 * line)
            ]
            beside = jnp.clip(ctx + step, 0, 2 * line - 1)
            rows = lax.dynamic_index_in_dim(gathered, beside, 0, keepdims=False)[edge]
            gathered, rows = between(0, [pieces[0][0], rows])
            pieces[0] = (gathered, pieces[0][1])
            stages = [pieces[:2]]
            for i in range(2, 2 * line, 2):
                (first,) = between(i // 2, [pieces[i][0]])
                stages.append([(first, pieces[i][1]), pieces[i + 1]])
            return stages, rows
        along = [(i, i + 2 * step) for i in range(2 * line) if 0 <= i + 2 * step < 2 * line]
        across = flip(own, "ctx")
        near = 1 if step == 1 else 0
        diagonal = [
            (i + step, i) for i in range(2 * line) if i % 2 == near and 0 <= i + step < 2 * line
        ]
        beside = lax.ppermute(own[edge], "ctx", diagonal)
        moving = lax.ppermute(own, "ctx", along)
        across, moving, beside = between(0, [across, moving, beside])
        rows = jnp.where(column == near, beside, across[edge])
        stages = [[(across, jnp.where(column == near, ctx - step, -1))]]
        for hop in range(1, line):
            there = level - step * hop
            exists = (there >= 0) & (there < line)
            stages[-1].append((moving, jnp.where(exists, 2 * there + column, -1)))
            across = flip(moving, "ctx")
            if hop + 1 < line:
                moving = lax.ppermute(moving, "ctx", along)
                across, moving = between(hop, [across, moving])
            else:
                (across,) = between(hop, [across])
            stages.append([(across, jnp.where(exists, 2 * there + 1 - column, -1))])
        return stages, rows

    mine = tokens.reshape(own_rows, width)
    first_own = value_first.reshape(own_rows, width)
    key_marks = blocks.reshape(-1)
    padded_marks = jnp.concatenate([key_marks, jnp.full((BOUNDARY,), 1 << 30, key_marks.dtype)])
    query_marks = lax.dynamic_slice_in_dim(key_marks, ctx * group_rows, group_rows, 0)
    next_marks = lax.dynamic_slice_in_dim(padded_marks, (ctx + 1) * group_rows, BOUNDARY, 0)
    keep = valid.reshape(own_rows).astype(F32)

    theirs = flip(mine, "tp")
    first_theirs = flip(cols_of(first_own, 1 - tp, half), "tp")
    weight_qkv = shard_gather(jnp.concatenate([w_query, w_key, w_value], axis=1), 0)
    count = tree_sum(jnp.broadcast_to(jnp.sum(keep), (1, 128)))[0, 0]

    group = in_order(tp, mine, theirs, 0).astype(F32)
    normed_one = rms_norm(group, gain_attn).astype(BF16)
    first_group = in_order(tp, cols_of(first_own, tp, half), first_theirs, 0).astype(F32)
    qkv = nn(normed_one, weight_qkv)
    queries = (qkv[:, :half] * QUERY_SCALE).astype(BF16)
    kv = jnp.concatenate(
        [qkv[:, half : 2 * half], 0.5 * qkv[:, 2 * half :] + 0.5 * first_group], axis=1
    ).astype(BF16)

    def pair_up(gathered):
        return [
            lax.dynamic_index_in_dim(gathered, at, 0, keepdims=False) for at in (tp, 1 - tp)
        ]

    def gather_rows(values):
        gathered = lax.all_gather(values, ("tp", "shard"), axis=0, tiled=True)
        return pair_up(gathered.reshape(sizes["tp"], width, values.shape[1]))

    def gather_blocks(values):
        if sizes["shard"] == 2:
            both = [values, flip(values, "tp")]
            return [[one, flip(one, "shard")] for one in both]
        gathered = lax.all_gather(values, ("tp", "shard"), axis=0, tiled=False)
        gathered = pair_up(gathered.reshape(sizes["tp"], sizes["shard"], *values.shape))
        return [[one[i] for i in range(sizes["shard"])] for one in gathered]

    def block_of(values, at):
        if sizes["shard"] == 2:
            return cols_of(values, shard if at == 0 else 1 - shard, part)
        return values[:, at * part : (at + 1) * part]

    def join_blocks(terms):
        if sizes["shard"] == 2:
            return in_order(shard, terms[0], terms[1], 1)
        return jnp.concatenate(terms, axis=1)

    def times_blocks(lefts, blocks_of):
        return join_blocks(
            [
                sum(nn(left, blocks[at]) for left, blocks in zip(lefts, blocks_of))
                for at in range(sizes["shard"])
            ]
        )

    def times_turned(left, blocks):
        return sum(nt(block_of(left, at), block) for at, block in enumerate(blocks))

    kv, w_gate, w_up, w_down, w_out = lax.optimization_barrier((kv, w_gate, w_up, w_down, w_out))
    outs, downs = gather_blocks(w_out), gather_blocks(w_down)
    gates, ups = gather_rows(w_gate), gather_rows(w_up)

    qmark, kmark = query_marks.reshape(1, -1), key_marks.reshape(-1, 1)
    forward = {"state": None, "pieces": [(kv, 0, query_marks.reshape(-1, 1))]}

    def advance(last):
        forward["state"] = forward_stage(
            queries, qmark, forward["pieces"], forward["state"], last
        )
        forward["pieces"] = []

    def forward_between(at, arrays):
        advance(False)
        *arrays, out = lax.optimization_barrier((*arrays, forward["state"][2]))
        forward["state"] = (*forward["state"][:2], out)
        if sizes["ctx"] == 8:
            there = level - at
            if at == 0:
                rows = jnp.where(column == 1, arrays[2], arrays[0][:BOUNDARY])
                forward["pieces"] = [(rows, 0, next_marks.reshape(-1, 1))]
                forward["pieces"].append((arrays[0], jnp.where(column == 1, 0, -1), None))
            else:
                forward["pieces"].append((arrays[0], jnp.where(there >= 0, 0, -1), None))
            if len(arrays) > 1:
                forward["pieces"].append((arrays[1], jnp.where(there >= 1, 0, -1), None))
        return arrays

    if line == 4:
        stages, kv_next = spread(kv, 1, slice(0, BOUNDARY), forward_between)
        advance(True)
    else:
        stages, kv_next = spread(kv, 1, slice(0, BOUNDARY), lambda at, arrays: arrays)
        forward["pieces"].append((kv_next, 0, next_marks.reshape(-1, 1)))
        for at, stage in enumerate(stages):
            advance(False)
            forward["pieces"] = [(piece, place, None) for piece, place in stage]
        advance(True)
    attended, lse = forward["state"]

    attended, q_sent = lax.optimization_barrier((attended, queries))
    q_all = lax.all_gather(q_sent, "ctx", axis=0, tiled=True)
    att = [rows_of(attended, tp), flip(rows_of(attended, 1 - tp), "tp")]
    inputs = mine.astype(F32)
    hidden = inputs + times_blocks(att, outs)
    normed_two = rms_norm(hidden, gain_ffn).astype(BF16)
    gate = [nn(normed_two, w) for w in gates]
    up = [nn(normed_two, w) for w in ups]
    logistic = [jax.nn.sigmoid(g) for g in gate]
    act = [(g * s * u).astype(BF16) for g, s, u in zip(gate, logistic, up)]
    normed_pair = flip(normed_two, "tp")
    final = hidden + times_blocks(act, downs)
    final, normed_pair = lax.optimization_barrier((final, normed_pair))
    act_two = flip(act[1], "tp")
    difference = final - teacher.reshape(own_rows, width).astype(F32)
    local_error = jnp.sum(jnp.mean(difference * difference, axis=1) * keep)
    token_total = group_rows * sizes["ctx"] * sizes["shard"]
    grad_final = token_total / count * keep[:, None] * difference
    grad_round = grad_final.astype(BF16)
    grad_act = [times_turned(grad_round, w) for w in downs]
    grad_gate = [
        (a * u * s * (1.0 + g * (1.0 - s))).astype(BF16)
        for a, u, s, g in zip(grad_act, up, logistic, gate)
    ]
    grad_up = [(a * g * s).astype(BF16) for a, g, s in zip(grad_act, gate, logistic)]
    grad_gate[0], act_two, round_sent = lax.optimization_barrier(
        (grad_gate[0], act_two, grad_round)
    )
    round_two = flip(round_sent, "tp")
    grad_two = (
        nt(grad_gate[0], gates[0])
        + nt(grad_gate[1], gates[1])
        + nt(grad_up[0], ups[0])
        + nt(grad_up[1], ups[1])
    )
    hidden_part, gain_ffn_term = jax.vjp(rms_norm, hidden, gain_ffn)[1](grad_two)
    grad_hidden = grad_final + hidden_part
    hidden_round = grad_hidden.astype(BF16)
    grad_att = [times_turned(hidden_round, w).astype(BF16) for w in outs]
    grad_theirs, round_two = lax.optimization_barrier((flip(grad_att[1], "tp"), round_two))
    sent, stat = pack_gradient(
        tp.reshape(1).astype(jnp.int32), grad_att[0], grad_theirs, attended, lse
    )

    sent, hidden_sent, gate_sent = lax.optimization_barrier((sent, hidden_round, grad_gate[1]))
    hidden_two, gate_two = flip(hidden_sent, "tp"), flip(gate_sent, "tp")

    def shard_reduce(term, slice_rows):
        if sizes["shard"] == 2:
            return term(shard) + flip(term(1 - shard).astype(BF16), "shard").astype(F32)
        whole = jnp.concatenate(
            [term(i) for i in range(sizes["shard"])], axis=0 if slice_rows else 1
        )
        return lax.psum_scatter(
            whole.astype(BF16), "shard", scatter_dimension=0 if slice_rows else 1, tiled=True
        ).astype(F32)

    def over_rows(lefts, rights, slice_left):
        def term(position):
            if slice_left:
                return sum(tn(cols_of(a, position, part), b) for a, b in zip(lefts, rights))
            return sum(tn(a, cols_of(b, position, part)) for a, b in zip(lefts, rights))

        return shard_reduce(term, slice_left).astype(BF16)

    kv_pieces = [(kv, ctx), (kv_next, jnp.where(ctx + 1 < 2 * line, ctx + 1, -1))]
    kv_pieces += [piece for stage in stages for piece in stage]
    parts = {}

    def grad_between(at, arrays):
        if at == 0:
            parts["query_grad"] = query_gradient(queries, sent, stat, kv_pieces, qmark, kmark)
            parts["hidden_two"], parts["gate_two"] = hidden_two, gate_two
            hold = ["query_grad", "hidden_two", "gate_two"]
        elif at == 1:
            query_grad, up_sent = lax.optimization_barrier((parts["query_grad"], grad_up[1]))
            parts["query_grad"] = query_grad
            parts["up_two"] = flip(up_sent, "tp")
            parts["down"] = over_rows([grad_round, round_two], [act[0], act_two], True)
            parts["out"] = over_rows(
                [hidden_round, parts["hidden_two"]],
                [rows_of(attended, tp), rows_of(attended, 1 - tp)],
                True,
            )
            hold = ["down", "out", "up_two"]
        elif at == 2:
            parts["gate"] = over_rows([normed_two, normed_pair], [grad_gate[0], parts["gate_two"]], True)
            parts["up"] = over_rows([normed_two, normed_pair], [grad_up[0], parts["up_two"]], True)
            parts["query"] = over_rows([normed_one], [parts["query_grad"]], True)
            parts["all"] = jnp.concatenate(
                [parts[name] for name in ("gate", "up", "down", "query", "out")], axis=1
            )
            hold = ["all"]
        else:
            return arrays
        held = lax.optimization_barrier((*arrays, *[parts[name] for name in hold]))
        parts.update(zip(hold, held[len(arrays) :]))
        return list(held[: len(arrays)])

    grad_stages, sent_before = spread(
        sent, -1, slice(group_rows - BOUNDARY, None), grad_between
    )
    query_grad = parts["query_grad"]
    weight_grads = lax.all_gather(
        lax.psum_scatter(parts["all"], "ctx", scatter_dimension=0, tiled=True),
        "ctx",
        axis=0,
        tiled=True,
    ).astype(F32)
    hidden_half = w_gate.shape[1]
    ends = [hidden_half, 2 * hidden_half, 3 * hidden_half, 3 * hidden_half + half]
    w_gate_grad, w_up_grad, w_down_grad, w_query_grad, w_out_grad = jnp.split(
        weight_grads, ends, axis=1
    )
    grad_pieces = [(sent, ctx), (sent_before, ctx - 1)]
    grad_pieces += [piece for stage in grad_stages for piece in stage]
    key_grad, value_half = key_gradient(
        kv, q_all, grad_pieces, key_marks.reshape(1, -1), query_marks.reshape(-1, 1)
    )
    grads = jnp.concatenate([query_grad, key_grad, value_half], axis=1)
    kv_part = over_rows([normed_one], [grads[:, half:]], True)
    kv_grad = lax.psum(kv_part, "ctx").astype(F32)
    grad_one_theirs = flip(nt(rows_of(grads, 1 - tp), weight_qkv).astype(BF16), "tp")
    grad_one = nt(rows_of(grads, tp), weight_qkv) + grad_one_theirs.astype(F32)
    input_part, gain_attn_term = jax.vjp(rms_norm, inputs, gain_attn)[1](grad_one)
    tokens_grad = grad_hidden + input_part
    first_grad = in_order(
        tp, rows_of(value_half, tp), flip(rows_of(value_half, 1 - tp), "tp"), 1
    ).astype(F32)

    small = jnp.concatenate(
        [gain_attn_term, gain_ffn_term, jnp.broadcast_to(local_error, (128,))]
    )
    small = tree_sum(small.reshape(1, -1)).reshape(-1)
    return (
        final.astype(BF16).reshape(1, own_rows, width),
        small[2 * width] / count,
        tokens_grad.reshape(1, own_rows, width),
        first_grad.reshape(1, own_rows, width),
        small[:width],
        small[width : 2 * width],
        w_query_grad,
        kv_grad[:, :half],
        kv_grad[:, half:],
        w_out_grad.T,
        w_gate_grad,
        w_up_grad,
        w_down_grad.T,
    )


def solution(mesh):
    rows = P("shard", ("ctx", "tp"), None)
    wide, tall = P("shard", "tp"), P("tp", "shard")
    return jax.shard_map(
        on_device,
        mesh=mesh,
        in_specs=(
            rows,
            rows,
            rows,
            P("shard", ("ctx", "tp")),
            P("shard", None),
            P(),
            P(),
            wide,
            wide,
            wide,
            tall,
            wide,
            wide,
            tall,
        ),
        out_specs=(rows, P(), rows, rows, P(), P(), wide, wide, wide, tall, wide, wide, tall),
        check_vma=False,
    )
```

```python
import functools

import jax
import jax.numpy as jnp
from jax import lax
from jax.experimental import pallas as pl
from jax.experimental.pallas import tpu as pltpu
from jax.sharding import PartitionSpec as P

HEAD_DIM = 64
PAIR = 2 * HEAD_DIM
LN2 = 0.6931471805599453
QUERY_SCALE = HEAD_DIM ** (-0.5) / LN2
F32 = jnp.float32
BF16 = jnp.bfloat16
BOUNDARY = 256
STAT_ROWS = 3

epsilon = 1e-06


def rms_norm(values, gain):
    return values * lax.rsqrt(jnp.mean(values * values, axis=-1, keepdims=True) + epsilon) * gain


def dot(left, right, left_dim, right_dim):
    return lax.dot_general(
        left, right, (((left_dim,), (right_dim,)), ((), ())), preferred_element_type=F32
    )


def nn(left, right):
    return dot(left, right, 1, 0)


def nt(left, right):
    return dot(left, right, 1, 1)


def tn(left, right):
    return dot(left, right, 0, 0)


def split_heads(pair):
    lane = lax.broadcasted_iota(jnp.int32, (1, PAIR), 1)
    zero = jnp.zeros_like(pair)
    return [jnp.where(lane < HEAD_DIM, pair, zero), jnp.where(lane >= HEAD_DIM, pair, zero)]


def forward_kernel(pieces, first, last, flag_ref, q_ref, *refs):
    refs = list(refs)
    qmark_ref = refs.pop(0)
    arrays = []
    for masked in pieces:
        count = 3 if masked else 2
        arrays.append(refs[:count])
        refs = refs[count:]
    if not first:
        old_high, old_total, old_out = refs[:3]
        refs = refs[3:]
    if last:
        result_ref, lse_ref = refs[:2]
        refs = refs[2:]
    high_ref, total_ref, out_ref = refs
    rows = q_ref.shape[0]
    if first:
        high_ref[0] = jnp.full((2, rows), -1e30, F32)
        total_ref[0] = jnp.zeros((2, rows), F32)
        out_ref[...] = jnp.zeros((PAIR, rows), F32)
    else:
        high_ref[0] = old_high[0]
        total_ref[0] = old_total[0]
        out_ref[...] = old_out[...]
    queries = split_heads(q_ref[...])

    def add_piece(piece, masked):
        keys = piece[0][...]
        turned = piece[1][...].T
        scores = [nt(keys, queries[h]) for h in range(2)]
        if masked:
            allowed = piece[2][...] <= qmark_ref[...]
        for h in range(2):
            score = scores[h]
            if masked:
                score = jnp.where(allowed, score, -1e30)
            highest = high_ref[0, h : h + 1, :]
            top = jnp.maximum(highest, jnp.max(score, axis=0, keepdims=True))
            power = jnp.exp2(score - top)
            shrink = jnp.exp2(highest - top)
            high_ref[0, h : h + 1, :] = top
            total_ref[0, h : h + 1, :] = total_ref[0, h : h + 1, :] * shrink + jnp.sum(
                power, axis=0, keepdims=True
            )
            columns = pl.ds(HEAD_DIM * h, HEAD_DIM)
            out_ref[columns, :] = out_ref[columns, :] * shrink + nn(
                turned[HEAD_DIM * h : HEAD_DIM * (h + 1)], power.astype(BF16)
            )

    for at, masked in enumerate(pieces):
        if masked:
            add_piece(arrays[at], True)
        else:
            pl.when(flag_ref[at] >= 0)(functools.partial(add_piece, arrays[at], False))
    if last:
        for h in range(2):
            columns = pl.ds(HEAD_DIM * h, HEAD_DIM)
            out_ref[columns, :] = out_ref[columns, :] / total_ref[0, h : h + 1, :]
        result_ref[...] = out_ref[...].T.astype(BF16)
        lse_ref[0] = high_ref[0] + jnp.log2(total_ref[0])


def forward_stage(queries, qmark, pieces, state, last):
    rows, width = queries.shape
    pairs = width // PAIR
    flags = jnp.stack([jnp.asarray(place, jnp.int32) for _, place, _ in pieces])
    args = [queries, qmark]
    in_specs = [
        pl.BlockSpec((rows, PAIR), lambda h, s: (0, h)),
        pl.BlockSpec((1, rows), lambda h, s: (0, 0)),
    ]
    keys = 0
    for kv, _, marks in pieces:
        count = kv.shape[0]
        keys += count
        args += [kv, kv]
        in_specs += [
            pl.BlockSpec((count, PAIR), lambda h, s: (0, h)),
            pl.BlockSpec((count, PAIR), lambda h, s: (0, pairs + h)),
        ]
        if marks is not None:
            args.append(marks)
            in_specs.append(pl.BlockSpec((count, 1), lambda h, s: (0, 0)))
    stat = jax.ShapeDtypeStruct((pairs, 2, rows), F32)
    stat_spec = pl.BlockSpec((1, 2, rows), lambda h, s: (h, 0, 0))
    state_specs = [stat_spec, stat_spec, pl.BlockSpec((PAIR, rows), lambda h, s: (h, 0))]
    state_shapes = [stat, stat, jax.ShapeDtypeStruct((width, rows), F32)]
    if state is not None:
        args += list(state)
        in_specs += state_specs
    if last:
        out_specs = [pl.BlockSpec((rows, PAIR), lambda h, s: (0, h)), stat_spec]
        out_shape = [jax.ShapeDtypeStruct((rows, width), BF16), stat]
        scratch = [
            pltpu.VMEM((1, 2, rows), F32),
            pltpu.VMEM((1, 2, rows), F32),
            pltpu.VMEM((PAIR, rows), F32),
        ]
    else:
        out_specs, out_shape, scratch = state_specs, state_shapes, []
    return pl.pallas_call(
        functools.partial(
            forward_kernel, [m is not None for _, _, m in pieces], state is None, last
        ),
        grid_spec=pltpu.PrefetchScalarGridSpec(
            num_scalar_prefetch=1,
            grid=(pairs,),
            in_specs=in_specs,
            out_specs=out_specs,
            scratch_shapes=scratch,
        ),
        out_shape=out_shape,
        compiler_params=pltpu.CompilerParams(vmem_limit_bytes=40 << 20),
        cost_estimate=pl.CostEstimate(
            flops=16 * rows * keys * width,
            bytes_accessed=8 * keys * width,
            transcendentals=rows * keys * width // HEAD_DIM,
        ),
    )(flags, *args)


def stats_kernel(rows, place_ref, mine_ref, other_ref, out_ref, lse_ref, sent_ref, stat_ref):
    half = mine_ref.shape[0]
    place = place_ref[0]
    sent_ref[pl.ds(pl.multiple_of(place * half, half), half), :] = mine_ref[...]
    sent_ref[pl.ds(pl.multiple_of((1 - place) * half, half), half), :] = other_ref[...]
    width = mine_ref.shape[1]
    heads = width // HEAD_DIM
    deltas = []
    for pair in range(width // PAIR):
        columns = pl.ds(pair * PAIR, PAIR)
        grad = sent_ref[pl.ds(0, rows), columns]
        terms = (grad.astype(F32) * out_ref[:, columns].astype(F32)).T
        deltas += [
            jnp.sum(terms[:HEAD_DIM], axis=0, keepdims=True),
            jnp.sum(terms[HEAD_DIM:], axis=0, keepdims=True),
        ]
    stat = jnp.concatenate(
        [lse_ref[pair] for pair in range(width // PAIR)] + deltas, axis=0
    )
    stat_ref[...] = stat
    for at in range(STAT_ROWS):
        piece = stat.astype(BF16)
        sent_ref[pl.ds(rows + at * 2 * heads, 2 * heads), :] = piece
        stat = stat - piece.astype(F32)


def pack_gradient(place, mine, other, attended, lse):
    rows, width = attended.shape
    stat_rows = 2 * width // HEAD_DIM
    return pl.pallas_call(
        functools.partial(stats_kernel, rows),
        in_specs=[pl.BlockSpec(memory_space=pltpu.SMEM)]
        + [pl.BlockSpec(memory_space=pltpu.VMEM)] * 4,
        out_specs=[pl.BlockSpec(memory_space=pltpu.VMEM)] * 2,
        out_shape=[
            jax.ShapeDtypeStruct((rows + STAT_ROWS * stat_rows, width), BF16),
            jax.ShapeDtypeStruct((stat_rows, rows), F32),
        ],
    )(place, mine, other, attended, lse)


def query_kernel(
    sizes, step_keys, place_ref, q_ref, grad_ref, stat_ref, qmark_ref, kmark_ref, *refs
):
    count = len(sizes)
    pieces, out_ref, kv_ref, kt_ref, sems = refs[:count], *refs[count:]
    rows, length = q_ref.shape[0], kv_ref.shape[0]
    width = kv_ref.shape[1] // 2
    pair = pl.program_id(0)
    index = place_ref[0]
    full = (index * rows) // step_keys
    end = jnp.minimum(
        ((index + 1) * rows + BOUNDARY + step_keys - 1) // step_keys, length // step_keys
    )

    def copy(at):
        start = pl.multiple_of(place_ref[at] * rows, rows)
        return pltpu.make_async_copy(
            pieces[at], kv_ref.at[pl.ds(start, sizes[at]), :], sems.at[at]
        )

    @pl.when(pair == 0)
    def _():
        for at in range(count):
            pl.when(place_ref[at] >= 0)(lambda at=at: copy(at).start())

        def clear(at, _):
            start = pl.multiple_of(at * BOUNDARY, BOUNDARY)
            kv_ref[pl.ds(start, BOUNDARY), :] = jnp.zeros((BOUNDARY, 2 * width), BF16)
            return 0

        ratio = rows // BOUNDARY
        lax.fori_loop((index + 1) * ratio + 1, end * (step_keys // BOUNDARY), clear, 0)
        for at in range(count):
            pl.when(place_ref[at] >= 0)(lambda at=at: copy(at).wait())

    queries, grads = split_heads(q_ref[...]), split_heads(grad_ref[...])
    k_columns = pl.ds(pl.multiple_of(pair * PAIR, PAIR), PAIR)
    v_columns = pl.ds(pl.multiple_of(width + pair * PAIR, PAIR), PAIR)
    lse = [stat_ref[pl.ds(2 * pair + h, 1), :] for h in range(2)]
    delta = [
        stat_ref[pl.ds(stat_ref.shape[0] // 2 + 2 * pair + h, 1), :] for h in range(2)
    ]

    def turn(at, _):
        start = pl.multiple_of(at * step_keys, step_keys)
        kt_ref[:, pl.ds(start, step_keys)] = kv_ref[pl.ds(start, step_keys), k_columns].T
        return 0

    lax.fori_loop(0, end, turn, 0)

    def step(masked):
        def body(at, state):
            start = pl.multiple_of(at * step_keys, step_keys)
            keys = kv_ref[pl.ds(start, step_keys), k_columns]
            values = kv_ref[pl.ds(start, step_keys), v_columns]
            if masked:
                allowed = kmark_ref[pl.ds(start, step_keys), :] <= qmark_ref[...]
            new = []
            for h in range(2):
                score = nt(keys, queries[h])
                slope = nt(values, grads[h])
                prob = jnp.exp2(score - lse[h])
                if masked:
                    prob = jnp.where(allowed, prob, 0.0)
                grad = (prob * (slope - delta[h])).astype(BF16)
                turned = kt_ref[pl.ds(HEAD_DIM * h, HEAD_DIM), pl.ds(start, step_keys)]
                new.append(state[h] + nn(turned, grad))
            return tuple(new)

        return body

    empty = jnp.zeros((HEAD_DIM, rows), F32)
    state = lax.fori_loop(full, end, step(True), (empty, empty))
    state = lax.fori_loop(0, full, step(False), state)
    out_ref[...] = (jnp.concatenate(state, axis=0).T * HEAD_DIM ** (-0.5)).astype(out_ref.dtype)


def query_gradient(queries, sent, stat, pieces, qmark, kmark, step_keys=1024):
    rows, width = queries.shape
    length = kmark.shape[0]
    pairs = width // PAIR
    places = jnp.stack([jnp.asarray(place, jnp.int32) for _, place in pieces])
    sizes = [kv.shape[0] for kv, _ in pieces]
    return pl.pallas_call(
        functools.partial(query_kernel, sizes, step_keys),
        grid_spec=pltpu.PrefetchScalarGridSpec(
            num_scalar_prefetch=1,
            grid=(pairs,),
            in_specs=[
                pl.BlockSpec((rows, PAIR), lambda h, s: (0, h)),
                pl.BlockSpec((rows, PAIR), lambda h, s: (0, h)),
                pl.BlockSpec(stat.shape, lambda h, s: (0, 0)),
                pl.BlockSpec((1, rows), lambda h, s: (0, 0)),
                pl.BlockSpec((length, 1), lambda h, s: (0, 0)),
            ]
            + [pl.BlockSpec(memory_space=pl.ANY)] * len(pieces),
            out_specs=pl.BlockSpec((rows, PAIR), lambda h, s: (0, h)),
            scratch_shapes=[
                pltpu.VMEM((length, 2 * width), BF16),
                pltpu.VMEM((PAIR, length), BF16),
                pltpu.SemaphoreType.DMA((len(pieces),)),
            ],
        ),
        out_shape=jax.ShapeDtypeStruct((rows, width), BF16),
        compiler_params=pltpu.CompilerParams(vmem_limit_bytes=56 << 20),
        cost_estimate=pl.CostEstimate(
            flops=rows * length * width,
            bytes_accessed=4 * length * width,
            transcendentals=rows * length * width // HEAD_DIM,
        ),
    )(places, queries, sent, stat, qmark, kmark, *[kv for kv, _ in pieces])


def key_kernel(
    sizes, step_queries, place_ref, k_ref, v_ref, q_ref, qmark_ref, kmark_ref, *refs
):
    count = len(sizes)
    pieces = refs[:count]
    dk_ref, dv_ref, grad_ref, raw_ref, stat_ref, sems = refs[count:]
    rows, length = k_ref.shape[0], q_ref.shape[0]
    width = grad_ref.shape[1]
    stat_rows = stat_ref.shape[0]
    packed = STAT_ROWS * stat_rows
    pair = pl.program_id(0)
    index = place_ref[0]

    def copies(at):
        size = sizes[at]
        start = pl.multiple_of(place_ref[at] * rows + rows - size, BOUNDARY)
        return (
            pltpu.make_async_copy(
                pieces[at].at[pl.ds(0, size), :],
                grad_ref.at[pl.ds(start, size), :],
                sems.at[2 * at],
            ),
            pltpu.make_async_copy(
                pieces[at].at[pl.ds(size, packed), :],
                raw_ref.at[at],
                sems.at[2 * at + 1],
            ),
        )

    @pl.when(pair == 0)
    def _():
        for at in range(count):

            @pl.when(place_ref[at] >= 0)
            def _(at=at):
                for one in copies(at):
                    one.start()

        @pl.when(index > 0)
        def _():
            start = pl.multiple_of((index - 1) * rows, rows)
            grad_ref[pl.ds(start, rows - BOUNDARY), :] = jnp.zeros(
                (rows - BOUNDARY, width), BF16
            )

        for at in range(count):

            @pl.when(place_ref[at] >= 0)
            def _(at=at):
                for one in copies(at):
                    one.wait()
                stat = raw_ref[at, :stat_rows].astype(F32)
                for part in range(1, STAT_ROWS):
                    stat = stat + raw_ref[
                        at, part * stat_rows : (part + 1) * stat_rows
                    ].astype(F32)
                start = pl.multiple_of(place_ref[at] * rows, rows)
                stat_ref[:, pl.ds(start, rows)] = stat

    keys, values = split_heads(k_ref[...]), split_heads(v_ref[...])
    columns = pl.ds(pl.multiple_of(pair * PAIR, PAIR), PAIR)

    def step(masked):
        def body(at, state):
            start = pl.multiple_of(at * step_queries, step_queries)
            span = pl.ds(start, step_queries)
            queries = q_ref[span, :]
            grads = grad_ref[span, columns]
            if masked:
                allowed = kmark_ref[...] <= qmark_ref[:, span]
            new = []
            for h in range(2):
                lse = stat_ref[pl.ds(2 * pair + h, 1), span]
                delta = stat_ref[pl.ds(stat_rows // 2 + 2 * pair + h, 1), span]
                score = nt(keys[h], queries)
                slope = nt(values[h], grads)
                prob = jnp.exp2(score - lse)
                if masked:
                    prob = jnp.where(allowed, prob, 0.0)
                grad = prob * (slope - delta)
                new += [
                    state[2 * h] + nn(grad.astype(BF16), queries),
                    state[2 * h + 1] + nn(prob.astype(BF16), grads),
                ]
            return tuple(new)

        return body

    empty = jnp.zeros((rows, PAIR), F32)
    first = jnp.maximum((index * rows - BOUNDARY) // step_queries, 0)
    own = ((index + 1) * rows + step_queries - 1) // step_queries
    state = lax.fori_loop(first, own, step(True), (empty,) * 4)
    state = lax.fori_loop(own, length // step_queries, step(False), state)
    lane = lax.broadcasted_iota(jnp.int32, (1, PAIR), 1)
    dk_ref[...] = (jnp.where(lane < HEAD_DIM, state[0], state[2]) * LN2).astype(dk_ref.dtype)
    dv_ref[...] = (0.5 * jnp.where(lane < HEAD_DIM, state[1], state[3])).astype(dv_ref.dtype)


def key_gradient(kv, q_all, pieces, qmark, kmark, step_queries=512):
    rows = kv.shape[0]
    length, width = q_all.shape
    pairs = width // PAIR
    stat_rows = 2 * width // HEAD_DIM
    packed = STAT_ROWS * stat_rows
    places = jnp.stack([jnp.asarray(place, jnp.int32) for _, place in pieces])
    sizes = [sent.shape[0] - packed for sent, _ in pieces]
    return pl.pallas_call(
        functools.partial(key_kernel, sizes, step_queries),
        grid_spec=pltpu.PrefetchScalarGridSpec(
            num_scalar_prefetch=1,
            grid=(pairs,),
            in_specs=[
                pl.BlockSpec((rows, PAIR), lambda h, s: (0, h)),
                pl.BlockSpec((rows, PAIR), lambda h, s: (0, pairs + h)),
                pl.BlockSpec((length, PAIR), lambda h, s: (0, h)),
                pl.BlockSpec((1, length), lambda h, s: (0, 0)),
                pl.BlockSpec((rows, 1), lambda h, s: (0, 0)),
            ]
            + [pl.BlockSpec(memory_space=pl.ANY)] * len(pieces),
            out_specs=[pl.BlockSpec((rows, PAIR), lambda h, s: (0, h))] * 2,
            scratch_shapes=[
                pltpu.VMEM((length, width), BF16),
                pltpu.VMEM((len(pieces), packed, rows), BF16),
                pltpu.VMEM((stat_rows, length), F32),
                pltpu.SemaphoreType.DMA((2 * len(pieces),)),
            ],
        ),
        out_shape=[jax.ShapeDtypeStruct((rows, width), BF16)] * 2,
        compiler_params=pltpu.CompilerParams(vmem_limit_bytes=56 << 20),
        cost_estimate=pl.CostEstimate(
            flops=rows * length * width,
            bytes_accessed=4 * length * width,
            transcendentals=rows * length * width // HEAD_DIM,
        ),
    )(places, kv, kv, q_all, qmark, kmark, *[sent for sent, _ in pieces])


def on_device(
    tokens,
    value_first,
    teacher,
    valid,
    blocks,
    gain_attn,
    gain_ffn,
    w_query,
    w_key,
    w_value,
    w_out,
    w_gate,
    w_up,
    w_down,
):
    width = tokens.shape[2]
    own_rows = tokens.shape[1]
    sizes = {axis: lax.axis_size(axis) for axis in ("shard", "ctx", "tp")}
    shard, ctx, tp = (lax.axis_index(axis) for axis in ("shard", "ctx", "tp"))
    group_rows = own_rows * sizes["tp"]
    half = w_query.shape[1]
    part = w_query.shape[0]
    line = sizes["ctx"] // 2

    def flip(values, axis, bit=1):
        return lax.ppermute(values, axis, [(i, i ^ bit) for i in range(sizes[axis])])

    def tree_sum(values):
        for axis, size in sizes.items():
            bit = 1
            while bit < size:
                values = values + flip(values, axis, bit)
                bit *= 2
        return values

    def in_order(position, mine, other, axis):
        first = position == 0
        return jnp.concatenate(
            [jnp.where(first, mine, other), jnp.where(first, other, mine)], axis=axis
        )

    def shard_gather(values, axis):
        if sizes["shard"] == 2:
            return in_order(shard, values, flip(values, "shard"), axis)
        return lax.all_gather(values, "shard", axis=axis, tiled=True)

    def ctx_bits():
        bit = 1
        while bit < sizes["ctx"]:
            yield bit
            bit *= 2

    def reduce_ctx(parts, orders, between):
        parts, steps = list(parts), len(orders[0])
        for step in range(steps):
            for at, order in enumerate(orders):
                size = parts[at].shape[0] // 2
                side = (ctx // order[step]) % 2
                kept = lax.dynamic_slice_in_dim(parts[at], side * size, size, 0)
                sent = lax.dynamic_slice_in_dim(parts[at], (1 - side) * size, size, 0)
                got = flip(sent, "ctx", order[step])
                parts[at] = (kept.astype(F32) + got.astype(F32)).astype(BF16)
            parts = between(step, parts)
        for step in reversed(range(steps)):
            for at, order in enumerate(orders):
                side = (ctx // order[step]) % 2
                parts[at] = in_order(side, parts[at], flip(parts[at], "ctx", order[step]), 0)
        return parts

    def rows_of(values, position):
        return lax.dynamic_slice_in_dim(values, position * own_rows, own_rows, 0)

    def cols_of(values, position, size):
        return lax.dynamic_slice_in_dim(values, position * size, size, 1)

    level, column = ctx // 2, ctx % 2

    def spread(own, step, edge, between):
        if line != 4:
            gathered = lax.all_gather(own, "ctx", axis=0, tiled=False)
            below = [(place < ctx) if step == 1 else (place > ctx) for place in range(2 * line)]
            pieces = [
                (gathered[place], jnp.where(below[place], place, -1)) for place in range(2 * line)
            ]
            beside = jnp.clip(ctx + step, 0, 2 * line - 1)
            rows = lax.dynamic_index_in_dim(gathered, beside, 0, keepdims=False)[edge]
            gathered, rows = between(0, [pieces[0][0], rows])
            pieces[0] = (gathered, pieces[0][1])
            stages = [pieces[:2]]
            for i in range(2, 2 * line, 2):
                (first,) = between(i // 2, [pieces[i][0]])
                stages.append([(first, pieces[i][1]), pieces[i + 1]])
            return stages, rows
        along = [(i, i + 2 * step) for i in range(2 * line) if 0 <= i + 2 * step < 2 * line]
        across = flip(own, "ctx")
        near = 1 if step == 1 else 0
        diagonal = [
            (i + step, i) for i in range(2 * line) if i % 2 == near and 0 <= i + step < 2 * line
        ]
        beside = lax.ppermute(own[edge], "ctx", diagonal)
        moving = lax.ppermute(own, "ctx", along)
        across, moving, beside = between(0, [across, moving, beside])
        rows = jnp.where(column == near, beside, across[edge])
        stages = [[(across, jnp.where(column == near, ctx - step, -1))]]
        for hop in range(1, line):
            there = level - step * hop
            exists = (there >= 0) & (there < line)
            stages[-1].append((moving, jnp.where(exists, 2 * there + column, -1)))
            across = flip(moving, "ctx")
            if hop + 1 < line:
                moving = lax.ppermute(moving, "ctx", along)
                across, moving = between(hop, [across, moving])
            else:
                (across,) = between(hop, [across])
            stages.append([(across, jnp.where(exists, 2 * there + 1 - column, -1))])
        return stages, rows

    def shard_reduce(term, slice_rows):
        if sizes["shard"] == 2:
            return term(shard) + flip(term(1 - shard).astype(BF16), "shard").astype(F32)
        whole = jnp.concatenate(
            [term(i) for i in range(sizes["shard"])], axis=0 if slice_rows else 1
        )
        return lax.psum_scatter(
            whole.astype(BF16), "shard", scatter_dimension=0 if slice_rows else 1, tiled=True
        ).astype(F32)

    def over_rows(lefts, rights, slice_left):
        def term(position):
            if slice_left:
                return sum(tn(cols_of(a, position, part), b) for a, b in zip(lefts, rights))
            return sum(tn(a, cols_of(b, position, part)) for a, b in zip(lefts, rights))

        return shard_reduce(term, slice_left).astype(BF16)

    mine = tokens.reshape(own_rows, width)
    first_own = value_first.reshape(own_rows, width)
    key_marks = blocks.reshape(-1)
    padded_marks = jnp.concatenate([key_marks, jnp.full((BOUNDARY,), 1 << 30, key_marks.dtype)])
    query_marks = lax.dynamic_slice_in_dim(key_marks, ctx * group_rows, group_rows, 0)
    next_marks = lax.dynamic_slice_in_dim(padded_marks, (ctx + 1) * group_rows, BOUNDARY, 0)
    keep = valid.reshape(own_rows).astype(F32)

    theirs = flip(mine, "tp")
    first_theirs = flip(cols_of(first_own, 1 - tp, half), "tp")
    weight_qkv = shard_gather(jnp.concatenate([w_query, w_key, w_value], axis=1), 0)
    count = tree_sum(jnp.broadcast_to(jnp.sum(keep), (1, 128)))[0, 0]

    group = in_order(tp, mine, theirs, 0).astype(F32)
    normed_one = rms_norm(group, gain_attn).astype(BF16)
    first_group = in_order(tp, cols_of(first_own, tp, half), first_theirs, 0).astype(F32)
    qkv = nn(normed_one, weight_qkv)
    queries = (qkv[:, :half] * QUERY_SCALE).astype(BF16)
    kv = jnp.concatenate(
        [qkv[:, half : 2 * half], 0.5 * qkv[:, 2 * half :] + 0.5 * first_group], axis=1
    ).astype(BF16)

    def gather_blocks(values):
        if sizes["shard"] == 2:
            both = [values, flip(values, "tp")]
            return [[one, flip(one, "shard")] for one in both]
        both = [values, flip(values, "tp")]
        gathered = [lax.all_gather(one, "shard", axis=0, tiled=False) for one in both]
        return [[one[i] for i in range(sizes["shard"])] for one in gathered]

    def block_of(values, at):
        if sizes["shard"] == 2:
            return cols_of(values, shard if at == 0 else 1 - shard, part)
        return values[:, at * part : (at + 1) * part]

    def join_blocks(terms):
        if sizes["shard"] == 2:
            return in_order(shard, terms[0], terms[1], 1)
        return jnp.concatenate(terms, axis=1)

    def times_blocks(lefts, blocks_of):
        return join_blocks(
            [
                sum(nn(left, blocks[at]) for left, blocks in zip(lefts, blocks_of))
                for at in range(sizes["shard"])
            ]
        )

    def times_turned(left, blocks):
        return sum(nt(block_of(left, at), block) for at, block in enumerate(blocks))

    kv, w_gate, w_up, w_down, w_out, count = lax.optimization_barrier(
        (kv, w_gate, w_up, w_down, w_out, count)
    )
    outs = gather_blocks(w_out)
    gate_weight, up_weight = shard_gather(w_gate, 0), shard_gather(w_up, 0)
    down_weight = shard_gather(w_down, 1)

    qmark, kmark = query_marks.reshape(1, -1), key_marks.reshape(-1, 1)
    forward = {"state": None, "pieces": [(kv, 0, query_marks.reshape(-1, 1))]}

    def advance(last):
        forward["state"] = forward_stage(
            queries, qmark, forward["pieces"], forward["state"], last
        )
        forward["pieces"] = []

    def forward_between(at, arrays):
        advance(False)
        *arrays, out = lax.optimization_barrier((*arrays, forward["state"][2]))
        forward["state"] = (*forward["state"][:2], out)
        if sizes["ctx"] == 8:
            there = level - at
            if at == 0:
                rows = jnp.where(column == 1, arrays[2], arrays[0][:BOUNDARY])
                forward["pieces"] = [(rows, 0, next_marks.reshape(-1, 1))]
                forward["pieces"].append((arrays[0], jnp.where(column == 1, 0, -1), None))
            else:
                forward["pieces"].append((arrays[0], jnp.where(there >= 0, 0, -1), None))
            if len(arrays) > 1:
                forward["pieces"].append((arrays[1], jnp.where(there >= 1, 0, -1), None))
        return arrays

    if line == 4:
        stages, kv_next = spread(kv, 1, slice(0, BOUNDARY), forward_between)
        advance(True)
    else:
        stages, kv_next = spread(kv, 1, slice(0, BOUNDARY), lambda at, arrays: arrays)
        forward["pieces"].append((kv_next, 0, next_marks.reshape(-1, 1)))
        for at, stage in enumerate(stages):
            advance(False)
            forward["pieces"] = [(piece, place, None) for piece, place in stage]
        advance(True)
    attended, lse = forward["state"]

    attended, q_sent = lax.optimization_barrier((attended, queries))
    q_all = lax.all_gather(q_sent, "ctx", axis=0, tiled=True)
    att = [rows_of(attended, tp), flip(rows_of(attended, 1 - tp), "tp")]
    inputs = mine.astype(F32)
    hidden = inputs + times_blocks(att, outs)
    normed_two = rms_norm(hidden, gain_ffn).astype(BF16)
    normed = [normed_two, flip(normed_two, "tp")]
    gate, up, logistic, act = [], [], [], []

    def widen(rows):
        gate.append(nn(rows, gate_weight))
        up.append(nn(rows, up_weight))
        logistic.append(jax.nn.sigmoid(gate[-1]))
        act.append((gate[-1] * logistic[-1] * up[-1]).astype(BF16))

    widen(normed[0])
    normed[1], act[0] = lax.optimization_barrier((normed[1], act[0]))
    widen(normed[1])
    down_theirs = flip(nn(act[1], down_weight).astype(BF16), "tp")
    final = hidden + (nn(act[0], down_weight) + down_theirs.astype(F32))
    difference = final - teacher.reshape(own_rows, width).astype(F32)
    local_error = jnp.sum(jnp.mean(difference * difference, axis=1) * keep)
    token_total = group_rows * sizes["ctx"] * sizes["shard"]
    grad_final = token_total / count * keep[:, None] * difference
    grad_round = grad_final.astype(BF16)
    rounds = [grad_round, flip(grad_round, "tp")]
    grad_gate, grad_up = [], []

    def back(at):
        grad_act = nt(rounds[at], down_weight)
        part = grad_act * logistic[at]
        grad_gate.append((part * up[at] * (1.0 + gate[at] * (1.0 - logistic[at]))).astype(BF16))
        grad_up.append((part * gate[at]).astype(BF16))

    back(0)
    rounds[1], grad_gate[0], grad_up[0] = lax.optimization_barrier(
        (rounds[1], grad_gate[0], grad_up[0])
    )
    back(1)
    two_sent = (nt(grad_gate[1], gate_weight) + nt(grad_up[1], up_weight)).astype(BF16)
    two_theirs = flip(two_sent, "tp")
    gate_part = over_rows(normed, grad_gate, True)
    up_part = over_rows(normed, grad_up, True)
    down_part = over_rows(rounds, act, True)
    two_own = nt(grad_gate[0], gate_weight) + nt(grad_up[0], up_weight)
    two_theirs, two_own, gate_part, up_part, down_part = lax.optimization_barrier(
        (two_theirs, two_own, gate_part, up_part, down_part)
    )
    grad_two = two_own + two_theirs.astype(F32)
    hidden_part, gain_ffn_term = jax.vjp(rms_norm, hidden, gain_ffn)[1](grad_two)
    grad_hidden = grad_final + hidden_part
    hidden_round = grad_hidden.astype(BF16)
    grad_att = [times_turned(hidden_round, w).astype(BF16) for w in outs]
    grad_theirs = flip(grad_att[1], "tp")
    sent, stat = pack_gradient(
        tp.reshape(1).astype(jnp.int32), grad_att[0], grad_theirs, attended, lse
    )

    hidden_two = flip(hidden_round, "tp")

    kv_pieces = [(kv, ctx), (kv_next, jnp.where(ctx + 1 < 2 * line, ctx + 1, -1))]
    kv_pieces += [piece for stage in stages for piece in stage]
    parts = {}

    def grad_between(at, arrays):
        if at == 0:
            *arrays, hidden_held = lax.optimization_barrier((*arrays[:-1], arrays[-1], hidden_two)) if len(arrays) < 3 else (
                *arrays[:2],
                *lax.optimization_barrier((arrays[2], hidden_two)),
            )
            parts["out"] = over_rows(
                [hidden_round, hidden_held],
                [rows_of(attended, tp), rows_of(attended, 1 - tp)],
                True,
            )
            parts["all"] = jnp.concatenate(
                [gate_part, up_part, down_part, parts["out"]], axis=1
            )
            hold = ["all"]
        elif at == 1:
            held_stat, parts["q_all"], parts["all"] = lax.optimization_barrier(
                (stat, q_all, parts["all"])
            )
            parts["query_grad"] = query_gradient(
                queries, sent, held_stat, kv_pieces, qmark, kmark
            )
            hold = ["query_grad"]
        elif at == 2:
            parts["query"] = over_rows([normed_one], [parts["query_grad"]], True)
            hold = ["query"]
        else:
            return arrays
        held = lax.optimization_barrier((*arrays, *[parts[name] for name in hold]))
        parts.update(zip(hold, held[len(arrays) :]))
        return list(held[: len(arrays)])

    grad_stages, sent_before = spread(
        sent, -1, slice(group_rows - BOUNDARY, None), grad_between
    )
    query_grad = parts["query_grad"]
    scattered = lax.psum_scatter(parts["all"], "ctx", scatter_dimension=0, tiled=True)
    grad_pieces = [(sent, ctx), (sent_before, ctx - 1)]
    grad_pieces += [piece for stage in grad_stages for piece in stage]
    key_grad, value_half = key_gradient(
        kv, parts["q_all"], grad_pieces, key_marks.reshape(1, -1), query_marks.reshape(-1, 1)
    )
    scattered, key_grad, value_half = lax.optimization_barrier(
        (scattered, key_grad, value_half)
    )
    weight_grads = lax.all_gather(scattered, "ctx", axis=0, tiled=True).astype(F32)
    hidden_half = w_gate.shape[1]
    w_gate_grad, w_up_grad, w_down_grad, w_out_grad = jnp.split(
        weight_grads, [hidden_half, 2 * hidden_half, 3 * hidden_half], axis=1
    )
    grads = jnp.concatenate([query_grad, key_grad, value_half], axis=1)
    key_part = over_rows([normed_one], [key_grad], True)
    value_part = over_rows([normed_one], [value_half], True)
    last = {}

    def finish(step, parts):
        if step == 0:
            *parts, held = lax.optimization_barrier((*parts, grads))
            theirs = flip(nt(rows_of(held, 1 - tp), weight_qkv).astype(BF16), "tp")
            last["own"] = nt(rows_of(held, tp), weight_qkv)
            last["theirs"] = theirs
            last["value"] = flip(rows_of(held[:, 2 * half :], 1 - tp), "tp")
        if step == 1:
            *parts, last["own"], last["theirs"], last["value"] = lax.optimization_barrier(
                (*parts, last["own"], last["theirs"], last["value"])
            )
        return parts

    bits = list(ctx_bits())
    w_query_grad, w_key_grad, w_value_grad = reduce_ctx(
        [parts["query"], key_part, value_part],
        [bits[2:] + bits[:2], bits, bits[1:] + bits[:1]],
        finish,
    )
    grad_one = last["own"] + last["theirs"].astype(F32)
    input_part, gain_attn_term = jax.vjp(rms_norm, inputs, gain_attn)[1](grad_one)
    tokens_grad = grad_hidden + input_part
    first_grad = in_order(tp, rows_of(value_half, tp), last["value"], 1).astype(F32)

    small = jnp.concatenate(
        [gain_attn_term, gain_ffn_term, jnp.broadcast_to(local_error, (128,))]
    )
    small = tree_sum(small.reshape(1, -1)).reshape(-1)
    return (
        final.astype(BF16).reshape(1, own_rows, width),
        small[2 * width] / count,
        tokens_grad.reshape(1, own_rows, width),
        first_grad.reshape(1, own_rows, width),
        small[:width],
        small[width : 2 * width],
        w_query_grad.astype(F32),
        w_key_grad.astype(F32),
        w_value_grad.astype(F32),
        w_out_grad.T,
        w_gate_grad,
        w_up_grad,
        w_down_grad.T,
    )


def solution(mesh):
    rows = P("shard", ("ctx", "tp"), None)
    wide, tall = P("shard", "tp"), P("tp", "shard")
    return jax.shard_map(
        on_device,
        mesh=mesh,
        in_specs=(
            rows,
            rows,
            rows,
            P("shard", ("ctx", "tp")),
            P("shard", None),
            P(),
            P(),
            wide,
            wide,
            wide,
            tall,
            wide,
            wide,
            tall,
        ),
        out_specs=(rows, P(), rows, rows, P(), P(), wide, wide, wide, tall, wide, wide, tall),
        check_vma=False,
    )
```

```python
import functools

import jax
import jax.numpy as jnp
from jax import lax
from jax.experimental import pallas as pl
from jax.experimental.pallas import tpu as pltpu
from jax.sharding import PartitionSpec as P

HEAD_DIM = 64
PAIR = 2 * HEAD_DIM
LN2 = 0.6931471805599453
QUERY_SCALE = HEAD_DIM ** (-0.5) / LN2
F32 = jnp.float32
BF16 = jnp.bfloat16
BOUNDARY = 256
STAT_ROWS = 3

CTX = ("line", "side")

epsilon = 1e-06


def rms_norm(values, gain):
    return values * lax.rsqrt(jnp.mean(values * values, axis=-1, keepdims=True) + epsilon) * gain


def dot(left, right, left_dim, right_dim):
    return lax.dot_general(
        left, right, (((left_dim,), (right_dim,)), ((), ())), preferred_element_type=F32
    )


def nn(left, right):
    return dot(left, right, 1, 0)


def nt(left, right):
    return dot(left, right, 1, 1)


def tn(left, right):
    return dot(left, right, 0, 0)


def split_heads(pair):
    lane = lax.broadcasted_iota(jnp.int32, (1, PAIR), 1)
    zero = jnp.zeros_like(pair)
    return [jnp.where(lane < HEAD_DIM, pair, zero), jnp.where(lane >= HEAD_DIM, pair, zero)]


def forward_kernel(pieces, first, last, flag_ref, q_ref, *refs):
    refs = list(refs)
    qmark_ref = refs.pop(0)
    arrays = []
    for masked in pieces:
        count = 3 if masked else 2
        arrays.append(refs[:count])
        refs = refs[count:]
    if not first:
        old_high, old_total, old_out = refs[:3]
        refs = refs[3:]
    if last:
        result_ref, lse_ref = refs[:2]
        refs = refs[2:]
    high_ref, total_ref, out_ref = refs
    rows = q_ref.shape[0]
    if first:
        high_ref[0] = jnp.full((2, rows), -1e30, F32)
        total_ref[0] = jnp.zeros((2, rows), F32)
        out_ref[...] = jnp.zeros((PAIR, rows), F32)
    else:
        high_ref[0] = old_high[0]
        total_ref[0] = old_total[0]
        out_ref[...] = old_out[...]
    queries = split_heads(q_ref[...])

    def add_piece(piece, masked):
        keys = piece[0][...]
        turned = piece[1][...].T
        scores = [nt(keys, queries[h]) for h in range(2)]
        if masked:
            allowed = piece[2][...] <= qmark_ref[...]
        for h in range(2):
            score = scores[h]
            if masked:
                score = jnp.where(allowed, score, -1e30)
            highest = high_ref[0, h : h + 1, :]
            top = jnp.maximum(highest, jnp.max(score, axis=0, keepdims=True))
            power = jnp.exp2(score - top)
            shrink = jnp.exp2(highest - top)
            high_ref[0, h : h + 1, :] = top
            total_ref[0, h : h + 1, :] = total_ref[0, h : h + 1, :] * shrink + jnp.sum(
                power, axis=0, keepdims=True
            )
            columns = pl.ds(HEAD_DIM * h, HEAD_DIM)
            out_ref[columns, :] = out_ref[columns, :] * shrink + nn(
                turned[HEAD_DIM * h : HEAD_DIM * (h + 1)], power.astype(BF16)
            )

    for at, masked in enumerate(pieces):
        if masked:
            add_piece(arrays[at], True)
        else:
            pl.when(flag_ref[at] >= 0)(functools.partial(add_piece, arrays[at], False))
    if last:
        for h in range(2):
            columns = pl.ds(HEAD_DIM * h, HEAD_DIM)
            out_ref[columns, :] = out_ref[columns, :] / total_ref[0, h : h + 1, :]
        result_ref[...] = out_ref[...].T.astype(BF16)
        lse_ref[0] = high_ref[0] + jnp.log2(total_ref[0])


def forward_stage(queries, qmark, pieces, state, last):
    rows, width = queries.shape
    pairs = width // PAIR
    flags = jnp.stack([jnp.asarray(place, jnp.int32) for _, place, _ in pieces])
    args = [queries, qmark]
    in_specs = [
        pl.BlockSpec((rows, PAIR), lambda h, s: (0, h)),
        pl.BlockSpec((1, rows), lambda h, s: (0, 0)),
    ]
    keys = 0
    for kv, _, marks in pieces:
        count = kv.shape[0]
        keys += count
        args += [kv, kv]
        in_specs += [
            pl.BlockSpec((count, PAIR), lambda h, s: (0, h)),
            pl.BlockSpec((count, PAIR), lambda h, s: (0, pairs + h)),
        ]
        if marks is not None:
            args.append(marks)
            in_specs.append(pl.BlockSpec((count, 1), lambda h, s: (0, 0)))
    stat = jax.ShapeDtypeStruct((pairs, 2, rows), F32)
    stat_spec = pl.BlockSpec((1, 2, rows), lambda h, s: (h, 0, 0))
    state_specs = [stat_spec, stat_spec, pl.BlockSpec((PAIR, rows), lambda h, s: (h, 0))]
    state_shapes = [stat, stat, jax.ShapeDtypeStruct((width, rows), F32)]
    if state is not None:
        args += list(state)
        in_specs += state_specs
    if last:
        out_specs = [pl.BlockSpec((rows, PAIR), lambda h, s: (0, h)), stat_spec]
        out_shape = [jax.ShapeDtypeStruct((rows, width), BF16), stat]
        scratch = [
            pltpu.VMEM((1, 2, rows), F32),
            pltpu.VMEM((1, 2, rows), F32),
            pltpu.VMEM((PAIR, rows), F32),
        ]
    else:
        out_specs, out_shape, scratch = state_specs, state_shapes, []
    return pl.pallas_call(
        functools.partial(
            forward_kernel, [m is not None for _, _, m in pieces], state is None, last
        ),
        grid_spec=pltpu.PrefetchScalarGridSpec(
            num_scalar_prefetch=1,
            grid=(pairs,),
            in_specs=in_specs,
            out_specs=out_specs,
            scratch_shapes=scratch,
        ),
        out_shape=out_shape,
        compiler_params=pltpu.CompilerParams(vmem_limit_bytes=40 << 20),
        cost_estimate=pl.CostEstimate(
            flops=16 * rows * keys * width,
            bytes_accessed=8 * keys * width,
            transcendentals=rows * keys * width // HEAD_DIM,
        ),
    )(flags, *args)


def stats_kernel(rows, place_ref, mine_ref, other_ref, out_ref, lse_ref, sent_ref, stat_ref):
    half = mine_ref.shape[0]
    place = place_ref[0]
    sent_ref[pl.ds(pl.multiple_of(place * half, half), half), :] = mine_ref[...]
    sent_ref[pl.ds(pl.multiple_of((1 - place) * half, half), half), :] = other_ref[...]
    width = mine_ref.shape[1]
    heads = width // HEAD_DIM
    deltas = []
    for pair in range(width // PAIR):
        columns = pl.ds(pair * PAIR, PAIR)
        grad = sent_ref[pl.ds(0, rows), columns]
        terms = (grad.astype(F32) * out_ref[:, columns].astype(F32)).T
        deltas += [
            jnp.sum(terms[:HEAD_DIM], axis=0, keepdims=True),
            jnp.sum(terms[HEAD_DIM:], axis=0, keepdims=True),
        ]
    stat = jnp.concatenate(
        [lse_ref[pair] for pair in range(width // PAIR)] + deltas, axis=0
    )
    stat_ref[...] = stat
    for at in range(STAT_ROWS):
        piece = stat.astype(BF16)
        sent_ref[pl.ds(rows + at * 2 * heads, 2 * heads), :] = piece
        stat = stat - piece.astype(F32)


def pack_gradient(place, mine, other, attended, lse):
    rows, width = attended.shape
    stat_rows = 2 * width // HEAD_DIM
    return pl.pallas_call(
        functools.partial(stats_kernel, rows),
        in_specs=[pl.BlockSpec(memory_space=pltpu.SMEM)]
        + [pl.BlockSpec(memory_space=pltpu.VMEM)] * 4,
        out_specs=[pl.BlockSpec(memory_space=pltpu.VMEM)] * 2,
        out_shape=[
            jax.ShapeDtypeStruct((rows + STAT_ROWS * stat_rows, width), BF16),
            jax.ShapeDtypeStruct((stat_rows, rows), F32),
        ],
    )(place, mine, other, attended, lse)


def query_kernel(
    sizes, step_keys, first_pair, place_ref, q_ref, grad_ref, stat_ref, qmark_ref, kmark_ref, *refs
):
    count = len(sizes)
    pieces, out_ref, kv_ref, kt_ref, sems = refs[:count], *refs[count:]
    rows, length = q_ref.shape[0], kv_ref.shape[0]
    width = kv_ref.shape[1] // 2
    pair = pl.program_id(0)
    index = place_ref[0]
    full = (index * rows) // step_keys
    end = jnp.minimum(
        ((index + 1) * rows + BOUNDARY + step_keys - 1) // step_keys, length // step_keys
    )

    def copies(at):
        start = pl.multiple_of(place_ref[at] * rows, rows)
        whole = pieces[at].shape[1] // 2
        return [
            pltpu.make_async_copy(
                pieces[at].at[:, pl.ds(part * whole + first_pair * PAIR, width)],
                kv_ref.at[pl.ds(start, sizes[at]), pl.ds(part * width, width)],
                sems.at[2 * at + part],
            )
            for part in range(2)
        ]

    def each(act):
        for at in range(count):

            @pl.when(place_ref[at] >= 0)
            def _(at=at):
                for one in copies(at):
                    act(one)

    @pl.when(pair == 0)
    def _():
        each(lambda one: one.start())

        def clear(at, _):
            start = pl.multiple_of(at * BOUNDARY, BOUNDARY)
            kv_ref[pl.ds(start, BOUNDARY), :] = jnp.zeros((BOUNDARY, 2 * width), BF16)
            return 0

        ratio = rows // BOUNDARY
        lax.fori_loop((index + 1) * ratio + 1, end * (step_keys // BOUNDARY), clear, 0)
        each(lambda one: one.wait())

    queries, grads = split_heads(q_ref[...]), split_heads(grad_ref[...])
    k_columns = pl.ds(pl.multiple_of(pair * PAIR, PAIR), PAIR)
    v_columns = pl.ds(pl.multiple_of(width + pair * PAIR, PAIR), PAIR)
    head = 2 * (first_pair + pair)
    lse = [stat_ref[pl.ds(head + h, 1), :] for h in range(2)]
    delta = [stat_ref[pl.ds(stat_ref.shape[0] // 2 + head + h, 1), :] for h in range(2)]

    def turn(at, _):
        start = pl.multiple_of(at * step_keys, step_keys)
        kt_ref[:, pl.ds(start, step_keys)] = kv_ref[pl.ds(start, step_keys), k_columns].T
        return 0

    lax.fori_loop(0, end, turn, 0)

    def step(masked):
        def body(at, state):
            start = pl.multiple_of(at * step_keys, step_keys)
            keys = kv_ref[pl.ds(start, step_keys), k_columns]
            values = kv_ref[pl.ds(start, step_keys), v_columns]
            if masked:
                allowed = kmark_ref[pl.ds(start, step_keys), :] <= qmark_ref[...]
            new = []
            for h in range(2):
                score = nt(keys, queries[h])
                slope = nt(values, grads[h])
                prob = jnp.exp2(score - lse[h])
                if masked:
                    prob = jnp.where(allowed, prob, 0.0)
                grad = (prob * (slope - delta[h])).astype(BF16)
                turned = kt_ref[pl.ds(HEAD_DIM * h, HEAD_DIM), pl.ds(start, step_keys)]
                new.append(state[h] + nn(turned, grad))
            return tuple(new)

        return body

    empty = jnp.zeros((HEAD_DIM, rows), F32)
    state = lax.fori_loop(full, end, step(True), (empty, empty))
    state = lax.fori_loop(0, full, step(False), state)
    out_ref[...] = (jnp.concatenate(state, axis=0).T * HEAD_DIM ** (-0.5)).astype(out_ref.dtype)


def query_gradient(
    queries, sent, stat, pieces, qmark, kmark, first_pair, pairs, step_keys=1024
):
    rows, width = queries.shape[0], pairs * PAIR
    length = kmark.shape[0]
    places = jnp.stack([jnp.asarray(place, jnp.int32) for _, place in pieces])
    sizes = [kv.shape[0] for kv, _ in pieces]
    return pl.pallas_call(
        functools.partial(query_kernel, sizes, step_keys, first_pair),
        grid_spec=pltpu.PrefetchScalarGridSpec(
            num_scalar_prefetch=1,
            grid=(pairs,),
            in_specs=[
                pl.BlockSpec((rows, PAIR), lambda h, s: (0, first_pair + h)),
                pl.BlockSpec((rows, PAIR), lambda h, s: (0, first_pair + h)),
                pl.BlockSpec(stat.shape, lambda h, s: (0, 0)),
                pl.BlockSpec((1, rows), lambda h, s: (0, 0)),
                pl.BlockSpec((length, 1), lambda h, s: (0, 0)),
            ]
            + [pl.BlockSpec(memory_space=pl.ANY)] * len(pieces),
            out_specs=pl.BlockSpec((rows, PAIR), lambda h, s: (0, h)),
            scratch_shapes=[
                pltpu.VMEM((length, 2 * width), BF16),
                pltpu.VMEM((PAIR, length), BF16),
                pltpu.SemaphoreType.DMA((2 * len(pieces),)),
            ],
        ),
        out_shape=jax.ShapeDtypeStruct((rows, width), BF16),
        compiler_params=pltpu.CompilerParams(vmem_limit_bytes=56 << 20),
        cost_estimate=pl.CostEstimate(
            flops=rows * length * width,
            bytes_accessed=4 * length * width,
            transcendentals=rows * length * width // HEAD_DIM,
        ),
    )(places, queries, sent, stat, qmark, kmark, *[kv for kv, _ in pieces])


def key_kernel(
    sizes, step_queries, first_pair, place_ref, k_ref, v_ref, q_ref, qmark_ref, kmark_ref, *refs
):
    count = len(sizes)
    pieces = refs[:count]
    dk_ref, dv_ref, grad_ref, raw_ref, stat_ref, sems = refs[count:]
    rows, length = k_ref.shape[0], q_ref.shape[0]
    width = grad_ref.shape[1]
    stat_rows = stat_ref.shape[0]
    packed = STAT_ROWS * stat_rows
    pair = pl.program_id(0)
    index = place_ref[0]

    def copies(at):
        size = sizes[at]
        start = pl.multiple_of(place_ref[at] * rows + rows - size, BOUNDARY)
        return (
            pltpu.make_async_copy(
                pieces[at].at[pl.ds(0, size), pl.ds(first_pair * PAIR, width)],
                grad_ref.at[pl.ds(start, size), :],
                sems.at[2 * at],
            ),
            pltpu.make_async_copy(
                pieces[at].at[pl.ds(size, packed), :],
                raw_ref.at[at],
                sems.at[2 * at + 1],
            ),
        )

    @pl.when(pair == 0)
    def _():
        for at in range(count):

            @pl.when(place_ref[at] >= 0)
            def _(at=at):
                for one in copies(at):
                    one.start()

        @pl.when(index > 0)
        def _():
            start = pl.multiple_of((index - 1) * rows, rows)
            grad_ref[pl.ds(start, rows - BOUNDARY), :] = jnp.zeros(
                (rows - BOUNDARY, width), BF16
            )

        for at in range(count):

            @pl.when(place_ref[at] >= 0)
            def _(at=at):
                for one in copies(at):
                    one.wait()
                stat = raw_ref[at, :stat_rows].astype(F32)
                for part in range(1, STAT_ROWS):
                    stat = stat + raw_ref[
                        at, part * stat_rows : (part + 1) * stat_rows
                    ].astype(F32)
                start = pl.multiple_of(place_ref[at] * rows, rows)
                stat_ref[:, pl.ds(start, rows)] = stat

    keys, values = split_heads(k_ref[...]), split_heads(v_ref[...])
    columns = pl.ds(pl.multiple_of(pair * PAIR, PAIR), PAIR)
    head = 2 * (first_pair + pair)

    def step(masked):
        def body(at, state):
            start = pl.multiple_of(at * step_queries, step_queries)
            span = pl.ds(start, step_queries)
            queries = q_ref[span, :]
            grads = grad_ref[span, columns]
            if masked:
                allowed = kmark_ref[...] <= qmark_ref[:, span]
            new = []
            for h in range(2):
                lse = stat_ref[pl.ds(head + h, 1), span]
                delta = stat_ref[pl.ds(stat_rows // 2 + head + h, 1), span]
                score = nt(keys[h], queries)
                slope = nt(values[h], grads)
                prob = jnp.exp2(score - lse)
                if masked:
                    prob = jnp.where(allowed, prob, 0.0)
                grad = prob * (slope - delta)
                new += [
                    state[2 * h] + nn(grad.astype(BF16), queries),
                    state[2 * h + 1] + nn(prob.astype(BF16), grads),
                ]
            return tuple(new)

        return body

    empty = jnp.zeros((rows, PAIR), F32)
    first = jnp.maximum((index * rows - BOUNDARY) // step_queries, 0)
    own = ((index + 1) * rows + step_queries - 1) // step_queries
    state = lax.fori_loop(first, own, step(True), (empty,) * 4)
    state = lax.fori_loop(own, length // step_queries, step(False), state)
    lane = lax.broadcasted_iota(jnp.int32, (1, PAIR), 1)
    dk_ref[...] = (jnp.where(lane < HEAD_DIM, state[0], state[2]) * LN2).astype(dk_ref.dtype)
    dv_ref[...] = (0.5 * jnp.where(lane < HEAD_DIM, state[1], state[3])).astype(dv_ref.dtype)


def key_gradient(kv, q_all, pieces, qmark, kmark, first_pair, pairs, step_queries=512):
    rows = kv.shape[0]
    length, whole = q_all.shape
    width = pairs * PAIR
    stat_rows = 2 * whole // HEAD_DIM
    values_at = whole // PAIR + first_pair
    packed = STAT_ROWS * stat_rows
    places = jnp.stack([jnp.asarray(place, jnp.int32) for _, place in pieces])
    sizes = [sent.shape[0] - packed for sent, _ in pieces]
    return pl.pallas_call(
        functools.partial(key_kernel, sizes, step_queries, first_pair),
        grid_spec=pltpu.PrefetchScalarGridSpec(
            num_scalar_prefetch=1,
            grid=(pairs,),
            in_specs=[
                pl.BlockSpec((rows, PAIR), lambda h, s: (0, first_pair + h)),
                pl.BlockSpec((rows, PAIR), lambda h, s: (0, values_at + h)),
                pl.BlockSpec((length, PAIR), lambda h, s: (0, first_pair + h)),
                pl.BlockSpec((1, length), lambda h, s: (0, 0)),
                pl.BlockSpec((rows, 1), lambda h, s: (0, 0)),
            ]
            + [pl.BlockSpec(memory_space=pl.ANY)] * len(pieces),
            out_specs=[pl.BlockSpec((rows, PAIR), lambda h, s: (0, h))] * 2,
            scratch_shapes=[
                pltpu.VMEM((length, width), BF16),
                pltpu.VMEM((len(pieces), packed, rows), BF16),
                pltpu.VMEM((stat_rows, length), F32),
                pltpu.SemaphoreType.DMA((2 * len(pieces),)),
            ],
        ),
        out_shape=[jax.ShapeDtypeStruct((rows, width), BF16)] * 2,
        compiler_params=pltpu.CompilerParams(vmem_limit_bytes=56 << 20),
        cost_estimate=pl.CostEstimate(
            flops=rows * length * width,
            bytes_accessed=4 * length * width,
            transcendentals=rows * length * width // HEAD_DIM,
        ),
    )(places, kv, kv, q_all, qmark, kmark, *[sent for sent, _ in pieces])


def on_device(
    tokens,
    value_first,
    teacher,
    valid,
    blocks,
    gain_attn,
    gain_ffn,
    w_query,
    w_key,
    w_value,
    w_out,
    w_gate,
    w_up,
    w_down,
):
    width = tokens.shape[2]
    own_rows = tokens.shape[1]
    sizes = {axis: lax.axis_size(axis) for axis in ("shard", CTX, "tp")}
    shard, ctx, tp = (lax.axis_index(axis) for axis in ("shard", CTX, "tp"))
    group_rows = own_rows * sizes["tp"]
    half = w_query.shape[1]
    part = w_query.shape[0]
    line = sizes[CTX] // 2

    def flip(values, axis, bit=1):
        return lax.ppermute(values, axis, [(i, i ^ bit) for i in range(lax.axis_size(axis))])

    def tree_sum(values):
        for axis, size in sizes.items():
            bit = 1
            while bit < size:
                values = values + flip(values, axis, bit)
                bit *= 2
        return values

    def in_order(position, mine, other, axis):
        first = position == 0
        return jnp.concatenate(
            [jnp.where(first, mine, other), jnp.where(first, other, mine)], axis=axis
        )

    def shard_blocks(values):
        if sizes["shard"] == 2:
            return [values, flip(values, "shard")]
        gathered = lax.all_gather(values, "shard", axis=0, tiled=False)
        return [gathered[i] for i in range(sizes["shard"])]

    def block_of(values, at):
        if sizes["shard"] == 2:
            return cols_of(values, shard if at == 0 else 1 - shard, part)
        return values[:, at * part : (at + 1) * part]

    def join_blocks(terms):
        if sizes["shard"] == 2:
            return in_order(shard, terms[0], terms[1], 1)
        return jnp.concatenate(terms, axis=1)

    def times_blocks(lefts, blocks_of):
        return join_blocks(
            [
                sum(nn(left, blocks[at]) for left, blocks in zip(lefts, blocks_of))
                for at in range(sizes["shard"])
            ]
        )

    def times_turned(left, blocks):
        return sum(nt(block_of(left, at), block) for at, block in enumerate(blocks))

    def times_rows(left, blocks):
        return sum(nn(block_of(left, at), block) for at, block in enumerate(blocks))

    def times_rows_turned(lefts, blocks_of):
        return join_blocks(
            [
                sum(nt(left, blocks[at]) for left, blocks in zip(lefts, blocks_of))
                for at in range(sizes["shard"])
            ]
        )

    def ctx_bits():
        bit = 1
        while bit < sizes[CTX]:
            yield bit
            bit *= 2

    def reduce_ctx(parts, orders, between):
        parts, steps = list(parts), len(orders[0])
        for step in range(steps):
            for at, order in enumerate(orders):
                size = parts[at].shape[0] // 2
                side = (ctx // order[step]) % 2
                kept = lax.dynamic_slice_in_dim(parts[at], side * size, size, 0)
                sent = lax.dynamic_slice_in_dim(parts[at], (1 - side) * size, size, 0)
                got = flip(sent, CTX, order[step])
                parts[at] = (kept.astype(F32) + got.astype(F32)).astype(BF16)
            parts = between(step, parts)
        for step in reversed(range(steps)):
            for at, order in enumerate(orders):
                side = (ctx // order[step]) % 2
                parts[at] = in_order(side, parts[at], flip(parts[at], CTX, order[step]), 0)
            parts = between(2 * steps - 1 - step, parts)
        return parts

    def rows_of(values, position):
        return lax.dynamic_slice_in_dim(values, position * own_rows, own_rows, 0)

    def cols_of(values, position, size):
        return lax.dynamic_slice_in_dim(values, position * size, size, 1)

    level, column = ctx // 2, ctx % 2

    def spread(own, step, edge, between):
        if line != 4:
            gathered = lax.all_gather(own, CTX, axis=0, tiled=False)
            below = [(place < ctx) if step == 1 else (place > ctx) for place in range(2 * line)]
            pieces = [
                (gathered[place], jnp.where(below[place], place, -1)) for place in range(2 * line)
            ]
            beside = jnp.clip(ctx + step, 0, 2 * line - 1)
            rows = lax.dynamic_index_in_dim(gathered, beside, 0, keepdims=False)[edge]
            gathered, rows = between(0, [pieces[0][0], rows])
            pieces[0] = (gathered, pieces[0][1])
            stages = [pieces[:2]]
            for i in range(2, 2 * line, 2):
                (first,) = between(i // 2, [pieces[i][0]])
                stages.append([(first, pieces[i][1]), pieces[i + 1]])
            return stages, rows
        inside = range(2 * line)
        along = [(i, i + 2 * step) for i in inside if i + 2 * step in inside]
        near = 1 if step == 1 else 0
        against = [(i, i - 2 * step) for i in inside if i % 2 == near and i - 2 * step in inside]

        def place(hop, aside):
            there = level - step * hop
            at = 2 * there + ((1 - column) if aside else column)
            return jnp.where((there >= 0) & (there < line), at, -1)

        across, moving = between(0, [flip(own, CTX), lax.ppermute(own, CTX, along)])
        stages = [[(across, jnp.where(column == near, ctx - step, -1)), (moving, place(1, False))]]
        beside = lax.ppermute(across[edge], CTX, against)
        beside_here = across[edge]
        across, moving, beside = between(
            1, [flip(moving, CTX), lax.ppermute(moving, CTX, along), beside]
        )
        rows = jnp.where(column == near, beside, beside_here)
        stages.append([(across, place(1, True)), (moving, place(2, False))])
        across, moving = between(2, [flip(moving, CTX), lax.ppermute(moving, CTX, along)])
        stages.append([(across, place(2, True)), (moving, place(3, False))])
        cut = own.shape[0] // 32 * 16
        last = between(
            3, [flip(moving[:cut], CTX), lax.ppermute(across[cut:], CTX, along)]
        )
        stages.append([(jnp.concatenate(last, axis=0), place(3, True))])
        return stages, rows

    def shard_reduce(term, slice_rows):
        if sizes["shard"] == 2:
            return term(shard) + flip(term(1 - shard).astype(BF16), "shard").astype(F32)
        whole = jnp.concatenate(
            [term(i) for i in range(sizes["shard"])], axis=0 if slice_rows else 1
        )
        return lax.psum_scatter(
            whole.astype(BF16), "shard", scatter_dimension=0 if slice_rows else 1, tiled=True
        ).astype(F32)

    def over_rows(lefts, rights, slice_left):
        def term(position):
            if slice_left:
                return sum(tn(cols_of(a, position, part), b) for a, b in zip(lefts, rights))
            return sum(tn(a, cols_of(b, position, part)) for a, b in zip(lefts, rights))

        return shard_reduce(term, slice_left).astype(BF16)

    mine = tokens.reshape(own_rows, width)
    first_own = value_first.reshape(own_rows, width)
    key_marks = blocks.reshape(-1)
    padded_marks = jnp.concatenate([key_marks, jnp.full((BOUNDARY,), 1 << 30, key_marks.dtype)])
    query_marks = lax.dynamic_slice_in_dim(key_marks, ctx * group_rows, group_rows, 0)
    next_marks = lax.dynamic_slice_in_dim(padded_marks, (ctx + 1) * group_rows, BOUNDARY, 0)
    keep = valid.reshape(own_rows).astype(F32)

    theirs = flip(mine, "tp")
    first_theirs = flip(cols_of(first_own, 1 - tp, half), "tp")
    weight_qkv = shard_blocks(jnp.concatenate([w_query, w_key, w_value], axis=1))
    count = tree_sum(jnp.broadcast_to(jnp.sum(keep), (1, 128)))[0, 0]

    group = in_order(tp, mine, theirs, 0).astype(F32)
    normed_one = rms_norm(group, gain_attn).astype(BF16)
    first_group = in_order(tp, cols_of(first_own, tp, half), first_theirs, 0).astype(F32)
    qkv = times_rows(normed_one, weight_qkv)
    queries = (qkv[:, :half] * QUERY_SCALE).astype(BF16)
    kv = jnp.concatenate(
        [qkv[:, half : 2 * half], 0.5 * qkv[:, 2 * half :] + 0.5 * first_group], axis=1
    ).astype(BF16)

    kv, w_gate, w_up, w_down, w_out, count = lax.optimization_barrier(
        (kv, w_gate, w_up, w_down, w_out, count)
    )
    gathered = {
        "gate": shard_blocks(w_gate),
        "up": shard_blocks(w_up),
        "down": shard_blocks(w_down),
        "outs": [shard_blocks(w_out), shard_blocks(flip(w_out, "tp"))],
    }

    qmark, kmark = query_marks.reshape(1, -1), key_marks.reshape(-1, 1)
    forward = {"state": None, "pieces": [(kv, 0, query_marks.reshape(-1, 1))]}

    def advance(last):
        forward["state"] = forward_stage(
            queries, qmark, forward["pieces"], forward["state"], last
        )
        forward["pieces"] = []

    def forward_between(at, arrays):
        advance(False)
        *arrays, out = lax.optimization_barrier((*arrays, forward["state"][2]))
        forward["state"] = (*forward["state"][:2], out)
        if line != 4:
            return arrays
        here = (column == 1) if at == 0 else (level >= at)
        if at == 3:
            forward["pieces"] = [(jnp.concatenate(arrays, axis=0), jnp.where(here, 0, -1), None)]
            return arrays
        forward["pieces"] = [
            (arrays[0], jnp.where(here, 0, -1), None),
            (arrays[1], jnp.where(level > at, 0, -1), None),
        ]
        if at == 0:
            forward["beside"] = arrays[0][:BOUNDARY]
        if at == 1:
            rows = jnp.where(column == 1, arrays[2], forward["beside"])
            forward["pieces"].insert(0, (rows, 0, next_marks.reshape(-1, 1)))
        return arrays

    if line == 4:
        stages, kv_next = spread(kv, 1, slice(0, BOUNDARY), forward_between)
        advance(True)
    else:
        stages, kv_next = spread(kv, 1, slice(0, BOUNDARY), lambda at, arrays: arrays)
        forward["pieces"].append((kv_next, 0, next_marks.reshape(-1, 1)))
        for at, stage in enumerate(stages):
            advance(False)
            forward["pieces"] = [(piece, place, None) for piece, place in stage]
        advance(True)
    attended, lse = forward["state"]

    outs, gate_weight = gathered["outs"], gathered["gate"]
    up_weight, down_weight = gathered["up"], gathered["down"]
    attended, q_own = lax.optimization_barrier((attended, queries))
    q_pair = in_order(column, q_own, flip(q_own, "side"), 0)
    q_all = lax.all_gather(q_pair, "line", axis=0, tiled=True)
    att = [rows_of(attended, tp), flip(rows_of(attended, 1 - tp), "tp")]
    inputs = mine.astype(F32)
    hidden = inputs + times_blocks(att, outs)
    normed_two = rms_norm(hidden, gain_ffn).astype(BF16)
    normed = [normed_two, flip(normed_two, "tp")]
    gate, up, logistic, act = [], [], [], []

    def widen(rows):
        gate.append(times_rows(rows, gate_weight))
        up.append(times_rows(rows, up_weight))
        logistic.append(jax.nn.sigmoid(gate[-1]))
        act.append((gate[-1] * logistic[-1] * up[-1]).astype(BF16))

    widen(normed[0])
    normed[1], act[0] = lax.optimization_barrier((normed[1], act[0]))
    widen(normed[1])
    down_theirs = flip(times_blocks([act[1]], [down_weight]).astype(BF16), "tp")
    down_theirs, q_pair = lax.optimization_barrier((down_theirs, q_pair))
    final = hidden + (times_blocks([act[0]], [down_weight]) + down_theirs.astype(F32))
    difference = final - teacher.reshape(own_rows, width).astype(F32)
    local_error = jnp.sum(jnp.mean(difference * difference, axis=1) * keep)
    token_total = group_rows * sizes[CTX] * sizes["shard"]
    grad_final = token_total / count * keep[:, None] * difference
    grad_round = grad_final.astype(BF16)
    rounds = [grad_round, flip(grad_round, "tp")]
    grad_gate, grad_up = [], []

    def back(at):
        grad_act = times_turned(rounds[at], down_weight)
        part = grad_act * logistic[at]
        grad_gate.append((part * up[at] * (1.0 + gate[at] * (1.0 - logistic[at]))).astype(BF16))
        grad_up.append((part * gate[at]).astype(BF16))

    back(0)
    rounds[1], grad_gate[0], grad_up[0] = lax.optimization_barrier(
        (rounds[1], grad_gate[0], grad_up[0])
    )
    back(1)
    both_weights = [gate_weight, up_weight]
    two_sent = times_rows_turned([grad_gate[1], grad_up[1]], both_weights).astype(BF16)
    two_theirs = flip(two_sent, "tp")
    gate_part = over_rows(normed, grad_gate, True)
    up_part = over_rows(normed, grad_up, True)
    down_part = over_rows(rounds, act, True)
    two_own = times_rows_turned([grad_gate[0], grad_up[0]], both_weights)
    two_theirs, two_own, gate_part, up_part, down_part = lax.optimization_barrier(
        (two_theirs, two_own, gate_part, up_part, down_part)
    )
    ffn_part = jnp.concatenate([gate_part, up_part, down_part], axis=1)
    grad_two = two_own + two_theirs.astype(F32)
    hidden_part, gain_ffn_term = jax.vjp(rms_norm, hidden, gain_ffn)[1](grad_two)
    grad_hidden = grad_final + hidden_part
    hidden_round = grad_hidden.astype(BF16)
    grad_att = [times_turned(hidden_round, w).astype(BF16) for w in outs]
    grad_theirs = flip(grad_att[1], "tp")
    sent, stat = pack_gradient(
        tp.reshape(1).astype(jnp.int32), grad_att[0], grad_theirs, attended, lse
    )

    hidden_two = flip(hidden_round, "tp")

    kv_pieces = [(kv, ctx), (kv_next, jnp.where(ctx + 1 < 2 * line, ctx + 1, -1))]
    kv_pieces += [piece for stage in stages for piece in stage]
    parts = {}

    pairs = half // PAIR
    quarters = max(pairs // 4, 1)

    def query_part(at):
        first = at * quarters
        count = quarters if at < 3 else pairs - first
        return query_gradient(
            queries, sent, parts["stat"], kv_pieces, qmark, kmark, first, count
        )

    def grad_between(at, arrays):
        if at == 0:
            parts["stat"], parts["q_all"], parts["hidden_two"] = stat, q_all, hidden_two
        if at > 3:
            return arrays
        name = "query" + str(at)
        parts[name] = query_part(at)
        hold = [name, "stat"]
        if at == 0:
            hold += ["q_all", "hidden_two"]
        if at == 3:
            parts["ffn"] = ffn_part
            hold.append("ffn")
        arrays, held = lax.optimization_barrier((arrays, [parts[name] for name in hold]))
        parts.update(zip(hold, held))
        return arrays

    grad_stages, sent_before = spread(
        sent, -1, slice(group_rows - BOUNDARY, None), grad_between
    )
    scattered = lax.psum_scatter(parts["ffn"], CTX, scatter_dimension=0, tiled=True)
    query_grad = jnp.concatenate([parts["query" + str(at)] for at in range(4)], axis=1)
    grad_pieces = [(sent, ctx), (sent_before, ctx - 1)]
    grad_pieces += [piece for stage in grad_stages for piece in stage]
    marks = (key_marks.reshape(1, -1), query_marks.reshape(-1, 1))
    key_grad, value_half = key_gradient(kv, parts["q_all"], grad_pieces, *marks, 0, pairs)
    key_grad, normed_held, parts["hidden_two"] = lax.optimization_barrier(
        (key_grad, normed_one, parts["hidden_two"])
    )
    early_part = jnp.concatenate(
        [
            over_rows([normed_held], [query_grad], True),
            over_rows(
                [hidden_round, parts["hidden_two"]],
                [rows_of(attended, tp), rows_of(attended, 1 - tp)],
                True,
            ),
        ],
        axis=1,
    )
    grads = jnp.concatenate([query_grad, key_grad, value_half], axis=1)
    kv_part = over_rows([normed_one], [grads[:, half:]], True)
    last = {}
    hidden_half = w_gate.shape[1]

    def finish(step, parts):
        if step == 0:
            parts, held, ready = lax.optimization_barrier((parts, grads, scattered))
            last["spread"] = lax.all_gather(ready, CTX, axis=0, tiled=True)
            theirs = times_rows_turned([rows_of(held, 1 - tp)], [weight_qkv]).astype(BF16)
            theirs = flip(theirs, "tp")
            last["own"] = times_rows_turned([rows_of(held, tp)], [weight_qkv])
            last["theirs"] = theirs
            last["value"] = flip(rows_of(held[:, 2 * half :], 1 - tp), "tp")
        if step == 1:
            *parts, last["own"], last["theirs"], last["value"] = lax.optimization_barrier(
                (*parts, last["own"], last["theirs"], last["value"])
            )
        if step == len(bits) + 1:
            parts, spread_out = lax.optimization_barrier((parts, last["spread"]))
            last["grads"] = [
                spread_out[:, at * hidden_half : (at + 1) * hidden_half].astype(F32)
                for at in range(3)
            ]
        return parts

    bits = list(ctx_bits())
    early, late = reduce_ctx([early_part, kv_part], [bits, bits[1:] + bits[:1]], finish)
    early, late = early.astype(F32), late.astype(F32)
    w_gate_grad, w_up_grad, w_down_grad = last["grads"]
    grad_one = last["own"] + last["theirs"].astype(F32)
    input_part, gain_attn_term = jax.vjp(rms_norm, inputs, gain_attn)[1](grad_one)
    tokens_grad = grad_hidden + input_part
    first_grad = in_order(tp, rows_of(value_half, tp), last["value"], 1).astype(F32)

    small = jnp.concatenate(
        [gain_attn_term, gain_ffn_term, jnp.broadcast_to(local_error, (128,))]
    )
    small = tree_sum(small.reshape(1, -1)).reshape(-1)
    return (
        final.astype(BF16).reshape(1, own_rows, width),
        small[2 * width] / count,
        tokens_grad.reshape(1, own_rows, width),
        first_grad.reshape(1, own_rows, width),
        small[:width],
        small[width : 2 * width],
        early[:, :half],
        late[:, :half],
        late[:, half:],
        early[:, half:].T,
        w_gate_grad,
        w_up_grad,
        w_down_grad.T,
    )


def solution(mesh):
    places = dict(mesh.shape)
    devices = mesh.devices.reshape(places["shard"], places["ctx"] // 2, 2, places["tp"])
    rows = P("shard", (*CTX, "tp"), None)
    wide, tall = P("shard", "tp"), P("tp", "shard")
    return jax.shard_map(
        on_device,
        mesh=jax.sharding.Mesh(devices, ("shard", *CTX, "tp")),
        in_specs=(
            rows,
            rows,
            rows,
            P("shard", (*CTX, "tp")),
            P("shard", None),
            P(),
            P(),
            wide,
            wide,
            wide,
            tall,
            wide,
            wide,
            tall,
        ),
        out_specs=(rows, P(), rows, rows, P(), P(), wide, wide, wide, tall, wide, wide, tall),
        check_vma=False,
    )
```

```python
import functools

import jax
import jax.numpy as jnp
from jax import lax
from jax.experimental import pallas as pl
from jax.experimental.pallas import tpu as pltpu
from jax.sharding import PartitionSpec as P

HEAD_DIM = 64
PAIR = 2 * HEAD_DIM
LN2 = 0.6931471805599453
QUERY_SCALE = HEAD_DIM ** (-0.5) / LN2
F32 = jnp.float32
BF16 = jnp.bfloat16
BOUNDARY = 256
STAT_ROWS = 3
KEY_STEP = 1024

CTX = ("line", "side")

epsilon = 1e-06


def rms_norm(values, gain):
    return values * lax.rsqrt(jnp.mean(values * values, axis=-1, keepdims=True) + epsilon) * gain


def dot(left, right, left_dim, right_dim):
    return lax.dot_general(
        left, right, (((left_dim,), (right_dim,)), ((), ())), preferred_element_type=F32
    )


def nn(left, right):
    return dot(left, right, 1, 0)


def nt(left, right):
    return dot(left, right, 1, 1)


def tn(left, right):
    return dot(left, right, 0, 0)


def split_heads(pair):
    lane = lax.broadcasted_iota(jnp.int32, (1, PAIR), 1)
    zero = jnp.zeros_like(pair)
    return [jnp.where(lane < HEAD_DIM, pair, zero), jnp.where(lane >= HEAD_DIM, pair, zero)]


def forward_kernel(pieces, first, last, flag_ref, q_ref, *refs):
    refs = list(refs)
    qmark_ref = refs.pop(0)
    arrays = []
    for masked in pieces:
        count = 3 if masked else 2
        arrays.append(refs[:count])
        refs = refs[count:]
    if not first:
        old_high, old_total, old_out = refs[:3]
        refs = refs[3:]
    if last:
        result_ref, lse_ref = refs[:2]
        refs = refs[2:]
    high_ref, total_ref, out_ref = refs
    rows = q_ref.shape[0]
    if first:
        high_ref[0] = jnp.full((2, rows), -1e30, F32)
        total_ref[0] = jnp.zeros((2, rows), F32)
        out_ref[...] = jnp.zeros((PAIR, rows), F32)
    else:
        high_ref[0] = old_high[0]
        total_ref[0] = old_total[0]
        out_ref[...] = old_out[...]
    queries = split_heads(q_ref[...])

    def add_piece(piece, masked):
        keys = piece[0][...]
        turned = piece[1][...].T
        scores = [nt(keys, queries[h]) for h in range(2)]
        if masked:
            allowed = piece[2][...] <= qmark_ref[...]
        for h in range(2):
            score = scores[h]
            if masked:
                score = jnp.where(allowed, score, -1e30)
            highest = high_ref[0, h : h + 1, :]
            top = jnp.maximum(highest, jnp.max(score, axis=0, keepdims=True))
            power = jnp.exp2(score - top)
            shrink = jnp.exp2(highest - top)
            high_ref[0, h : h + 1, :] = top
            total_ref[0, h : h + 1, :] = total_ref[0, h : h + 1, :] * shrink + jnp.sum(
                power, axis=0, keepdims=True
            )
            columns = pl.ds(HEAD_DIM * h, HEAD_DIM)
            out_ref[columns, :] = out_ref[columns, :] * shrink + nn(
                turned[HEAD_DIM * h : HEAD_DIM * (h + 1)], power.astype(BF16)
            )

    for at, masked in enumerate(pieces):
        if masked:
            add_piece(arrays[at], True)
        else:
            pl.when(flag_ref[at] >= 0)(functools.partial(add_piece, arrays[at], False))
    if last:
        for h in range(2):
            columns = pl.ds(HEAD_DIM * h, HEAD_DIM)
            out_ref[columns, :] = out_ref[columns, :] / total_ref[0, h : h + 1, :]
        result_ref[...] = out_ref[...].T.astype(BF16)
        lse_ref[0] = high_ref[0] + jnp.log2(total_ref[0])


def forward_stage(queries, qmark, pieces, state, last):
    rows, width = queries.shape
    pairs = width // PAIR
    flags = jnp.stack([jnp.asarray(place, jnp.int32) for _, place, _ in pieces])
    args = [queries, qmark]
    in_specs = [
        pl.BlockSpec((rows, PAIR), lambda h, s: (0, h)),
        pl.BlockSpec((1, rows), lambda h, s: (0, 0)),
    ]
    keys = 0
    for kv, _, marks in pieces:
        count = kv.shape[0]
        keys += count
        args += [kv, kv]
        in_specs += [
            pl.BlockSpec((count, PAIR), lambda h, s: (0, h)),
            pl.BlockSpec((count, PAIR), lambda h, s: (0, pairs + h)),
        ]
        if marks is not None:
            args.append(marks)
            in_specs.append(pl.BlockSpec((count, 1), lambda h, s: (0, 0)))
    stat = jax.ShapeDtypeStruct((pairs, 2, rows), F32)
    stat_spec = pl.BlockSpec((1, 2, rows), lambda h, s: (h, 0, 0))
    state_specs = [stat_spec, stat_spec, pl.BlockSpec((PAIR, rows), lambda h, s: (h, 0))]
    state_shapes = [stat, stat, jax.ShapeDtypeStruct((width, rows), F32)]
    if state is not None:
        args += list(state)
        in_specs += state_specs
    if last:
        out_specs = [pl.BlockSpec((rows, PAIR), lambda h, s: (0, h)), stat_spec]
        out_shape = [jax.ShapeDtypeStruct((rows, width), BF16), stat]
        scratch = [
            pltpu.VMEM((1, 2, rows), F32),
            pltpu.VMEM((1, 2, rows), F32),
            pltpu.VMEM((PAIR, rows), F32),
        ]
    else:
        out_specs, out_shape, scratch = state_specs, state_shapes, []
    return pl.pallas_call(
        functools.partial(
            forward_kernel, [m is not None for _, _, m in pieces], state is None, last
        ),
        grid_spec=pltpu.PrefetchScalarGridSpec(
            num_scalar_prefetch=1,
            grid=(pairs,),
            in_specs=in_specs,
            out_specs=out_specs,
            scratch_shapes=scratch,
        ),
        out_shape=out_shape,
        compiler_params=pltpu.CompilerParams(vmem_limit_bytes=40 << 20),
        cost_estimate=pl.CostEstimate(
            flops=16 * rows * keys * width,
            bytes_accessed=8 * keys * width,
            transcendentals=rows * keys * width // HEAD_DIM,
        ),
    )(flags, *args)


def stats_kernel(rows, place_ref, mine_ref, other_ref, out_ref, lse_ref, sent_ref, stat_ref):
    half = mine_ref.shape[0]
    place = place_ref[0]
    sent_ref[pl.ds(pl.multiple_of(place * half, half), half), :] = mine_ref[...]
    sent_ref[pl.ds(pl.multiple_of((1 - place) * half, half), half), :] = other_ref[...]
    width = mine_ref.shape[1]
    heads = width // HEAD_DIM
    deltas = []
    for pair in range(width // PAIR):
        columns = pl.ds(pair * PAIR, PAIR)
        grad = sent_ref[pl.ds(0, rows), columns]
        terms = (grad.astype(F32) * out_ref[:, columns].astype(F32)).T
        deltas += [
            jnp.sum(terms[:HEAD_DIM], axis=0, keepdims=True),
            jnp.sum(terms[HEAD_DIM:], axis=0, keepdims=True),
        ]
    stat = jnp.concatenate(
        [lse_ref[pair] for pair in range(width // PAIR)] + deltas, axis=0
    )
    stat_ref[...] = stat
    for at in range(STAT_ROWS):
        piece = stat.astype(BF16)
        sent_ref[pl.ds(rows + at * 2 * heads, 2 * heads), :] = piece
        stat = stat - piece.astype(F32)


def pack_gradient(place, mine, other, attended, lse):
    rows, width = attended.shape
    stat_rows = 2 * width // HEAD_DIM
    return pl.pallas_call(
        functools.partial(stats_kernel, rows),
        in_specs=[pl.BlockSpec(memory_space=pltpu.SMEM)]
        + [pl.BlockSpec(memory_space=pltpu.VMEM)] * 4,
        out_specs=[pl.BlockSpec(memory_space=pltpu.VMEM)] * 2,
        out_shape=[
            jax.ShapeDtypeStruct((rows + STAT_ROWS * stat_rows, width), BF16),
            jax.ShapeDtypeStruct((stat_rows, rows), F32),
        ],
    )(place, mine, other, attended, lse)


def query_kernel(
    sizes, step_keys, first_pair, place_ref, q_ref, grad_ref, stat_ref, qmark_ref, kmark_ref, *refs
):
    count = len(sizes)
    pieces, out_ref, kv_ref, kt_ref, sems = refs[:count], *refs[count:]
    rows, length = q_ref.shape[0], kv_ref.shape[0]
    width = kv_ref.shape[1] // 2
    pair = pl.program_id(0)
    index = place_ref[0]
    full = (index * rows) // step_keys
    end = jnp.minimum(
        ((index + 1) * rows + BOUNDARY + step_keys - 1) // step_keys, length // step_keys
    )

    def copies(at):
        start = pl.multiple_of(place_ref[at] * rows, rows)
        whole = pieces[at].shape[1] // 2
        return [
            pltpu.make_async_copy(
                pieces[at].at[:, pl.ds(part * whole + first_pair * PAIR, width)],
                kv_ref.at[pl.ds(start, sizes[at]), pl.ds(part * width, width)],
                sems.at[2 * at + part],
            )
            for part in range(2)
        ]

    def each(act):
        for at in range(count):

            @pl.when(place_ref[at] >= 0)
            def _(at=at):
                for one in copies(at):
                    act(one)

    @pl.when(pair == 0)
    def _():
        each(lambda one: one.start())

        def clear(at, _):
            start = pl.multiple_of(at * BOUNDARY, BOUNDARY)
            kv_ref[pl.ds(start, BOUNDARY), :] = jnp.zeros((BOUNDARY, 2 * width), BF16)
            return 0

        ratio = rows // BOUNDARY
        lax.fori_loop((index + 1) * ratio + 1, end * (step_keys // BOUNDARY), clear, 0)
        each(lambda one: one.wait())

    queries, grads = split_heads(q_ref[...]), split_heads(grad_ref[...])
    k_columns = pl.ds(pl.multiple_of(pair * PAIR, PAIR), PAIR)
    v_columns = pl.ds(pl.multiple_of(width + pair * PAIR, PAIR), PAIR)
    head = 2 * (first_pair + pair)
    lse = [stat_ref[pl.ds(head + h, 1), :] for h in range(2)]
    delta = [stat_ref[pl.ds(stat_ref.shape[0] // 2 + head + h, 1), :] for h in range(2)]

    def turn(at, _):
        start = pl.multiple_of(at * step_keys, step_keys)
        kt_ref[:, pl.ds(start, step_keys)] = kv_ref[pl.ds(start, step_keys), k_columns].T
        return 0

    lax.fori_loop(0, end, turn, 0)

    def step(masked):
        def body(at, state):
            start = pl.multiple_of(at * step_keys, step_keys)
            keys = kv_ref[pl.ds(start, step_keys), k_columns]
            values = kv_ref[pl.ds(start, step_keys), v_columns]
            if masked:
                window = pl.multiple_of((at - full) * step_keys, step_keys)
                allowed = kmark_ref[pl.ds(window, step_keys), :] <= qmark_ref[...]
            new = []
            for h in range(2):
                score = nt(keys, queries[h])
                slope = nt(values, grads[h])
                prob = jnp.exp2(score - lse[h])
                if masked:
                    prob = jnp.where(allowed, prob, 0.0)
                grad = (prob * (slope - delta[h])).astype(BF16)
                turned = kt_ref[pl.ds(HEAD_DIM * h, HEAD_DIM), pl.ds(start, step_keys)]
                new.append(state[h] + nn(turned, grad))
            return tuple(new)

        return body

    empty = jnp.zeros((HEAD_DIM, rows), F32)
    state = lax.fori_loop(full, end, step(True), (empty, empty))
    state = lax.fori_loop(0, full, step(False), state)
    out_ref[...] = (jnp.concatenate(state, axis=0).T * HEAD_DIM ** (-0.5)).astype(out_ref.dtype)


def query_gradient(
    queries, sent, stat, pieces, qmark, kmark, length, first_pair, pairs, step_keys=KEY_STEP
):
    rows, width = queries.shape[0], pairs * PAIR
    places = jnp.stack([jnp.asarray(place, jnp.int32) for _, place in pieces])
    sizes = [kv.shape[0] for kv, _ in pieces]
    return pl.pallas_call(
        functools.partial(query_kernel, sizes, step_keys, first_pair),
        grid_spec=pltpu.PrefetchScalarGridSpec(
            num_scalar_prefetch=1,
            grid=(pairs,),
            in_specs=[
                pl.BlockSpec((rows, PAIR), lambda h, s: (0, first_pair + h)),
                pl.BlockSpec((rows, PAIR), lambda h, s: (0, first_pair + h)),
                pl.BlockSpec(stat.shape, lambda h, s: (0, 0)),
                pl.BlockSpec((1, rows), lambda h, s: (0, 0)),
                pl.BlockSpec((2 * step_keys, 1), lambda h, s: (0, 0)),
            ]
            + [pl.BlockSpec(memory_space=pl.ANY)] * len(pieces),
            out_specs=pl.BlockSpec((rows, PAIR), lambda h, s: (0, h)),
            scratch_shapes=[
                pltpu.VMEM((length, 2 * width), BF16),
                pltpu.VMEM((PAIR, length), BF16),
                pltpu.SemaphoreType.DMA((2 * len(pieces),)),
            ],
        ),
        out_shape=jax.ShapeDtypeStruct((rows, width), BF16),
        compiler_params=pltpu.CompilerParams(vmem_limit_bytes=56 << 20),
        cost_estimate=pl.CostEstimate(
            flops=rows * length * width,
            bytes_accessed=4 * length * width,
            transcendentals=rows * length * width // HEAD_DIM,
        ),
    )(places, queries, sent, stat, qmark, kmark, *[kv for kv, _ in pieces])


def key_kernel(
    sizes, step_queries, first_pair, place_ref, k_ref, v_ref, q_ref, qmark_ref, kmark_ref, *refs
):
    count = len(sizes)
    pieces = refs[:count]
    dk_ref, dv_ref, grad_ref, raw_ref, stat_ref, sems = refs[count:]
    rows, length = k_ref.shape[0], q_ref.shape[0]
    width = grad_ref.shape[1]
    stat_rows = stat_ref.shape[0]
    packed = STAT_ROWS * stat_rows
    pair = pl.program_id(0)
    index = place_ref[0]

    def copies(at):
        size = sizes[at]
        start = pl.multiple_of(place_ref[at] * rows + rows - size, BOUNDARY)
        return (
            pltpu.make_async_copy(
                pieces[at].at[pl.ds(0, size), pl.ds(first_pair * PAIR, width)],
                grad_ref.at[pl.ds(start, size), :],
                sems.at[2 * at],
            ),
            pltpu.make_async_copy(
                pieces[at].at[pl.ds(size, packed), :],
                raw_ref.at[at],
                sems.at[2 * at + 1],
            ),
        )

    @pl.when(pair == 0)
    def _():
        for at in range(count):

            @pl.when(place_ref[at] >= 0)
            def _(at=at):
                for one in copies(at):
                    one.start()

        @pl.when(index > 0)
        def _():
            start = pl.multiple_of((index - 1) * rows, rows)
            grad_ref[pl.ds(start, rows - BOUNDARY), :] = jnp.zeros(
                (rows - BOUNDARY, width), BF16
            )

        for at in range(count):

            @pl.when(place_ref[at] >= 0)
            def _(at=at):
                for one in copies(at):
                    one.wait()
                stat = raw_ref[at, :stat_rows].astype(F32)
                for part in range(1, STAT_ROWS):
                    stat = stat + raw_ref[
                        at, part * stat_rows : (part + 1) * stat_rows
                    ].astype(F32)
                start = pl.multiple_of(place_ref[at] * rows, rows)
                stat_ref[:, pl.ds(start, rows)] = stat

    keys, values = split_heads(k_ref[...]), split_heads(v_ref[...])
    columns = pl.ds(pl.multiple_of(pair * PAIR, PAIR), PAIR)
    head = 2 * (first_pair + pair)

    def step(masked):
        def body(at, state):
            start = pl.multiple_of(at * step_queries, step_queries)
            span = pl.ds(start, step_queries)
            queries = q_ref[span, :]
            grads = grad_ref[span, columns]
            if masked:
                allowed = kmark_ref[...] <= qmark_ref[:, span]
            new = []
            for h in range(2):
                lse = stat_ref[pl.ds(head + h, 1), span]
                delta = stat_ref[pl.ds(stat_rows // 2 + head + h, 1), span]
                score = nt(keys[h], queries)
                slope = nt(values[h], grads)
                prob = jnp.exp2(score - lse)
                if masked:
                    prob = jnp.where(allowed, prob, 0.0)
                grad = prob * (slope - delta)
                new += [
                    state[2 * h] + nn(grad.astype(BF16), queries),
                    state[2 * h + 1] + nn(prob.astype(BF16), grads),
                ]
            return tuple(new)

        return body

    empty = jnp.zeros((rows, PAIR), F32)
    first = jnp.maximum((index * rows - BOUNDARY) // step_queries, 0)
    own = ((index + 1) * rows + step_queries - 1) // step_queries
    state = lax.fori_loop(first, own, step(True), (empty,) * 4)
    state = lax.fori_loop(own, length // step_queries, step(False), state)
    lane = lax.broadcasted_iota(jnp.int32, (1, PAIR), 1)
    dk_ref[...] = (jnp.where(lane < HEAD_DIM, state[0], state[2]) * LN2).astype(dk_ref.dtype)
    dv_ref[...] = (0.5 * jnp.where(lane < HEAD_DIM, state[1], state[3])).astype(dv_ref.dtype)


def key_gradient(kv, q_all, pieces, qmark, kmark, first_pair, pairs, step_queries=512):
    rows = kv.shape[0]
    length, whole = q_all.shape
    width = pairs * PAIR
    stat_rows = 2 * whole // HEAD_DIM
    values_at = whole // PAIR + first_pair
    packed = STAT_ROWS * stat_rows
    places = jnp.stack([jnp.asarray(place, jnp.int32) for _, place in pieces])
    sizes = [sent.shape[0] - packed for sent, _ in pieces]
    return pl.pallas_call(
        functools.partial(key_kernel, sizes, step_queries, first_pair),
        grid_spec=pltpu.PrefetchScalarGridSpec(
            num_scalar_prefetch=1,
            grid=(pairs,),
            in_specs=[
                pl.BlockSpec((rows, PAIR), lambda h, s: (0, first_pair + h)),
                pl.BlockSpec((rows, PAIR), lambda h, s: (0, values_at + h)),
                pl.BlockSpec((length, PAIR), lambda h, s: (0, first_pair + h)),
                pl.BlockSpec((1, length), lambda h, s: (0, 0)),
                pl.BlockSpec((rows, 1), lambda h, s: (0, 0)),
            ]
            + [pl.BlockSpec(memory_space=pl.ANY)] * len(pieces),
            out_specs=[pl.BlockSpec((rows, PAIR), lambda h, s: (0, h))] * 2,
            scratch_shapes=[
                pltpu.VMEM((length, width), BF16),
                pltpu.VMEM((len(pieces), packed, rows), BF16),
                pltpu.VMEM((stat_rows, length), F32),
                pltpu.SemaphoreType.DMA((2 * len(pieces),)),
            ],
        ),
        out_shape=[jax.ShapeDtypeStruct((rows, width), BF16)] * 2,
        compiler_params=pltpu.CompilerParams(vmem_limit_bytes=56 << 20),
        cost_estimate=pl.CostEstimate(
            flops=rows * length * width,
            bytes_accessed=4 * length * width,
            transcendentals=rows * length * width // HEAD_DIM,
        ),
    )(places, kv, kv, q_all, qmark, kmark, *[sent for sent, _ in pieces])


def on_device(
    tokens,
    value_first,
    teacher,
    valid,
    blocks,
    gain_attn,
    gain_ffn,
    w_query,
    w_key,
    w_value,
    w_out,
    w_gate,
    w_up,
    w_down,
):
    width = tokens.shape[2]
    own_rows = tokens.shape[1]
    sizes = {axis: lax.axis_size(axis) for axis in ("shard", CTX, "tp")}
    shard, ctx, tp = (lax.axis_index(axis) for axis in ("shard", CTX, "tp"))
    group_rows = own_rows * sizes["tp"]
    half = w_query.shape[1]
    part = w_query.shape[0]
    line = sizes[CTX] // 2

    def flip(values, axis, bit=1):
        return lax.ppermute(values, axis, [(i, i ^ bit) for i in range(lax.axis_size(axis))])

    def tree_sum(values):
        for axis, size in sizes.items():
            bit = 1
            while bit < size:
                values = values + flip(values, axis, bit)
                bit *= 2
        return values

    def in_order(position, mine, other, axis):
        first = position == 0
        return jnp.concatenate(
            [jnp.where(first, mine, other), jnp.where(first, other, mine)], axis=axis
        )

    def shard_blocks(values):
        if sizes["shard"] == 2:
            return [values, flip(values, "shard")]
        gathered = lax.all_gather(values, "shard", axis=0, tiled=False)
        return [gathered[i] for i in range(sizes["shard"])]

    def block_of(values, at):
        if sizes["shard"] == 2:
            return cols_of(values, shard if at == 0 else 1 - shard, part)
        return values[:, at * part : (at + 1) * part]

    def join_blocks(terms):
        if sizes["shard"] == 2:
            return in_order(shard, terms[0], terms[1], 1)
        return jnp.concatenate(terms, axis=1)

    def times_blocks(lefts, blocks_of):
        return join_blocks(
            [
                sum(nn(left, blocks[at]) for left, blocks in zip(lefts, blocks_of))
                for at in range(sizes["shard"])
            ]
        )

    def times_turned(left, blocks):
        return sum(nt(block_of(left, at), block) for at, block in enumerate(blocks))

    def times_rows(left, blocks):
        return sum(nn(block_of(left, at), block) for at, block in enumerate(blocks))

    def times_rows_turned(lefts, blocks_of):
        return join_blocks(
            [
                sum(nt(left, blocks[at]) for left, blocks in zip(lefts, blocks_of))
                for at in range(sizes["shard"])
            ]
        )

    def ctx_bits():
        bit = 1
        while bit < sizes[CTX]:
            yield bit
            bit *= 2

    def reduce_ctx(parts, orders, between):
        parts, steps = list(parts), len(orders[0])
        for step in range(steps):
            for at, order in enumerate(orders):
                size = parts[at].shape[0] // 2
                side = (ctx // order[step]) % 2
                kept = lax.dynamic_slice_in_dim(parts[at], side * size, size, 0)
                sent = lax.dynamic_slice_in_dim(parts[at], (1 - side) * size, size, 0)
                got = flip(sent, CTX, order[step])
                parts[at] = (kept.astype(F32) + got.astype(F32)).astype(BF16)
            parts = between(step, parts)
        for step in reversed(range(steps)):
            for at, order in enumerate(orders):
                side = (ctx // order[step]) % 2
                parts[at] = in_order(side, parts[at], flip(parts[at], CTX, order[step]), 0)
            parts = between(2 * steps - 1 - step, parts)
        return parts

    def rows_of(values, position):
        return lax.dynamic_slice_in_dim(values, position * own_rows, own_rows, 0)

    def cols_of(values, position, size):
        return lax.dynamic_slice_in_dim(values, position * size, size, 1)

    level, column = ctx // 2, ctx % 2

    def spread(own, step, edge, between):
        if line != 4:
            gathered = lax.all_gather(own, CTX, axis=0, tiled=False)
            below = [(place < ctx) if step == 1 else (place > ctx) for place in range(2 * line)]
            pieces = [
                (gathered[place], jnp.where(below[place], place, -1)) for place in range(2 * line)
            ]
            beside = jnp.clip(ctx + step, 0, 2 * line - 1)
            rows = lax.dynamic_index_in_dim(gathered, beside, 0, keepdims=False)[edge]
            gathered, rows = between(0, [pieces[0][0], rows])
            pieces[0] = (gathered, pieces[0][1])
            stages = [pieces[:2]]
            for i in range(2, 2 * line, 2):
                (first,) = between(i // 2, [pieces[i][0]])
                stages.append([(first, pieces[i][1]), pieces[i + 1]])
            return stages, rows
        inside = range(2 * line)
        along = [(i, i + 2 * step) for i in inside if i + 2 * step in inside]
        near = 1 if step == 1 else 0
        against = [(i, i - 2 * step) for i in inside if i % 2 == near and i - 2 * step in inside]

        def place(hop, aside):
            there = level - step * hop
            at = 2 * there + ((1 - column) if aside else column)
            return jnp.where((there >= 0) & (there < line), at, -1)

        across, moving = between(0, [flip(own, CTX), lax.ppermute(own, CTX, along)])
        stages = [[(across, jnp.where(column == near, ctx - step, -1)), (moving, place(1, False))]]
        beside = lax.ppermute(across[edge], CTX, against)
        beside_here = across[edge]
        across, moving, beside = between(
            1, [flip(moving, CTX), lax.ppermute(moving, CTX, along), beside]
        )
        rows = jnp.where(column == near, beside, beside_here)
        stages.append([(across, place(1, True)), (moving, place(2, False))])
        across, moving = between(2, [flip(moving, CTX), lax.ppermute(moving, CTX, along)])
        stages.append([(across, place(2, True)), (moving, place(3, False))])
        cut = own.shape[0] // 32 * 16
        last = between(
            3, [flip(moving[:cut], CTX), lax.ppermute(across[cut:], CTX, along)]
        )
        stages.append([(jnp.concatenate(last, axis=0), place(3, True))])
        return stages, rows

    def shard_reduce(term, slice_rows):
        if sizes["shard"] == 2:
            return term(shard) + flip(term(1 - shard).astype(BF16), "shard").astype(F32)
        whole = jnp.concatenate(
            [term(i) for i in range(sizes["shard"])], axis=0 if slice_rows else 1
        )
        return lax.psum_scatter(
            whole.astype(BF16), "shard", scatter_dimension=0 if slice_rows else 1, tiled=True
        ).astype(F32)

    def over_rows(lefts, rights, slice_left):
        def term(position):
            if slice_left:
                return sum(tn(cols_of(a, position, part), b) for a, b in zip(lefts, rights))
            return sum(tn(a, cols_of(b, position, part)) for a, b in zip(lefts, rights))

        return shard_reduce(term, slice_left).astype(BF16)

    mine = tokens.reshape(own_rows, width)
    first_own = value_first.reshape(own_rows, width)
    key_marks = blocks.reshape(-1)
    padded_marks = jnp.concatenate([key_marks, jnp.full((BOUNDARY,), 1 << 30, key_marks.dtype)])
    query_marks = lax.dynamic_slice_in_dim(key_marks, ctx * group_rows, group_rows, 0)
    next_marks = lax.dynamic_slice_in_dim(padded_marks, (ctx + 1) * group_rows, BOUNDARY, 0)
    keep = valid.reshape(own_rows).astype(F32)

    theirs = flip(mine, "tp")
    first_theirs = flip(cols_of(first_own, 1 - tp, half), "tp")
    weight_qkv = shard_blocks(jnp.concatenate([w_query, w_key, w_value], axis=1))
    count = tree_sum(jnp.broadcast_to(jnp.sum(keep), (1, 128)))[0, 0]

    group = in_order(tp, mine, theirs, 0).astype(F32)
    normed_one = rms_norm(group, gain_attn).astype(BF16)
    first_group = in_order(tp, cols_of(first_own, tp, half), first_theirs, 0).astype(F32)
    qkv = times_rows(normed_one, weight_qkv)
    queries = (qkv[:, :half] * QUERY_SCALE).astype(BF16)
    kv = jnp.concatenate(
        [qkv[:, half : 2 * half], 0.5 * qkv[:, 2 * half :] + 0.5 * first_group], axis=1
    ).astype(BF16)

    kv, w_gate, w_up, w_down, w_out, count = lax.optimization_barrier(
        (kv, w_gate, w_up, w_down, w_out, count)
    )
    gathered = {
        "gate": shard_blocks(w_gate),
        "up": shard_blocks(w_up),
        "down": shard_blocks(w_down),
        "outs": [shard_blocks(w_out), shard_blocks(flip(w_out, "tp"))],
    }

    qmark = query_marks.reshape(1, -1)
    far_marks = jnp.concatenate(
        [key_marks, jnp.full((2 * KEY_STEP,), 1 << 30, key_marks.dtype)]
    )
    kmark = lax.dynamic_slice_in_dim(
        far_marks, ctx * group_rows // KEY_STEP * KEY_STEP, 2 * KEY_STEP, 0
    ).reshape(-1, 1)
    forward = {"state": None, "pieces": [(kv, 0, query_marks.reshape(-1, 1))]}

    def advance(last):
        forward["state"] = forward_stage(
            queries, qmark, forward["pieces"], forward["state"], last
        )
        forward["pieces"] = []

    def forward_between(at, arrays):
        advance(False)
        *arrays, out = lax.optimization_barrier((*arrays, forward["state"][2]))
        forward["state"] = (*forward["state"][:2], out)
        if line != 4:
            return arrays
        here = (column == 1) if at == 0 else (level >= at)
        if at == 3:
            forward["pieces"] = [(jnp.concatenate(arrays, axis=0), jnp.where(here, 0, -1), None)]
            return arrays
        forward["pieces"] = [
            (arrays[0], jnp.where(here, 0, -1), None),
            (arrays[1], jnp.where(level > at, 0, -1), None),
        ]
        if at == 0:
            forward["beside"] = arrays[0][:BOUNDARY]
        if at == 1:
            rows = jnp.where(column == 1, arrays[2], forward["beside"])
            forward["pieces"].insert(0, (rows, 0, next_marks.reshape(-1, 1)))
        return arrays

    if line == 4:
        stages, kv_next = spread(kv, 1, slice(0, BOUNDARY), forward_between)
        advance(True)
    else:
        stages, kv_next = spread(kv, 1, slice(0, BOUNDARY), lambda at, arrays: arrays)
        forward["pieces"].append((kv_next, 0, next_marks.reshape(-1, 1)))
        for at, stage in enumerate(stages):
            advance(False)
            forward["pieces"] = [(piece, place, None) for piece, place in stage]
        advance(True)
    attended, lse = forward["state"]

    outs, gate_weight = gathered["outs"], gathered["gate"]
    up_weight, down_weight = gathered["up"], gathered["down"]
    attended, q_own = lax.optimization_barrier((attended, queries))
    q_pair = in_order(column, q_own, flip(q_own, "side"), 0)
    q_all = lax.all_gather(q_pair, "line", axis=0, tiled=True)
    att = [rows_of(attended, tp), flip(rows_of(attended, 1 - tp), "tp")]
    inputs = mine.astype(F32)
    hidden = inputs + times_blocks(att, outs)
    normed_two = rms_norm(hidden, gain_ffn).astype(BF16)
    normed = [normed_two, flip(normed_two, "tp")]
    gate, up, logistic, act = [], [], [], []

    def widen(rows):
        gate.append(times_rows(rows, gate_weight))
        up.append(times_rows(rows, up_weight))
        logistic.append(jax.nn.sigmoid(gate[-1]))
        act.append((gate[-1] * logistic[-1] * up[-1]).astype(BF16))

    widen(normed[0])
    normed[1], act[0] = lax.optimization_barrier((normed[1], act[0]))
    widen(normed[1])
    down_theirs = flip(times_blocks([act[1]], [down_weight]).astype(BF16), "tp")
    down_theirs, q_pair = lax.optimization_barrier((down_theirs, q_pair))
    final = hidden + (times_blocks([act[0]], [down_weight]) + down_theirs.astype(F32))
    difference = final - teacher.reshape(own_rows, width).astype(F32)
    local_error = jnp.sum(jnp.mean(difference * difference, axis=1) * keep)
    token_total = group_rows * sizes[CTX] * sizes["shard"]
    grad_final = token_total / count * keep[:, None] * difference
    grad_round = grad_final.astype(BF16)
    rounds = [grad_round, flip(grad_round, "tp")]
    grad_gate, grad_up = [], []

    def back(at):
        grad_act = times_turned(rounds[at], down_weight)
        part = grad_act * logistic[at]
        grad_gate.append((part * up[at] * (1.0 + gate[at] * (1.0 - logistic[at]))).astype(BF16))
        grad_up.append((part * gate[at]).astype(BF16))

    back(0)
    rounds[1], grad_gate[0], grad_up[0] = lax.optimization_barrier(
        (rounds[1], grad_gate[0], grad_up[0])
    )
    back(1)
    both_weights = [gate_weight, up_weight]
    two_sent = times_rows_turned([grad_gate[1], grad_up[1]], both_weights).astype(BF16)
    two_theirs = flip(two_sent, "tp")
    gate_part = over_rows(normed, grad_gate, True)
    up_part = over_rows(normed, grad_up, True)
    down_part = over_rows(rounds, act, True)
    two_own = times_rows_turned([grad_gate[0], grad_up[0]], both_weights)
    two_theirs, two_own, gate_part, up_part, down_part = lax.optimization_barrier(
        (two_theirs, two_own, gate_part, up_part, down_part)
    )
    ffn_part = jnp.concatenate([gate_part, up_part, down_part], axis=1)
    grad_two = two_own + two_theirs.astype(F32)
    hidden_part, gain_ffn_term = jax.vjp(rms_norm, hidden, gain_ffn)[1](grad_two)
    grad_hidden = grad_final + hidden_part
    hidden_round = grad_hidden.astype(BF16)
    grad_att = [times_turned(hidden_round, w).astype(BF16) for w in outs]
    grad_theirs = flip(grad_att[1], "tp")
    sent, stat = pack_gradient(
        tp.reshape(1).astype(jnp.int32), grad_att[0], grad_theirs, attended, lse
    )

    hidden_two = flip(hidden_round, "tp")

    kv_pieces = [(kv, ctx), (kv_next, jnp.where(ctx + 1 < 2 * line, ctx + 1, -1))]
    kv_pieces += [piece for stage in stages for piece in stage]
    parts = {}

    pairs = half // PAIR
    quarters = max(pairs // 4, 1)

    def query_part(at):
        first = at * quarters
        count = quarters if at < 3 else pairs - first
        return query_gradient(
            queries, sent, parts["stat"], kv_pieces, qmark, kmark, key_marks.shape[0], first, count
        )

    def grad_between(at, arrays):
        if at == 0:
            parts["stat"], parts["q_all"], parts["hidden_two"] = stat, q_all, hidden_two
        if at > 3:
            return arrays
        name = "query" + str(at)
        parts[name] = query_part(at)
        hold = [name, "stat"]
        if at == 0:
            hold += ["q_all", "hidden_two"]
        if at == 3:
            parts["ffn"] = ffn_part
            hold.append("ffn")
        arrays, held = lax.optimization_barrier((arrays, [parts[name] for name in hold]))
        parts.update(zip(hold, held))
        return arrays

    grad_stages, sent_before = spread(
        sent, -1, slice(group_rows - BOUNDARY, None), grad_between
    )
    scattered = lax.psum_scatter(parts["ffn"], CTX, scatter_dimension=0, tiled=True)
    query_grad = jnp.concatenate([parts["query" + str(at)] for at in range(4)], axis=1)
    grad_pieces = [(sent, ctx), (sent_before, ctx - 1)]
    grad_pieces += [piece for stage in grad_stages for piece in stage]
    marks = (key_marks.reshape(1, -1), query_marks.reshape(-1, 1))
    key_grad, value_half = key_gradient(kv, parts["q_all"], grad_pieces, *marks, 0, pairs)
    key_grad, normed_held, parts["hidden_two"] = lax.optimization_barrier(
        (key_grad, normed_one, parts["hidden_two"])
    )
    early_part = jnp.concatenate(
        [
            over_rows([normed_held], [query_grad], True),
            over_rows(
                [hidden_round, parts["hidden_two"]],
                [rows_of(attended, tp), rows_of(attended, 1 - tp)],
                True,
            ),
        ],
        axis=1,
    )
    grads = jnp.concatenate([query_grad, key_grad, value_half], axis=1)
    kv_part = over_rows([normed_one], [grads[:, half:]], True)
    last = {}
    hidden_half = w_gate.shape[1]

    def finish(step, parts):
        if step == 0:
            parts, held, ready = lax.optimization_barrier((parts, grads, scattered))
            last["spread"] = lax.all_gather(ready, CTX, axis=0, tiled=True)
            theirs = times_rows_turned([rows_of(held, 1 - tp)], [weight_qkv]).astype(BF16)
            theirs = flip(theirs, "tp")
            last["own"] = times_rows_turned([rows_of(held, tp)], [weight_qkv])
            last["theirs"] = theirs
            last["value"] = flip(rows_of(held[:, 2 * half :], 1 - tp), "tp")
        if step == 1:
            *parts, last["own"], last["theirs"], last["value"] = lax.optimization_barrier(
                (*parts, last["own"], last["theirs"], last["value"])
            )
        if step == len(bits) + 1:
            parts, spread_out = lax.optimization_barrier((parts, last["spread"]))
            last["grads"] = [
                spread_out[:, at * hidden_half : (at + 1) * hidden_half].astype(F32)
                for at in range(3)
            ]
        return parts

    bits = list(ctx_bits())
    early, late = reduce_ctx([early_part, kv_part], [bits, bits[1:] + bits[:1]], finish)
    early, late = early.astype(F32), late.astype(F32)
    w_gate_grad, w_up_grad, w_down_grad = last["grads"]
    grad_one = last["own"] + last["theirs"].astype(F32)
    input_part, gain_attn_term = jax.vjp(rms_norm, inputs, gain_attn)[1](grad_one)
    tokens_grad = grad_hidden + input_part
    first_grad = in_order(tp, rows_of(value_half, tp), last["value"], 1).astype(F32)

    small = jnp.concatenate(
        [gain_attn_term, gain_ffn_term, jnp.broadcast_to(local_error, (128,))]
    )
    small = tree_sum(small.reshape(1, -1)).reshape(-1)
    return (
        final.astype(BF16).reshape(1, own_rows, width),
        small[2 * width] / count,
        tokens_grad.reshape(1, own_rows, width),
        first_grad.reshape(1, own_rows, width),
        small[:width],
        small[width : 2 * width],
        early[:, :half],
        late[:, :half],
        late[:, half:],
        early[:, half:].T,
        w_gate_grad,
        w_up_grad,
        w_down_grad.T,
    )


def solution(mesh):
    places = dict(mesh.shape)
    devices = mesh.devices.reshape(places["shard"], places["ctx"] // 2, 2, places["tp"])
    rows = P("shard", (*CTX, "tp"), None)
    wide, tall = P("shard", "tp"), P("tp", "shard")
    return jax.shard_map(
        on_device,
        mesh=jax.sharding.Mesh(devices, ("shard", *CTX, "tp")),
        in_specs=(
            rows,
            rows,
            rows,
            P("shard", (*CTX, "tp")),
            P("shard", None),
            P(),
            P(),
            wide,
            wide,
            wide,
            tall,
            wide,
            wide,
            tall,
        ),
        out_specs=(rows, P(), rows, rows, P(), P(), wide, wide, wide, tall, wide, wide, tall),
        check_vma=False,
    )
```

```python
import functools

import jax
import jax.numpy as jnp
from jax import lax
from jax.experimental import pallas as pl
from jax.experimental.pallas import tpu as pltpu
from jax.sharding import PartitionSpec as P

HEAD_DIM = 64
PAIR = 2 * HEAD_DIM
LN2 = 0.6931471805599453
QUERY_SCALE = HEAD_DIM ** (-0.5) / LN2
F32 = jnp.float32
BF16 = jnp.bfloat16
BOUNDARY = 256
STAT_ROWS = 3
KEY_STEP = 1024

CTX = ("line", "side")

epsilon = 1e-06


def rms_norm(values, gain):
    return values * lax.rsqrt(jnp.mean(values * values, axis=-1, keepdims=True) + epsilon) * gain


def dot(left, right, left_dim, right_dim):
    return lax.dot_general(
        left, right, (((left_dim,), (right_dim,)), ((), ())), preferred_element_type=F32
    )


def nn(left, right):
    return dot(left, right, 1, 0)


def nt(left, right):
    return dot(left, right, 1, 1)


def tn(left, right):
    return dot(left, right, 0, 0)


def split_heads(pair):
    lane = lax.broadcasted_iota(jnp.int32, (1, PAIR), 1)
    zero = jnp.zeros_like(pair)
    return [jnp.where(lane < HEAD_DIM, pair, zero), jnp.where(lane >= HEAD_DIM, pair, zero)]


def forward_kernel(pieces, first, last, flag_ref, q_ref, *refs):
    refs = list(refs)
    qmark_ref = refs.pop(0)
    arrays = []
    for masked in pieces:
        count = 3 if masked else 2
        arrays.append(refs[:count])
        refs = refs[count:]
    if not first:
        old_high, old_total, old_out = refs[:3]
        refs = refs[3:]
    if last:
        result_ref, lse_ref = refs[:2]
        refs = refs[2:]
    high_ref, total_ref, out_ref = refs
    rows = q_ref.shape[0]
    if first:
        high_ref[0] = jnp.full((2, rows), -1e30, F32)
        total_ref[0] = jnp.zeros((2, rows), F32)
        out_ref[...] = jnp.zeros((PAIR, rows), F32)
    else:
        high_ref[0] = old_high[0]
        total_ref[0] = old_total[0]
        out_ref[...] = old_out[...]
    queries = split_heads(q_ref[...])

    def add_piece(piece, masked):
        keys = piece[0][...]
        turned = piece[1][...].T
        scores = [nt(keys, queries[h]) for h in range(2)]
        if masked:
            allowed = piece[2][...] <= qmark_ref[...]
        for h in range(2):
            score = scores[h]
            if masked:
                score = jnp.where(allowed, score, -1e30)
            highest = high_ref[0, h : h + 1, :]
            top = jnp.maximum(highest, jnp.max(score, axis=0, keepdims=True))
            power = jnp.exp2(score - top)
            shrink = jnp.exp2(highest - top)
            high_ref[0, h : h + 1, :] = top
            total_ref[0, h : h + 1, :] = total_ref[0, h : h + 1, :] * shrink + jnp.sum(
                power, axis=0, keepdims=True
            )
            columns = pl.ds(HEAD_DIM * h, HEAD_DIM)
            out_ref[columns, :] = out_ref[columns, :] * shrink + nn(
                turned[HEAD_DIM * h : HEAD_DIM * (h + 1)], power.astype(BF16)
            )

    for at, masked in enumerate(pieces):
        if masked:
            add_piece(arrays[at], True)
        else:
            pl.when(flag_ref[at] >= 0)(functools.partial(add_piece, arrays[at], False))
    if last:
        for h in range(2):
            columns = pl.ds(HEAD_DIM * h, HEAD_DIM)
            out_ref[columns, :] = out_ref[columns, :] / total_ref[0, h : h + 1, :]
        result_ref[...] = out_ref[...].T.astype(BF16)
        lse_ref[0] = high_ref[0] + jnp.log2(total_ref[0])


def forward_stage(queries, qmark, pieces, state, last):
    rows, width = queries.shape
    pairs = width // PAIR
    flags = jnp.stack([jnp.asarray(place, jnp.int32) for _, place, _ in pieces])
    args = [queries, qmark]
    in_specs = [
        pl.BlockSpec((rows, PAIR), lambda h, s: (0, h)),
        pl.BlockSpec((1, rows), lambda h, s: (0, 0)),
    ]
    keys = 0
    for kv, _, marks in pieces:
        count = kv.shape[0]
        keys += count
        args += [kv, kv]
        in_specs += [
            pl.BlockSpec((count, PAIR), lambda h, s: (0, h)),
            pl.BlockSpec((count, PAIR), lambda h, s: (0, pairs + h)),
        ]
        if marks is not None:
            args.append(marks)
            in_specs.append(pl.BlockSpec((count, 1), lambda h, s: (0, 0)))
    stat = jax.ShapeDtypeStruct((pairs, 2, rows), F32)
    stat_spec = pl.BlockSpec((1, 2, rows), lambda h, s: (h, 0, 0))
    state_specs = [stat_spec, stat_spec, pl.BlockSpec((PAIR, rows), lambda h, s: (h, 0))]
    state_shapes = [stat, stat, jax.ShapeDtypeStruct((width, rows), F32)]
    if state is not None:
        args += list(state)
        in_specs += state_specs
    if last:
        out_specs = [pl.BlockSpec((rows, PAIR), lambda h, s: (0, h)), stat_spec]
        out_shape = [jax.ShapeDtypeStruct((rows, width), BF16), stat]
        scratch = [
            pltpu.VMEM((1, 2, rows), F32),
            pltpu.VMEM((1, 2, rows), F32),
            pltpu.VMEM((PAIR, rows), F32),
        ]
    else:
        out_specs, out_shape, scratch = state_specs, state_shapes, []
    return pl.pallas_call(
        functools.partial(
            forward_kernel, [m is not None for _, _, m in pieces], state is None, last
        ),
        grid_spec=pltpu.PrefetchScalarGridSpec(
            num_scalar_prefetch=1,
            grid=(pairs,),
            in_specs=in_specs,
            out_specs=out_specs,
            scratch_shapes=scratch,
        ),
        out_shape=out_shape,
        compiler_params=pltpu.CompilerParams(vmem_limit_bytes=40 << 20),
        cost_estimate=pl.CostEstimate(
            flops=16 * rows * keys * width,
            bytes_accessed=8 * keys * width,
            transcendentals=rows * keys * width // HEAD_DIM,
        ),
    )(flags, *args)


def stats_kernel(rows, place_ref, mine_ref, other_ref, out_ref, lse_ref, sent_ref, stat_ref):
    half = mine_ref.shape[0]
    place = place_ref[0]
    sent_ref[pl.ds(pl.multiple_of(place * half, half), half), :] = mine_ref[...]
    sent_ref[pl.ds(pl.multiple_of((1 - place) * half, half), half), :] = other_ref[...]
    width = mine_ref.shape[1]
    heads = width // HEAD_DIM
    deltas = []
    for pair in range(width // PAIR):
        columns = pl.ds(pair * PAIR, PAIR)
        grad = sent_ref[pl.ds(0, rows), columns]
        terms = (grad.astype(F32) * out_ref[:, columns].astype(F32)).T
        deltas += [
            jnp.sum(terms[:HEAD_DIM], axis=0, keepdims=True),
            jnp.sum(terms[HEAD_DIM:], axis=0, keepdims=True),
        ]
    stat = jnp.concatenate(
        [lse_ref[pair] for pair in range(width // PAIR)] + deltas, axis=0
    )
    stat_ref[...] = stat
    for at in range(STAT_ROWS):
        piece = stat.astype(BF16)
        sent_ref[pl.ds(rows + at * 2 * heads, 2 * heads), :] = piece
        stat = stat - piece.astype(F32)


def pack_gradient(place, mine, other, attended, lse):
    rows, width = attended.shape
    stat_rows = 2 * width // HEAD_DIM
    return pl.pallas_call(
        functools.partial(stats_kernel, rows),
        in_specs=[pl.BlockSpec(memory_space=pltpu.SMEM)]
        + [pl.BlockSpec(memory_space=pltpu.VMEM)] * 4,
        out_specs=[pl.BlockSpec(memory_space=pltpu.VMEM)] * 2,
        out_shape=[
            jax.ShapeDtypeStruct((rows + STAT_ROWS * stat_rows, width), BF16),
            jax.ShapeDtypeStruct((stat_rows, rows), F32),
        ],
    )(place, mine, other, attended, lse)


def query_kernel(
    sizes, step_keys, first_pair, place_ref, q_ref, grad_ref, stat_ref, qmark_ref, kmark_ref, *refs
):
    count = len(sizes)
    pieces, out_ref, kv_ref, kt_ref, sems = refs[:count], *refs[count:]
    rows, length = q_ref.shape[0], kv_ref.shape[0]
    width = kv_ref.shape[1] // 2
    pair = pl.program_id(0)
    index = place_ref[0]
    full = (index * rows) // step_keys
    end = jnp.minimum(
        ((index + 1) * rows + BOUNDARY + step_keys - 1) // step_keys, length // step_keys
    )

    def copies(at):
        start = pl.multiple_of(place_ref[at] * rows, rows)
        whole = pieces[at].shape[1] // 2
        return [
            pltpu.make_async_copy(
                pieces[at].at[:, pl.ds(part * whole + first_pair * PAIR, width)],
                kv_ref.at[pl.ds(start, sizes[at]), pl.ds(part * width, width)],
                sems.at[2 * at + part],
            )
            for part in range(2)
        ]

    def each(act):
        for at in range(count):

            @pl.when(place_ref[at] >= 0)
            def _(at=at):
                for one in copies(at):
                    act(one)

    @pl.when(pair == 0)
    def _():
        each(lambda one: one.start())

        def clear(at, _):
            start = pl.multiple_of(at * BOUNDARY, BOUNDARY)
            kv_ref[pl.ds(start, BOUNDARY), :] = jnp.zeros((BOUNDARY, 2 * width), BF16)
            return 0

        ratio = rows // BOUNDARY
        lax.fori_loop((index + 1) * ratio + 1, end * (step_keys // BOUNDARY), clear, 0)
        each(lambda one: one.wait())

    queries, grads = split_heads(q_ref[...]), split_heads(grad_ref[...])
    k_columns = pl.ds(pl.multiple_of(pair * PAIR, PAIR), PAIR)
    v_columns = pl.ds(pl.multiple_of(width + pair * PAIR, PAIR), PAIR)
    head = 2 * (first_pair + pair)
    lse = [stat_ref[pl.ds(head + h, 1), :] for h in range(2)]
    delta = [stat_ref[pl.ds(stat_ref.shape[0] // 2 + head + h, 1), :] for h in range(2)]

    def turn(at, _):
        start = pl.multiple_of(at * step_keys, step_keys)
        kt_ref[:, pl.ds(start, step_keys)] = kv_ref[pl.ds(start, step_keys), k_columns].T
        return 0

    lax.fori_loop(0, end, turn, 0)

    def step(masked):
        def body(at, state):
            start = pl.multiple_of(at * step_keys, step_keys)
            keys = kv_ref[pl.ds(start, step_keys), k_columns]
            values = kv_ref[pl.ds(start, step_keys), v_columns]
            if masked:
                window = pl.multiple_of((at - full) * step_keys, step_keys)
                allowed = kmark_ref[pl.ds(window, step_keys), :] <= qmark_ref[...]
            new = []
            for h in range(2):
                score = nt(keys, queries[h])
                slope = nt(values, grads[h])
                prob = jnp.exp2(score - lse[h])
                if masked:
                    prob = jnp.where(allowed, prob, 0.0)
                grad = (prob * (slope - delta[h])).astype(BF16)
                turned = kt_ref[pl.ds(HEAD_DIM * h, HEAD_DIM), pl.ds(start, step_keys)]
                new.append(state[h] + nn(turned, grad))
            return tuple(new)

        return body

    empty = jnp.zeros((HEAD_DIM, rows), F32)
    state = lax.fori_loop(full, end, step(True), (empty, empty))
    state = lax.fori_loop(0, full, step(False), state)
    out_ref[...] = (jnp.concatenate(state, axis=0).T * HEAD_DIM ** (-0.5)).astype(out_ref.dtype)


def query_gradient(
    queries, sent, stat, pieces, qmark, kmark, length, first_pair, pairs, step_keys=KEY_STEP
):
    rows, width = queries.shape[0], pairs * PAIR
    places = jnp.stack([jnp.asarray(place, jnp.int32) for _, place in pieces])
    sizes = [kv.shape[0] for kv, _ in pieces]
    return pl.pallas_call(
        functools.partial(query_kernel, sizes, step_keys, first_pair),
        grid_spec=pltpu.PrefetchScalarGridSpec(
            num_scalar_prefetch=1,
            grid=(pairs,),
            in_specs=[
                pl.BlockSpec((rows, PAIR), lambda h, s: (0, first_pair + h)),
                pl.BlockSpec((rows, PAIR), lambda h, s: (0, first_pair + h)),
                pl.BlockSpec(stat.shape, lambda h, s: (0, 0)),
                pl.BlockSpec((1, rows), lambda h, s: (0, 0)),
                pl.BlockSpec((2 * step_keys, 1), lambda h, s: (0, 0)),
            ]
            + [pl.BlockSpec(memory_space=pl.ANY)] * len(pieces),
            out_specs=pl.BlockSpec((rows, PAIR), lambda h, s: (0, h)),
            scratch_shapes=[
                pltpu.VMEM((length, 2 * width), BF16),
                pltpu.VMEM((PAIR, length), BF16),
                pltpu.SemaphoreType.DMA((2 * len(pieces),)),
            ],
        ),
        out_shape=jax.ShapeDtypeStruct((rows, width), BF16),
        compiler_params=pltpu.CompilerParams(vmem_limit_bytes=56 << 20),
        cost_estimate=pl.CostEstimate(
            flops=rows * length * width,
            bytes_accessed=4 * length * width,
            transcendentals=rows * length * width // HEAD_DIM,
        ),
    )(places, queries, sent, stat, qmark, kmark, *[kv for kv, _ in pieces])


def key_kernel(
    sizes, step_queries, first_pair, place_ref, k_ref, v_ref, q_ref, qmark_ref, kmark_ref, *refs
):
    count = len(sizes)
    pieces = refs[:count]
    dk_ref, dv_ref, grad_ref, raw_ref, stat_ref, sems = refs[count:]
    rows, length = k_ref.shape[0], q_ref.shape[0]
    width = grad_ref.shape[1]
    stat_rows = stat_ref.shape[0]
    packed = STAT_ROWS * stat_rows
    pair = pl.program_id(0)
    index = place_ref[0]

    def copies(at):
        size = sizes[at]
        start = pl.multiple_of(place_ref[at] * rows + rows - size, BOUNDARY)
        return (
            pltpu.make_async_copy(
                pieces[at].at[pl.ds(0, size), pl.ds(first_pair * PAIR, width)],
                grad_ref.at[pl.ds(start, size), :],
                sems.at[2 * at],
            ),
            pltpu.make_async_copy(
                pieces[at].at[pl.ds(size, packed), :],
                raw_ref.at[at],
                sems.at[2 * at + 1],
            ),
        )

    @pl.when(pair == 0)
    def _():
        for at in range(count):

            @pl.when(place_ref[at] >= 0)
            def _(at=at):
                for one in copies(at):
                    one.start()

        @pl.when(index > 0)
        def _():
            start = pl.multiple_of((index - 1) * rows, rows)
            grad_ref[pl.ds(start, rows - BOUNDARY), :] = jnp.zeros(
                (rows - BOUNDARY, width), BF16
            )

        for at in range(count):

            @pl.when(place_ref[at] >= 0)
            def _(at=at):
                for one in copies(at):
                    one.wait()
                stat = raw_ref[at, :stat_rows].astype(F32)
                for part in range(1, STAT_ROWS):
                    stat = stat + raw_ref[
                        at, part * stat_rows : (part + 1) * stat_rows
                    ].astype(F32)
                start = pl.multiple_of(place_ref[at] * rows, rows)
                stat_ref[:, pl.ds(start, rows)] = stat

    keys, values = split_heads(k_ref[...]), split_heads(v_ref[...])
    columns = pl.ds(pl.multiple_of(pair * PAIR, PAIR), PAIR)
    head = 2 * (first_pair + pair)

    def step(masked):
        def body(at, state):
            start = pl.multiple_of(at * step_queries, step_queries)
            span = pl.ds(start, step_queries)
            queries = q_ref[span, :]
            grads = grad_ref[span, columns]
            if masked:
                allowed = kmark_ref[...] <= qmark_ref[:, span]
            new = []
            for h in range(2):
                lse = stat_ref[pl.ds(head + h, 1), span]
                delta = stat_ref[pl.ds(stat_rows // 2 + head + h, 1), span]
                score = nt(keys[h], queries)
                slope = nt(values[h], grads)
                prob = jnp.exp2(score - lse)
                if masked:
                    prob = jnp.where(allowed, prob, 0.0)
                grad = prob * (slope - delta)
                new += [
                    state[2 * h] + nn(grad.astype(BF16), queries),
                    state[2 * h + 1] + nn(prob.astype(BF16), grads),
                ]
            return tuple(new)

        return body

    empty = jnp.zeros((rows, PAIR), F32)
    first = jnp.maximum((index * rows - BOUNDARY) // step_queries, 0)
    own = ((index + 1) * rows + step_queries - 1) // step_queries
    state = lax.fori_loop(first, own, step(True), (empty,) * 4)
    state = lax.fori_loop(own, length // step_queries, step(False), state)
    lane = lax.broadcasted_iota(jnp.int32, (1, PAIR), 1)
    dk_ref[...] = (jnp.where(lane < HEAD_DIM, state[0], state[2]) * LN2).astype(dk_ref.dtype)
    dv_ref[...] = (0.5 * jnp.where(lane < HEAD_DIM, state[1], state[3])).astype(dv_ref.dtype)


def key_gradient(kv, q_all, pieces, qmark, kmark, first_pair, pairs, step_queries=512):
    rows = kv.shape[0]
    length, whole = q_all.shape
    width = pairs * PAIR
    stat_rows = 2 * whole // HEAD_DIM
    values_at = whole // PAIR + first_pair
    packed = STAT_ROWS * stat_rows
    places = jnp.stack([jnp.asarray(place, jnp.int32) for _, place in pieces])
    sizes = [sent.shape[0] - packed for sent, _ in pieces]
    return pl.pallas_call(
        functools.partial(key_kernel, sizes, step_queries, first_pair),
        grid_spec=pltpu.PrefetchScalarGridSpec(
            num_scalar_prefetch=1,
            grid=(pairs,),
            in_specs=[
                pl.BlockSpec((rows, PAIR), lambda h, s: (0, first_pair + h)),
                pl.BlockSpec((rows, PAIR), lambda h, s: (0, values_at + h)),
                pl.BlockSpec((length, PAIR), lambda h, s: (0, first_pair + h)),
                pl.BlockSpec((1, length), lambda h, s: (0, 0)),
                pl.BlockSpec((rows, 1), lambda h, s: (0, 0)),
            ]
            + [pl.BlockSpec(memory_space=pl.ANY)] * len(pieces),
            out_specs=[pl.BlockSpec((rows, PAIR), lambda h, s: (0, h))] * 2,
            scratch_shapes=[
                pltpu.VMEM((length, width), BF16),
                pltpu.VMEM((len(pieces), packed, rows), BF16),
                pltpu.VMEM((stat_rows, length), F32),
                pltpu.SemaphoreType.DMA((2 * len(pieces),)),
            ],
        ),
        out_shape=[jax.ShapeDtypeStruct((rows, width), BF16)] * 2,
        compiler_params=pltpu.CompilerParams(vmem_limit_bytes=56 << 20),
        cost_estimate=pl.CostEstimate(
            flops=rows * length * width,
            bytes_accessed=4 * length * width,
            transcendentals=rows * length * width // HEAD_DIM,
        ),
    )(places, kv, kv, q_all, qmark, kmark, *[sent for sent, _ in pieces])


def on_device(
    tokens,
    value_first,
    teacher,
    valid,
    blocks,
    gain_attn,
    gain_ffn,
    w_query,
    w_key,
    w_value,
    w_out,
    w_gate,
    w_up,
    w_down,
):
    width = tokens.shape[2]
    own_rows = tokens.shape[1]
    sizes = {axis: lax.axis_size(axis) for axis in ("shard", CTX, "tp")}
    shard, ctx, tp = (lax.axis_index(axis) for axis in ("shard", CTX, "tp"))
    group_rows = own_rows * sizes["tp"]
    half = w_query.shape[1]
    part = w_query.shape[0]
    line = sizes[CTX] // 2

    def flip(values, axis, bit=1):
        return lax.ppermute(values, axis, [(i, i ^ bit) for i in range(lax.axis_size(axis))])

    def tree_sum(values):
        for axis, size in sizes.items():
            bit = 1
            while bit < size:
                values = values + flip(values, axis, bit)
                bit *= 2
        return values

    def in_order(position, mine, other, axis):
        first = position == 0
        return jnp.concatenate(
            [jnp.where(first, mine, other), jnp.where(first, other, mine)], axis=axis
        )

    def shard_blocks(values):
        if sizes["shard"] == 2:
            return [values, flip(values, "shard")]
        gathered = lax.all_gather(values, "shard", axis=0, tiled=False)
        return [gathered[i] for i in range(sizes["shard"])]

    def block_of(values, at):
        if sizes["shard"] == 2:
            return cols_of(values, shard if at == 0 else 1 - shard, part)
        return values[:, at * part : (at + 1) * part]

    def join_blocks(terms):
        if sizes["shard"] == 2:
            return in_order(shard, terms[0], terms[1], 1)
        return jnp.concatenate(terms, axis=1)

    def times_blocks(lefts, blocks_of):
        return join_blocks(
            [
                sum(nn(left, blocks[at]) for left, blocks in zip(lefts, blocks_of))
                for at in range(sizes["shard"])
            ]
        )

    def times_turned(left, blocks):
        return sum(nt(block_of(left, at), block) for at, block in enumerate(blocks))

    def times_rows(left, blocks):
        return sum(nn(block_of(left, at), block) for at, block in enumerate(blocks))

    def times_rows_turned(lefts, blocks_of):
        return join_blocks(
            [
                sum(nt(left, blocks[at]) for left, blocks in zip(lefts, blocks_of))
                for at in range(sizes["shard"])
            ]
        )

    def ctx_bits():
        bit = 1
        while bit < sizes[CTX]:
            yield bit
            bit *= 2

    def reduce_ctx(parts, orders, between):
        parts, steps = list(parts), len(orders[0])
        for step in range(steps):
            for at, order in enumerate(orders):
                size = parts[at].shape[0] // 2
                side = (ctx // order[step]) % 2
                kept = lax.dynamic_slice_in_dim(parts[at], side * size, size, 0)
                sent = lax.dynamic_slice_in_dim(parts[at], (1 - side) * size, size, 0)
                got = flip(sent, CTX, order[step])
                parts[at] = (kept.astype(F32) + got.astype(F32)).astype(BF16)
            parts = between(step, parts)
        for step in reversed(range(steps)):
            for at, order in enumerate(orders):
                side = (ctx // order[step]) % 2
                parts[at] = in_order(side, parts[at], flip(parts[at], CTX, order[step]), 0)
            parts = between(2 * steps - 1 - step, parts)
        return parts

    def rows_of(values, position):
        return lax.dynamic_slice_in_dim(values, position * own_rows, own_rows, 0)

    def cols_of(values, position, size):
        return lax.dynamic_slice_in_dim(values, position * size, size, 1)

    level, column = ctx // 2, ctx % 2

    def spread(own, step, edge, between):
        if line != 4:
            gathered = lax.all_gather(own, CTX, axis=0, tiled=False)
            below = [(place < ctx) if step == 1 else (place > ctx) for place in range(2 * line)]
            pieces = [
                (gathered[place], jnp.where(below[place], place, -1)) for place in range(2 * line)
            ]
            beside = jnp.clip(ctx + step, 0, 2 * line - 1)
            rows = lax.dynamic_index_in_dim(gathered, beside, 0, keepdims=False)[edge]
            gathered, rows = between(0, [pieces[0][0], rows])
            pieces[0] = (gathered, pieces[0][1])
            stages = [pieces[:2]]
            for i in range(2, 2 * line, 2):
                (first,) = between(i // 2, [pieces[i][0]])
                stages.append([(first, pieces[i][1]), pieces[i + 1]])
            return stages, rows
        inside = range(2 * line)
        along = [(i, i + 2 * step) for i in inside if i + 2 * step in inside]
        near = 1 if step == 1 else 0
        against = [(i, i - 2 * step) for i in inside if i % 2 == near and i - 2 * step in inside]

        def place(hop, aside):
            there = level - step * hop
            at = 2 * there + ((1 - column) if aside else column)
            return jnp.where((there >= 0) & (there < line), at, -1)

        across, moving = between(0, [flip(own, CTX), lax.ppermute(own, CTX, along)])
        stages = [[(across, jnp.where(column == near, ctx - step, -1)), (moving, place(1, False))]]
        beside = lax.ppermute(across[edge], CTX, against)
        beside_here = across[edge]
        across, moving, beside = between(
            1, [flip(moving, CTX), lax.ppermute(moving, CTX, along), beside]
        )
        rows = jnp.where(column == near, beside, beside_here)
        stages.append([(across, place(1, True)), (moving, place(2, False))])
        across, moving = between(2, [flip(moving, CTX), lax.ppermute(moving, CTX, along)])
        stages.append([(across, place(2, True)), (moving, place(3, False))])
        cut = own.shape[0] // 32 * 16
        last = between(
            3, [flip(moving[:cut], CTX), lax.ppermute(across[cut:], CTX, along)]
        )
        stages.append([(jnp.concatenate(last, axis=0), place(3, True))])
        return stages, rows

    def shard_reduce(term, slice_rows):
        if sizes["shard"] == 2:
            return term(shard) + flip(term(1 - shard).astype(BF16), "shard").astype(F32)
        whole = jnp.concatenate(
            [term(i) for i in range(sizes["shard"])], axis=0 if slice_rows else 1
        )
        return lax.psum_scatter(
            whole.astype(BF16), "shard", scatter_dimension=0 if slice_rows else 1, tiled=True
        ).astype(F32)

    def over_rows(lefts, rights, slice_left):
        def term(position):
            if slice_left:
                return sum(tn(cols_of(a, position, part), b) for a, b in zip(lefts, rights))
            return sum(tn(a, cols_of(b, position, part)) for a, b in zip(lefts, rights))

        return shard_reduce(term, slice_left).astype(BF16)

    mine = tokens.reshape(own_rows, width)
    first_own = value_first.reshape(own_rows, width)
    key_marks = blocks.reshape(-1)
    padded_marks = jnp.concatenate([key_marks, jnp.full((BOUNDARY,), 1 << 30, key_marks.dtype)])
    query_marks = lax.dynamic_slice_in_dim(key_marks, ctx * group_rows, group_rows, 0)
    next_marks = lax.dynamic_slice_in_dim(padded_marks, (ctx + 1) * group_rows, BOUNDARY, 0)
    keep = valid.reshape(own_rows).astype(F32)

    theirs = flip(mine, "tp")
    first_theirs = flip(cols_of(first_own, 1 - tp, half), "tp")
    weight_qkv = shard_blocks(jnp.concatenate([w_query, w_key, w_value], axis=1))
    count = tree_sum(jnp.broadcast_to(jnp.sum(keep), (1, 128)))[0, 0]

    group = in_order(tp, mine, theirs, 0).astype(F32)
    normed_one = rms_norm(group, gain_attn).astype(BF16)
    first_group = in_order(tp, cols_of(first_own, tp, half), first_theirs, 0).astype(F32)
    qkv = times_rows(normed_one, weight_qkv)
    queries = (qkv[:, :half] * QUERY_SCALE).astype(BF16)
    kv = jnp.concatenate(
        [qkv[:, half : 2 * half], 0.5 * qkv[:, 2 * half :] + 0.5 * first_group], axis=1
    ).astype(BF16)

    kv, w_gate, w_up, w_down, w_out, count = lax.optimization_barrier(
        (kv, w_gate, w_up, w_down, w_out, count)
    )
    gathered = {
        "gate": shard_blocks(w_gate),
        "up": shard_blocks(w_up),
        "down": shard_blocks(w_down),
        "outs": [shard_blocks(w_out), shard_blocks(flip(w_out, "tp"))],
    }

    qmark = query_marks.reshape(1, -1)
    far_marks = jnp.concatenate(
        [key_marks, jnp.full((2 * KEY_STEP,), 1 << 30, key_marks.dtype)]
    )
    kmark = lax.dynamic_slice_in_dim(
        far_marks, ctx * group_rows // KEY_STEP * KEY_STEP, 2 * KEY_STEP, 0
    ).reshape(-1, 1)
    forward = {"state": None, "pieces": [(kv, 0, query_marks.reshape(-1, 1))]}

    def advance(last):
        forward["state"] = forward_stage(
            queries, qmark, forward["pieces"], forward["state"], last
        )
        forward["pieces"] = []

    def forward_between(at, arrays):
        advance(False)
        *arrays, out = lax.optimization_barrier((*arrays, forward["state"][2]))
        forward["state"] = (*forward["state"][:2], out)
        if line != 4:
            return arrays
        here = (column == 1) if at == 0 else (level >= at)
        if at == 3:
            forward["pieces"] = [(jnp.concatenate(arrays, axis=0), jnp.where(here, 0, -1), None)]
            return arrays
        forward["pieces"] = [
            (arrays[0], jnp.where(here, 0, -1), None),
            (arrays[1], jnp.where(level > at, 0, -1), None),
        ]
        if at == 0:
            forward["beside"] = arrays[0][:BOUNDARY]
        if at == 1:
            rows = jnp.where(column == 1, arrays[2], forward["beside"])
            forward["pieces"].insert(0, (rows, 0, next_marks.reshape(-1, 1)))
        return arrays

    if line == 4:
        stages, kv_next = spread(kv, 1, slice(0, BOUNDARY), forward_between)
        advance(True)
    else:
        stages, kv_next = spread(kv, 1, slice(0, BOUNDARY), lambda at, arrays: arrays)
        forward["pieces"].append((kv_next, 0, next_marks.reshape(-1, 1)))
        for at, stage in enumerate(stages):
            advance(False)
            forward["pieces"] = [(piece, place, None) for piece, place in stage]
        advance(True)
    attended, lse = forward["state"]

    outs, gate_weight = gathered["outs"], gathered["gate"]
    up_weight, down_weight = gathered["up"], gathered["down"]
    attended, q_own = lax.optimization_barrier((attended, queries))
    q_pair = in_order(column, q_own, flip(q_own, "side"), 0)
    q_all = lax.all_gather(q_pair, "line", axis=0, tiled=True)
    att = [rows_of(attended, tp), flip(rows_of(attended, 1 - tp), "tp")]
    inputs = mine.astype(F32)
    hidden = inputs + times_blocks(att, outs)
    normed_two = rms_norm(hidden, gain_ffn).astype(BF16)
    normed = [normed_two, flip(normed_two, "tp")]
    gate, up, logistic, act = [], [], [], []

    def widen(rows):
        gate.append(times_rows(rows, gate_weight))
        up.append(times_rows(rows, up_weight))
        logistic.append(jax.nn.sigmoid(gate[-1]))
        act.append((gate[-1] * logistic[-1] * up[-1]).astype(BF16))

    widen(normed[0])
    normed[1], act[0] = lax.optimization_barrier((normed[1], act[0]))
    widen(normed[1])
    down_theirs = flip(times_blocks([act[1]], [down_weight]).astype(BF16), "tp")
    down_theirs, q_pair = lax.optimization_barrier((down_theirs, q_pair))
    final = hidden + (times_blocks([act[0]], [down_weight]) + down_theirs.astype(F32))
    difference = final - teacher.reshape(own_rows, width).astype(F32)
    local_error = jnp.sum(jnp.mean(difference * difference, axis=1) * keep)
    token_total = group_rows * sizes[CTX] * sizes["shard"]
    grad_final = token_total / count * keep[:, None] * difference
    grad_round = grad_final.astype(BF16)
    rounds = [grad_round, flip(grad_round, "tp")]
    grad_gate, grad_up = [], []

    def back(at):
        grad_act = times_turned(rounds[at], down_weight)
        part = grad_act * logistic[at]
        grad_gate.append((part * up[at] * (1.0 + gate[at] * (1.0 - logistic[at]))).astype(BF16))
        grad_up.append((part * gate[at]).astype(BF16))

    back(0)
    rounds[1], grad_gate[0], grad_up[0] = lax.optimization_barrier(
        (rounds[1], grad_gate[0], grad_up[0])
    )
    back(1)
    both_weights = [gate_weight, up_weight]
    two_sent = times_rows_turned([grad_gate[1], grad_up[1]], both_weights).astype(BF16)
    two_theirs = flip(two_sent, "tp")
    gate_part = over_rows(normed, grad_gate, True)
    up_part = over_rows(normed, grad_up, True)
    down_part = over_rows(rounds, act, True)
    two_own = times_rows_turned([grad_gate[0], grad_up[0]], both_weights)
    two_theirs, two_own, gate_part, up_part, down_part = lax.optimization_barrier(
        (two_theirs, two_own, gate_part, up_part, down_part)
    )
    ffn_part = jnp.concatenate([gate_part, up_part, down_part], axis=1)
    grad_two = two_own + two_theirs.astype(F32)
    hidden_part, gain_ffn_term = jax.vjp(rms_norm, hidden, gain_ffn)[1](grad_two)
    grad_hidden = grad_final + hidden_part
    hidden_round = grad_hidden.astype(BF16)
    grad_att = [times_turned(hidden_round, w).astype(BF16) for w in outs]
    grad_theirs = flip(grad_att[1], "tp")
    sent, stat = pack_gradient(
        tp.reshape(1).astype(jnp.int32), grad_att[0], grad_theirs, attended, lse
    )

    hidden_two = flip(hidden_round, "tp")

    kv_pieces = [(kv, ctx), (kv_next, jnp.where(ctx + 1 < 2 * line, ctx + 1, -1))]
    kv_pieces += [piece for stage in stages for piece in stage]
    parts = {}

    pairs = half // PAIR
    quarters = max(pairs // 4, 1)

    def query_part(at):
        first = at * quarters
        count = quarters if at < 3 else pairs - first
        return query_gradient(
            queries, sent, parts["stat"], kv_pieces, qmark, kmark, key_marks.shape[0], first, count
        )

    def grad_between(at, arrays):
        if at == 0:
            parts["stat"], parts["q_all"], parts["hidden_two"] = stat, q_all, hidden_two
        if at > 3:
            return arrays
        name = "query" + str(at)
        parts[name] = query_part(at)
        hold = [name, "stat"]
        if at == 0:
            hold += ["q_all", "hidden_two"]
        if at == 3:
            parts["ffn"] = ffn_part
            hold.append("ffn")
        arrays, held = lax.optimization_barrier((arrays, [parts[name] for name in hold]))
        parts.update(zip(hold, held))
        return arrays

    grad_stages, sent_before = spread(
        sent, -1, slice(group_rows - BOUNDARY, None), grad_between
    )
    scattered = lax.psum_scatter(parts["ffn"], CTX, scatter_dimension=0, tiled=True)
    query_grad = jnp.concatenate([parts["query" + str(at)] for at in range(4)], axis=1)
    grad_pieces = [(sent, ctx), (sent_before, ctx - 1)]
    grad_pieces += [piece for stage in grad_stages for piece in stage]
    marks = (key_marks.reshape(1, -1), query_marks.reshape(-1, 1))
    key_grad, value_half = key_gradient(kv, parts["q_all"], grad_pieces, *marks, 0, pairs)
    key_grad, normed_held, parts["hidden_two"] = lax.optimization_barrier(
        (key_grad, normed_one, parts["hidden_two"])
    )
    early_part = jnp.concatenate(
        [
            over_rows([normed_held], [query_grad], True),
            over_rows(
                [hidden_round, parts["hidden_two"]],
                [rows_of(attended, tp), rows_of(attended, 1 - tp)],
                True,
            ),
        ],
        axis=1,
    )
    grads = jnp.concatenate([query_grad, key_grad, value_half], axis=1)
    kv_part = over_rows([normed_one], [grads[:, half:]], True)
    last = {}
    hidden_half = w_gate.shape[1]

    def finish(step, parts):
        if step == 0:
            parts, held, ready = lax.optimization_barrier((parts, grads, scattered))
            last["spread"] = lax.all_gather(ready, CTX, axis=0, tiled=True)
            theirs = times_rows_turned([rows_of(held, 1 - tp)], [weight_qkv]).astype(BF16)
            theirs = flip(theirs, "tp")
            last["own"] = times_rows_turned([rows_of(held, tp)], [weight_qkv])
            last["theirs"] = theirs
            last["value"] = flip(rows_of(held[:, 2 * half :], 1 - tp), "tp")
        if step == 1:
            *parts, last["own"], last["theirs"], last["value"] = lax.optimization_barrier(
                (*parts, last["own"], last["theirs"], last["value"])
            )
        if step == len(bits) + 1:
            parts, spread_out = lax.optimization_barrier((parts, last["spread"]))
            pieces = [
                spread_out[:, at * hidden_half : (at + 1) * hidden_half] for at in range(3)
            ]
            pieces[2] = lax.optimization_barrier(pieces[2].T)
            last["grads"] = [piece.astype(F32) for piece in pieces]
        return parts

    bits = list(ctx_bits())
    early, late = reduce_ctx([early_part, kv_part], [bits, bits[1:] + bits[:1]], finish)
    early, late = early.astype(F32), late.astype(F32)
    w_gate_grad, w_up_grad, w_down_grad = last["grads"]
    grad_one = last["own"] + last["theirs"].astype(F32)
    input_part, gain_attn_term = jax.vjp(rms_norm, inputs, gain_attn)[1](grad_one)
    tokens_grad = grad_hidden + input_part
    first_grad = in_order(tp, rows_of(value_half, tp), last["value"], 1).astype(F32)

    small = jnp.concatenate(
        [gain_attn_term, gain_ffn_term, jnp.broadcast_to(local_error, (128,))]
    )
    small = tree_sum(small.reshape(1, -1)).reshape(-1)
    return (
        final.astype(BF16).reshape(1, own_rows, width),
        small[2 * width] / count,
        tokens_grad.reshape(1, own_rows, width),
        first_grad.reshape(1, own_rows, width),
        small[:width],
        small[width : 2 * width],
        early[:, :half],
        late[:, :half],
        late[:, half:],
        early[:, half:].T,
        w_gate_grad,
        w_up_grad,
        w_down_grad,
    )


def solution(mesh):
    places = dict(mesh.shape)
    devices = mesh.devices.reshape(places["shard"], places["ctx"] // 2, 2, places["tp"])
    rows = P("shard", (*CTX, "tp"), None)
    wide, tall = P("shard", "tp"), P("tp", "shard")
    return jax.shard_map(
        on_device,
        mesh=jax.sharding.Mesh(devices, ("shard", *CTX, "tp")),
        in_specs=(
            rows,
            rows,
            rows,
            P("shard", (*CTX, "tp")),
            P("shard", None),
            P(),
            P(),
            wide,
            wide,
            wide,
            tall,
            wide,
            wide,
            tall,
        ),
        out_specs=(rows, P(), rows, rows, P(), P(), wide, wide, wide, tall, wide, wide, tall),
        check_vma=False,
    )
```

```python
import functools

import jax
import jax.numpy as jnp
from jax import lax
from jax.experimental import pallas as pl
from jax.experimental.pallas import tpu as pltpu
from jax.sharding import PartitionSpec as P

HEAD_DIM = 64
PAIR = 2 * HEAD_DIM
LN2 = 0.6931471805599453
QUERY_SCALE = HEAD_DIM ** (-0.5) / LN2
F32 = jnp.float32
BF16 = jnp.bfloat16
BOUNDARY = 256
STAT_ROWS = 3
KEY_STEP = 1024

CTX = ("line", "side")

epsilon = 1e-06


def rms_norm(values, gain):
    return values * lax.rsqrt(jnp.mean(values * values, axis=-1, keepdims=True) + epsilon) * gain


def dot(left, right, left_dim, right_dim):
    return lax.dot_general(
        left, right, (((left_dim,), (right_dim,)), ((), ())), preferred_element_type=F32
    )


def nn(left, right):
    return dot(left, right, 1, 0)


def nt(left, right):
    return dot(left, right, 1, 1)


def tn(left, right):
    return dot(left, right, 0, 0)


def split_heads(pair):
    lane = lax.broadcasted_iota(jnp.int32, (1, PAIR), 1)
    zero = jnp.zeros_like(pair)
    return [jnp.where(lane < HEAD_DIM, pair, zero), jnp.where(lane >= HEAD_DIM, pair, zero)]


def forward_kernel(pieces, first, last, flag_ref, q_ref, *refs):
    refs = list(refs)
    qmark_ref = refs.pop(0)
    arrays = []
    for masked in pieces:
        count = 3 if masked else 2
        arrays.append(refs[:count])
        refs = refs[count:]
    if not first:
        old_high, old_total, old_out = refs[:3]
        refs = refs[3:]
    if last:
        result_ref, lse_ref = refs[:2]
        refs = refs[2:]
    high_ref, total_ref, out_ref = refs
    rows = q_ref.shape[0]
    if first:
        high_ref[0] = jnp.full((2, rows), -1e30, F32)
        total_ref[0] = jnp.zeros((2, rows), F32)
        out_ref[...] = jnp.zeros((PAIR, rows), F32)
    else:
        high_ref[0] = old_high[0]
        total_ref[0] = old_total[0]
        out_ref[...] = old_out[...]
    queries = split_heads(q_ref[...])

    def add_piece(piece, masked):
        keys = piece[0][...]
        turned = piece[1][...].T
        scores = [nt(keys, queries[h]) for h in range(2)]
        if masked:
            allowed = piece[2][...] <= qmark_ref[...]
        for h in range(2):
            score = scores[h]
            if masked:
                score = jnp.where(allowed, score, -1e30)
            highest = high_ref[0, h : h + 1, :]
            top = jnp.maximum(highest, jnp.max(score, axis=0, keepdims=True))
            power = jnp.exp2(score - top)
            shrink = jnp.exp2(highest - top)
            high_ref[0, h : h + 1, :] = top
            total_ref[0, h : h + 1, :] = total_ref[0, h : h + 1, :] * shrink + jnp.sum(
                power, axis=0, keepdims=True
            )
            columns = pl.ds(HEAD_DIM * h, HEAD_DIM)
            out_ref[columns, :] = out_ref[columns, :] * shrink + nn(
                turned[HEAD_DIM * h : HEAD_DIM * (h + 1)], power.astype(BF16)
            )

    for at, masked in enumerate(pieces):
        if masked:
            add_piece(arrays[at], True)
        else:
            pl.when(flag_ref[at] >= 0)(functools.partial(add_piece, arrays[at], False))
    if last:
        for h in range(2):
            columns = pl.ds(HEAD_DIM * h, HEAD_DIM)
            out_ref[columns, :] = out_ref[columns, :] / total_ref[0, h : h + 1, :]
        result_ref[...] = out_ref[...].T.astype(BF16)
        lse_ref[0] = high_ref[0] + jnp.log2(total_ref[0])


def forward_stage(queries, qmark, pieces, state, last):
    rows, width = queries.shape
    pairs = width // PAIR
    flags = jnp.stack([jnp.asarray(place, jnp.int32) for _, place, _ in pieces])
    args = [queries, qmark]
    in_specs = [
        pl.BlockSpec((rows, PAIR), lambda h, s: (0, h)),
        pl.BlockSpec((1, rows), lambda h, s: (0, 0)),
    ]
    keys = 0
    for kv, _, marks in pieces:
        count = kv.shape[0]
        keys += count
        args += [kv, kv]
        in_specs += [
            pl.BlockSpec((count, PAIR), lambda h, s: (0, h)),
            pl.BlockSpec((count, PAIR), lambda h, s: (0, pairs + h)),
        ]
        if marks is not None:
            args.append(marks)
            in_specs.append(pl.BlockSpec((count, 1), lambda h, s: (0, 0)))
    stat = jax.ShapeDtypeStruct((pairs, 2, rows), F32)
    stat_spec = pl.BlockSpec((1, 2, rows), lambda h, s: (h, 0, 0))
    state_specs = [stat_spec, stat_spec, pl.BlockSpec((PAIR, rows), lambda h, s: (h, 0))]
    state_shapes = [stat, stat, jax.ShapeDtypeStruct((width, rows), F32)]
    if state is not None:
        args += list(state)
        in_specs += state_specs
    if last:
        out_specs = [pl.BlockSpec((rows, PAIR), lambda h, s: (0, h)), stat_spec]
        out_shape = [jax.ShapeDtypeStruct((rows, width), BF16), stat]
        scratch = [
            pltpu.VMEM((1, 2, rows), F32),
            pltpu.VMEM((1, 2, rows), F32),
            pltpu.VMEM((PAIR, rows), F32),
        ]
    else:
        out_specs, out_shape, scratch = state_specs, state_shapes, []
    return pl.pallas_call(
        functools.partial(
            forward_kernel, [m is not None for _, _, m in pieces], state is None, last
        ),
        grid_spec=pltpu.PrefetchScalarGridSpec(
            num_scalar_prefetch=1,
            grid=(pairs,),
            in_specs=in_specs,
            out_specs=out_specs,
            scratch_shapes=scratch,
        ),
        out_shape=out_shape,
        compiler_params=pltpu.CompilerParams(vmem_limit_bytes=40 << 20),
        cost_estimate=pl.CostEstimate(
            flops=16 * rows * keys * width,
            bytes_accessed=8 * keys * width,
            transcendentals=rows * keys * width // HEAD_DIM,
        ),
    )(flags, *args)


def stats_kernel(rows, place_ref, mine_ref, other_ref, out_ref, lse_ref, sent_ref, stat_ref):
    half = mine_ref.shape[0]
    place = place_ref[0]
    sent_ref[pl.ds(pl.multiple_of(place * half, half), half), :] = mine_ref[...]
    sent_ref[pl.ds(pl.multiple_of((1 - place) * half, half), half), :] = other_ref[...]
    width = mine_ref.shape[1]
    heads = width // HEAD_DIM
    deltas = []
    for pair in range(width // PAIR):
        columns = pl.ds(pair * PAIR, PAIR)
        grad = sent_ref[pl.ds(0, rows), columns]
        terms = (grad.astype(F32) * out_ref[:, columns].astype(F32)).T
        deltas += [
            jnp.sum(terms[:HEAD_DIM], axis=0, keepdims=True),
            jnp.sum(terms[HEAD_DIM:], axis=0, keepdims=True),
        ]
    stat = jnp.concatenate(
        [lse_ref[pair] for pair in range(width // PAIR)] + deltas, axis=0
    )
    stat_ref[...] = stat
    for at in range(STAT_ROWS):
        piece = stat.astype(BF16)
        sent_ref[pl.ds(rows + at * 2 * heads, 2 * heads), :] = piece
        stat = stat - piece.astype(F32)


def pack_gradient(place, mine, other, attended, lse):
    rows, width = attended.shape
    stat_rows = 2 * width // HEAD_DIM
    return pl.pallas_call(
        functools.partial(stats_kernel, rows),
        in_specs=[pl.BlockSpec(memory_space=pltpu.SMEM)]
        + [pl.BlockSpec(memory_space=pltpu.VMEM)] * 4,
        out_specs=[pl.BlockSpec(memory_space=pltpu.VMEM)] * 2,
        out_shape=[
            jax.ShapeDtypeStruct((rows + STAT_ROWS * stat_rows, width), BF16),
            jax.ShapeDtypeStruct((stat_rows, rows), F32),
        ],
    )(place, mine, other, attended, lse)


def query_kernel(
    sizes, step_keys, first_pair, place_ref, q_ref, grad_ref, stat_ref, qmark_ref, kmark_ref, *refs
):
    count = len(sizes)
    pieces, out_ref, kv_ref, kt_ref, sems = refs[:count], *refs[count:]
    rows, length = q_ref.shape[0], kv_ref.shape[0]
    width = kv_ref.shape[1] // 2
    pair = pl.program_id(0)
    index = place_ref[0]
    full = (index * rows) // step_keys
    end = jnp.minimum(
        ((index + 1) * rows + BOUNDARY + step_keys - 1) // step_keys, length // step_keys
    )

    def copies(at):
        start = pl.multiple_of(place_ref[at] * rows, rows)
        whole = pieces[at].shape[1] // 2
        return [
            pltpu.make_async_copy(
                pieces[at].at[:, pl.ds(part * whole + first_pair * PAIR, width)],
                kv_ref.at[pl.ds(start, sizes[at]), pl.ds(part * width, width)],
                sems.at[2 * at + part],
            )
            for part in range(2)
        ]

    def each(act):
        for at in range(count):

            @pl.when(place_ref[at] >= 0)
            def _(at=at):
                for one in copies(at):
                    act(one)

    @pl.when(pair == 0)
    def _():
        each(lambda one: one.start())

        def clear(at, _):
            start = pl.multiple_of(at * BOUNDARY, BOUNDARY)
            kv_ref[pl.ds(start, BOUNDARY), :] = jnp.zeros((BOUNDARY, 2 * width), BF16)
            return 0

        ratio = rows // BOUNDARY
        lax.fori_loop((index + 1) * ratio + 1, end * (step_keys // BOUNDARY), clear, 0)
        each(lambda one: one.wait())

    queries, grads = split_heads(q_ref[...]), split_heads(grad_ref[...])
    k_columns = pl.ds(pl.multiple_of(pair * PAIR, PAIR), PAIR)
    v_columns = pl.ds(pl.multiple_of(width + pair * PAIR, PAIR), PAIR)
    head = 2 * (first_pair + pair)
    lse = [stat_ref[pl.ds(head + h, 1), :] for h in range(2)]
    delta = [stat_ref[pl.ds(stat_ref.shape[0] // 2 + head + h, 1), :] for h in range(2)]

    def turn(at, _):
        start = pl.multiple_of(at * step_keys, step_keys)
        kt_ref[:, pl.ds(start, step_keys)] = kv_ref[pl.ds(start, step_keys), k_columns].T
        return 0

    lax.fori_loop(0, end, turn, 0)

    def step(masked):
        def body(at, state):
            start = pl.multiple_of(at * step_keys, step_keys)
            keys = kv_ref[pl.ds(start, step_keys), k_columns]
            values = kv_ref[pl.ds(start, step_keys), v_columns]
            if masked:
                window = pl.multiple_of((at - full) * step_keys, step_keys)
                allowed = kmark_ref[pl.ds(window, step_keys), :] <= qmark_ref[...]
            new = []
            for h in range(2):
                score = nt(keys, queries[h])
                slope = nt(values, grads[h])
                prob = jnp.exp2(score - lse[h])
                if masked:
                    prob = jnp.where(allowed, prob, 0.0)
                grad = (prob * (slope - delta[h])).astype(BF16)
                turned = kt_ref[pl.ds(HEAD_DIM * h, HEAD_DIM), pl.ds(start, step_keys)]
                new.append(state[h] + nn(turned, grad))
            return tuple(new)

        return body

    empty = jnp.zeros((HEAD_DIM, rows), F32)
    state = lax.fori_loop(full, end, step(True), (empty, empty))
    state = lax.fori_loop(0, full, step(False), state)
    out_ref[...] = (jnp.concatenate(state, axis=0).T * HEAD_DIM ** (-0.5)).astype(out_ref.dtype)


def query_gradient(
    queries, sent, stat, pieces, qmark, kmark, length, first_pair, pairs, step_keys=KEY_STEP
):
    rows, width = queries.shape[0], pairs * PAIR
    places = jnp.stack([jnp.asarray(place, jnp.int32) for _, place in pieces])
    sizes = [kv.shape[0] for kv, _ in pieces]
    return pl.pallas_call(
        functools.partial(query_kernel, sizes, step_keys, first_pair),
        grid_spec=pltpu.PrefetchScalarGridSpec(
            num_scalar_prefetch=1,
            grid=(pairs,),
            in_specs=[
                pl.BlockSpec((rows, PAIR), lambda h, s: (0, first_pair + h)),
                pl.BlockSpec((rows, PAIR), lambda h, s: (0, first_pair + h)),
                pl.BlockSpec(stat.shape, lambda h, s: (0, 0)),
                pl.BlockSpec((1, rows), lambda h, s: (0, 0)),
                pl.BlockSpec((2 * step_keys, 1), lambda h, s: (0, 0)),
            ]
            + [pl.BlockSpec(memory_space=pl.ANY)] * len(pieces),
            out_specs=pl.BlockSpec((rows, PAIR), lambda h, s: (0, h)),
            scratch_shapes=[
                pltpu.VMEM((length, 2 * width), BF16),
                pltpu.VMEM((PAIR, length), BF16),
                pltpu.SemaphoreType.DMA((2 * len(pieces),)),
            ],
        ),
        out_shape=jax.ShapeDtypeStruct((rows, width), BF16),
        compiler_params=pltpu.CompilerParams(vmem_limit_bytes=56 << 20),
        cost_estimate=pl.CostEstimate(
            flops=rows * length * width,
            bytes_accessed=4 * length * width,
            transcendentals=rows * length * width // HEAD_DIM,
        ),
    )(places, queries, sent, stat, qmark, kmark, *[kv for kv, _ in pieces])


def key_kernel(
    sizes, step_queries, first_pair, place_ref, k_ref, v_ref, q_ref, qmark_ref, kmark_ref, *refs
):
    count = len(sizes)
    pieces = refs[:count]
    dk_ref, dv_ref, grad_ref, raw_ref, stat_ref, sems = refs[count:]
    rows, length = k_ref.shape[0], q_ref.shape[0]
    width = grad_ref.shape[1]
    stat_rows = stat_ref.shape[0]
    packed = STAT_ROWS * stat_rows
    pair = pl.program_id(0)
    index = place_ref[0]

    def copies(at):
        size = sizes[at]
        start = pl.multiple_of(place_ref[at] * rows + rows - size, BOUNDARY)
        return (
            pltpu.make_async_copy(
                pieces[at].at[pl.ds(0, size), pl.ds(first_pair * PAIR, width)],
                grad_ref.at[pl.ds(start, size), :],
                sems.at[2 * at],
            ),
            pltpu.make_async_copy(
                pieces[at].at[pl.ds(size, packed), :],
                raw_ref.at[at],
                sems.at[2 * at + 1],
            ),
        )

    @pl.when(pair == 0)
    def _():
        for at in range(count):

            @pl.when(place_ref[at] >= 0)
            def _(at=at):
                for one in copies(at):
                    one.start()

        @pl.when(index > 0)
        def _():
            start = pl.multiple_of((index - 1) * rows, rows)
            grad_ref[pl.ds(start, rows - BOUNDARY), :] = jnp.zeros(
                (rows - BOUNDARY, width), BF16
            )

        for at in range(count):

            @pl.when(place_ref[at] >= 0)
            def _(at=at):
                for one in copies(at):
                    one.wait()
                stat = raw_ref[at, :stat_rows].astype(F32)
                for part in range(1, STAT_ROWS):
                    stat = stat + raw_ref[
                        at, part * stat_rows : (part + 1) * stat_rows
                    ].astype(F32)
                start = pl.multiple_of(place_ref[at] * rows, rows)
                stat_ref[:, pl.ds(start, rows)] = stat

    keys, values = split_heads(k_ref[...]), split_heads(v_ref[...])
    columns = pl.ds(pl.multiple_of(pair * PAIR, PAIR), PAIR)
    head = 2 * (first_pair + pair)

    def step(masked):
        def body(at, state):
            start = pl.multiple_of(at * step_queries, step_queries)
            span = pl.ds(start, step_queries)
            queries = q_ref[span, :]
            grads = grad_ref[span, columns]
            if masked:
                allowed = kmark_ref[...] <= qmark_ref[:, span]
            new = []
            for h in range(2):
                lse = stat_ref[pl.ds(head + h, 1), span]
                delta = stat_ref[pl.ds(stat_rows // 2 + head + h, 1), span]
                score = nt(keys[h], queries)
                slope = nt(values[h], grads)
                prob = jnp.exp2(score - lse)
                if masked:
                    prob = jnp.where(allowed, prob, 0.0)
                grad = prob * (slope - delta)
                new += [
                    state[2 * h] + nn(grad.astype(BF16), queries),
                    state[2 * h + 1] + nn(prob.astype(BF16), grads),
                ]
            return tuple(new)

        return body

    empty = jnp.zeros((rows, PAIR), F32)
    first = jnp.maximum((index * rows - BOUNDARY) // step_queries, 0)
    own = ((index + 1) * rows + step_queries - 1) // step_queries
    state = lax.fori_loop(first, own, step(True), (empty,) * 4)
    state = lax.fori_loop(own, length // step_queries, step(False), state)
    lane = lax.broadcasted_iota(jnp.int32, (1, PAIR), 1)
    dk_ref[...] = (jnp.where(lane < HEAD_DIM, state[0], state[2]) * LN2).astype(dk_ref.dtype)
    dv_ref[...] = (0.5 * jnp.where(lane < HEAD_DIM, state[1], state[3])).astype(dv_ref.dtype)


def key_gradient(kv, q_all, pieces, qmark, kmark, first_pair, pairs, step_queries=512):
    rows = kv.shape[0]
    length, whole = q_all.shape
    width = pairs * PAIR
    stat_rows = 2 * whole // HEAD_DIM
    values_at = whole // PAIR + first_pair
    packed = STAT_ROWS * stat_rows
    places = jnp.stack([jnp.asarray(place, jnp.int32) for _, place in pieces])
    sizes = [sent.shape[0] - packed for sent, _ in pieces]
    return pl.pallas_call(
        functools.partial(key_kernel, sizes, step_queries, first_pair),
        grid_spec=pltpu.PrefetchScalarGridSpec(
            num_scalar_prefetch=1,
            grid=(pairs,),
            in_specs=[
                pl.BlockSpec((rows, PAIR), lambda h, s: (0, first_pair + h)),
                pl.BlockSpec((rows, PAIR), lambda h, s: (0, values_at + h)),
                pl.BlockSpec((length, PAIR), lambda h, s: (0, first_pair + h)),
                pl.BlockSpec((1, length), lambda h, s: (0, 0)),
                pl.BlockSpec((rows, 1), lambda h, s: (0, 0)),
            ]
            + [pl.BlockSpec(memory_space=pl.ANY)] * len(pieces),
            out_specs=[pl.BlockSpec((rows, PAIR), lambda h, s: (0, h))] * 2,
            scratch_shapes=[
                pltpu.VMEM((length, width), BF16),
                pltpu.VMEM((len(pieces), packed, rows), BF16),
                pltpu.VMEM((stat_rows, length), F32),
                pltpu.SemaphoreType.DMA((2 * len(pieces),)),
            ],
        ),
        out_shape=[jax.ShapeDtypeStruct((rows, width), BF16)] * 2,
        compiler_params=pltpu.CompilerParams(vmem_limit_bytes=56 << 20),
        cost_estimate=pl.CostEstimate(
            flops=rows * length * width,
            bytes_accessed=4 * length * width,
            transcendentals=rows * length * width // HEAD_DIM,
        ),
    )(places, kv, kv, q_all, qmark, kmark, *[sent for sent, _ in pieces])


def on_device(
    tokens,
    value_first,
    teacher,
    valid,
    blocks,
    gain_attn,
    gain_ffn,
    w_query,
    w_key,
    w_value,
    w_out,
    w_gate,
    w_up,
    w_down,
):
    width = tokens.shape[2]
    own_rows = tokens.shape[1]
    sizes = {axis: lax.axis_size(axis) for axis in ("shard", CTX, "tp")}
    shard, ctx, tp = (lax.axis_index(axis) for axis in ("shard", CTX, "tp"))
    group_rows = own_rows * sizes["tp"]
    half = w_query.shape[1]
    part = w_query.shape[0]
    line = sizes[CTX] // 2

    def flip(values, axis, bit=1):
        return lax.ppermute(values, axis, [(i, i ^ bit) for i in range(lax.axis_size(axis))])

    def tree_sum(values):
        for axis, size in sizes.items():
            bit = 1
            while bit < size:
                values = values + flip(values, axis, bit)
                bit *= 2
        return values

    def in_order(position, mine, other, axis):
        first = position == 0
        return jnp.concatenate(
            [jnp.where(first, mine, other), jnp.where(first, other, mine)], axis=axis
        )

    def shard_blocks(values):
        if sizes["shard"] == 2:
            return [values, flip(values, "shard")]
        gathered = lax.all_gather(values, "shard", axis=0, tiled=False)
        return [gathered[i] for i in range(sizes["shard"])]

    def block_of(values, at):
        if sizes["shard"] == 2:
            return cols_of(values, shard if at == 0 else 1 - shard, part)
        return values[:, at * part : (at + 1) * part]

    def join_blocks(terms):
        if sizes["shard"] == 2:
            return in_order(shard, terms[0], terms[1], 1)
        return jnp.concatenate(terms, axis=1)

    def times_blocks(lefts, blocks_of):
        return join_blocks(
            [
                sum(nn(left, blocks[at]) for left, blocks in zip(lefts, blocks_of))
                for at in range(sizes["shard"])
            ]
        )

    def times_turned(left, blocks):
        return sum(nt(block_of(left, at), block) for at, block in enumerate(blocks))

    def times_rows(left, blocks):
        return sum(nn(block_of(left, at), block) for at, block in enumerate(blocks))

    def times_rows_turned(lefts, blocks_of):
        return join_blocks(
            [
                sum(nt(left, blocks[at]) for left, blocks in zip(lefts, blocks_of))
                for at in range(sizes["shard"])
            ]
        )

    def ctx_bits():
        bit = 1
        while bit < sizes[CTX]:
            yield bit
            bit *= 2

    def reduce_ctx(parts, orders, between):
        parts, steps = list(parts), len(orders[0])
        for step in range(steps):
            for at, order in enumerate(orders):
                size = parts[at].shape[0] // 2
                side = (ctx // order[step]) % 2
                kept = lax.dynamic_slice_in_dim(parts[at], side * size, size, 0)
                sent = lax.dynamic_slice_in_dim(parts[at], (1 - side) * size, size, 0)
                got = flip(sent, CTX, order[step])
                parts[at] = (kept.astype(F32) + got.astype(F32)).astype(BF16)
            parts = between(step, parts)
        for step in reversed(range(steps)):
            for at, order in enumerate(orders):
                side = (ctx // order[step]) % 2
                parts[at] = in_order(side, parts[at], flip(parts[at], CTX, order[step]), 0)
            parts = between(2 * steps - 1 - step, parts)
        return parts

    def rows_of(values, position):
        return lax.dynamic_slice_in_dim(values, position * own_rows, own_rows, 0)

    def cols_of(values, position, size):
        return lax.dynamic_slice_in_dim(values, position * size, size, 1)

    level, column = ctx // 2, ctx % 2

    def spread(own, step, edge, between):
        if line != 4:
            gathered = lax.all_gather(own, CTX, axis=0, tiled=False)
            below = [(place < ctx) if step == 1 else (place > ctx) for place in range(2 * line)]
            pieces = [
                (gathered[place], jnp.where(below[place], place, -1)) for place in range(2 * line)
            ]
            beside = jnp.clip(ctx + step, 0, 2 * line - 1)
            rows = lax.dynamic_index_in_dim(gathered, beside, 0, keepdims=False)[edge]
            gathered, rows = between(0, [pieces[0][0], rows])
            pieces[0] = (gathered, pieces[0][1])
            stages = [pieces[:2]]
            for i in range(2, 2 * line, 2):
                (first,) = between(i // 2, [pieces[i][0]])
                stages.append([(first, pieces[i][1]), pieces[i + 1]])
            return stages, rows
        inside = range(2 * line)
        along = [(i, i + 2 * step) for i in inside if i + 2 * step in inside]
        near = 1 if step == 1 else 0
        against = [(i, i - 2 * step) for i in inside if i % 2 == near and i - 2 * step in inside]

        def place(hop, aside):
            there = level - step * hop
            at = 2 * there + ((1 - column) if aside else column)
            return jnp.where((there >= 0) & (there < line), at, -1)

        across, moving = between(0, [flip(own, CTX), lax.ppermute(own, CTX, along)])
        stages = [[(across, jnp.where(column == near, ctx - step, -1)), (moving, place(1, False))]]
        beside = lax.ppermute(across[edge], CTX, against)
        beside_here = across[edge]
        across, moving, beside = between(
            1, [flip(moving, CTX), lax.ppermute(moving, CTX, along), beside]
        )
        rows = jnp.where(column == near, beside, beside_here)
        stages.append([(across, place(1, True)), (moving, place(2, False))])
        across, moving = between(2, [flip(moving, CTX), lax.ppermute(moving, CTX, along)])
        stages.append([(across, place(2, True)), (moving, place(3, False))])
        cut = own.shape[0] // 32 * 16
        last = between(
            3, [flip(moving[:cut], CTX), lax.ppermute(across[cut:], CTX, along)]
        )
        stages.append([(jnp.concatenate(last, axis=0), place(3, True))])
        return stages, rows

    def shard_reduce(term, slice_rows):
        if sizes["shard"] == 2:
            return term(shard) + flip(term(1 - shard).astype(BF16), "shard").astype(F32)
        whole = jnp.concatenate(
            [term(i) for i in range(sizes["shard"])], axis=0 if slice_rows else 1
        )
        return lax.psum_scatter(
            whole.astype(BF16), "shard", scatter_dimension=0 if slice_rows else 1, tiled=True
        ).astype(F32)

    def over_rows(lefts, rights, slice_left):
        def term(position):
            if slice_left:
                return sum(tn(cols_of(a, position, part), b) for a, b in zip(lefts, rights))
            return sum(tn(a, cols_of(b, position, part)) for a, b in zip(lefts, rights))

        return shard_reduce(term, slice_left).astype(BF16)

    mine = tokens.reshape(own_rows, width)
    first_own = value_first.reshape(own_rows, width)
    key_marks = blocks.reshape(-1)
    padded_marks = jnp.concatenate([key_marks, jnp.full((BOUNDARY,), 1 << 30, key_marks.dtype)])
    query_marks = lax.dynamic_slice_in_dim(key_marks, ctx * group_rows, group_rows, 0)
    next_marks = lax.dynamic_slice_in_dim(padded_marks, (ctx + 1) * group_rows, BOUNDARY, 0)
    keep = valid.reshape(own_rows).astype(F32)

    theirs = flip(mine, "tp")
    first_theirs = flip(cols_of(first_own, 1 - tp, half), "tp")
    weight_qkv = shard_blocks(jnp.concatenate([w_query, w_key, w_value], axis=1))
    count = tree_sum(jnp.broadcast_to(jnp.sum(keep), (1, 128)))[0, 0]

    group = in_order(tp, mine, theirs, 0).astype(F32)
    normed_one = rms_norm(group, gain_attn).astype(BF16)
    first_group = in_order(tp, cols_of(first_own, tp, half), first_theirs, 0).astype(F32)
    qkv = times_rows(normed_one, weight_qkv)
    queries = (qkv[:, :half] * QUERY_SCALE).astype(BF16)
    kv = jnp.concatenate(
        [qkv[:, half : 2 * half], 0.5 * qkv[:, 2 * half :] + 0.5 * first_group], axis=1
    ).astype(BF16)

    kv, w_gate, w_up, w_down, w_out, count = lax.optimization_barrier(
        (kv, w_gate, w_up, w_down, w_out, count)
    )
    gathered = {
        "gate": shard_blocks(w_gate),
        "up": shard_blocks(w_up),
        "down": shard_blocks(w_down),
        "outs": [shard_blocks(w_out), shard_blocks(flip(w_out, "tp"))],
    }

    qmark = query_marks.reshape(1, -1)
    far_marks = jnp.concatenate(
        [key_marks, jnp.full((2 * KEY_STEP,), 1 << 30, key_marks.dtype)]
    )
    kmark = lax.dynamic_slice_in_dim(
        far_marks, ctx * group_rows // KEY_STEP * KEY_STEP, 2 * KEY_STEP, 0
    ).reshape(-1, 1)
    forward = {"state": None, "pieces": [(kv, 0, query_marks.reshape(-1, 1))]}

    def advance(last):
        forward["state"] = forward_stage(
            queries, qmark, forward["pieces"], forward["state"], last
        )
        forward["pieces"] = []

    def forward_between(at, arrays):
        advance(False)
        *arrays, out = lax.optimization_barrier((*arrays, forward["state"][2]))
        forward["state"] = (*forward["state"][:2], out)
        if line != 4:
            return arrays
        here = (column == 1) if at == 0 else (level >= at)
        if at == 3:
            forward["pieces"] = [(jnp.concatenate(arrays, axis=0), jnp.where(here, 0, -1), None)]
            return arrays
        forward["pieces"] = [
            (arrays[0], jnp.where(here, 0, -1), None),
            (arrays[1], jnp.where(level > at, 0, -1), None),
        ]
        if at == 0:
            forward["beside"] = arrays[0][:BOUNDARY]
        if at == 1:
            rows = jnp.where(column == 1, arrays[2], forward["beside"])
            forward["pieces"].insert(0, (rows, 0, next_marks.reshape(-1, 1)))
        return arrays

    if line == 4:
        stages, kv_next = spread(kv, 1, slice(0, BOUNDARY), forward_between)
        advance(True)
    else:
        stages, kv_next = spread(kv, 1, slice(0, BOUNDARY), lambda at, arrays: arrays)
        forward["pieces"].append((kv_next, 0, next_marks.reshape(-1, 1)))
        for at, stage in enumerate(stages):
            advance(False)
            forward["pieces"] = [(piece, place, None) for piece, place in stage]
        advance(True)
    attended, lse = forward["state"]

    outs, gate_weight = gathered["outs"], gathered["gate"]
    up_weight, down_weight = gathered["up"], gathered["down"]
    attended, q_own = lax.optimization_barrier((attended, queries))
    q_pair = in_order(column, q_own, flip(q_own, "side"), 0)
    q_all = lax.all_gather(q_pair, "line", axis=0, tiled=True)
    att = [rows_of(attended, tp), flip(rows_of(attended, 1 - tp), "tp")]
    inputs = mine.astype(F32)
    hidden = inputs + times_blocks(att, outs)
    normed_two = rms_norm(hidden, gain_ffn).astype(BF16)
    normed = [normed_two, flip(normed_two, "tp")]
    gate, up, logistic, act = [], [], [], []

    def widen(rows):
        gate.append(times_rows(rows, gate_weight))
        up.append(times_rows(rows, up_weight))
        logistic.append(jax.nn.sigmoid(gate[-1]))
        act.append((gate[-1] * logistic[-1] * up[-1]).astype(BF16))

    widen(normed[0])
    normed[1], act[0] = lax.optimization_barrier((normed[1], act[0]))
    widen(normed[1])
    down_theirs = flip(times_blocks([act[1]], [down_weight]).astype(BF16), "tp")
    down_theirs, q_pair = lax.optimization_barrier((down_theirs, q_pair))
    final = hidden + (times_blocks([act[0]], [down_weight]) + down_theirs.astype(F32))
    difference = final - teacher.reshape(own_rows, width).astype(F32)
    local_error = jnp.sum(jnp.mean(difference * difference, axis=1) * keep)
    token_total = group_rows * sizes[CTX] * sizes["shard"]
    grad_final = token_total / count * keep[:, None] * difference
    grad_round = grad_final.astype(BF16)
    rounds = [grad_round, flip(grad_round, "tp")]
    grad_gate, grad_up = [], []

    def back(at):
        grad_act = times_turned(rounds[at], down_weight)
        part = grad_act * logistic[at]
        grad_gate.append((part * up[at] * (1.0 + gate[at] * (1.0 - logistic[at]))).astype(BF16))
        grad_up.append((part * gate[at]).astype(BF16))

    back(0)
    rounds[1], grad_gate[0], grad_up[0] = lax.optimization_barrier(
        (rounds[1], grad_gate[0], grad_up[0])
    )
    back(1)
    both_weights = [gate_weight, up_weight]
    two_sent = times_rows_turned([grad_gate[1], grad_up[1]], both_weights).astype(BF16)
    two_theirs = flip(two_sent, "tp")
    gate_part = over_rows(normed, grad_gate, True)
    up_part = over_rows(normed, grad_up, True)
    down_part = over_rows(rounds, act, True)
    two_own = times_rows_turned([grad_gate[0], grad_up[0]], both_weights)
    two_theirs, two_own, gate_part, up_part, down_part = lax.optimization_barrier(
        (two_theirs, two_own, gate_part, up_part, down_part)
    )
    ffn_part = jnp.concatenate([gate_part, up_part, down_part], axis=1)
    grad_two = two_own + two_theirs.astype(F32)
    hidden_part, gain_ffn_term = jax.vjp(rms_norm, hidden, gain_ffn)[1](grad_two)
    grad_hidden = grad_final + hidden_part
    hidden_round = grad_hidden.astype(BF16)
    grad_att = [times_turned(hidden_round, w).astype(BF16) for w in outs]
    grad_theirs = flip(grad_att[1], "tp")
    sent, stat = pack_gradient(
        tp.reshape(1).astype(jnp.int32), grad_att[0], grad_theirs, attended, lse
    )

    hidden_two = flip(hidden_round, "tp")

    kv_pieces = [(kv, ctx), (kv_next, jnp.where(ctx + 1 < 2 * line, ctx + 1, -1))]
    kv_pieces += [piece for stage in stages for piece in stage]
    parts = {}

    pairs = half // PAIR
    quarters = max(pairs // 4, 1)

    def query_part(at):
        first = at * quarters
        count = quarters if at < 3 else pairs - first
        return query_gradient(
            queries, sent, parts["stat"], kv_pieces, qmark, kmark, key_marks.shape[0], first, count
        )

    def grad_between(at, arrays):
        if at == 0:
            parts["stat"], parts["q_all"], parts["hidden_two"] = stat, q_all, hidden_two
        if at > 3:
            return arrays
        name = "query" + str(at)
        parts[name] = query_part(at)
        hold = [name, "stat"]
        if at == 0:
            hold += ["q_all", "hidden_two"]
        if at == 3:
            parts["ffn"] = ffn_part
            hold.append("ffn")
        arrays, held = lax.optimization_barrier((arrays, [parts[name] for name in hold]))
        parts.update(zip(hold, held))
        return arrays

    grad_stages, sent_before = spread(
        sent, -1, slice(group_rows - BOUNDARY, None), grad_between
    )
    scattered = lax.psum_scatter(parts["ffn"], CTX, scatter_dimension=0, tiled=True)
    query_grad = jnp.concatenate([parts["query" + str(at)] for at in range(4)], axis=1)
    grad_pieces = [(sent, ctx), (sent_before, ctx - 1)]
    grad_pieces += [piece for stage in grad_stages for piece in stage]
    marks = (key_marks.reshape(1, -1), query_marks.reshape(-1, 1))
    key_grad, value_half = key_gradient(kv, parts["q_all"], grad_pieces, *marks, 0, pairs)
    key_grad, normed_held, parts["hidden_two"] = lax.optimization_barrier(
        (key_grad, normed_one, parts["hidden_two"])
    )
    early_part = jnp.concatenate(
        [
            over_rows([normed_held], [query_grad], True),
            over_rows(
                [hidden_round, parts["hidden_two"]],
                [rows_of(attended, tp), rows_of(attended, 1 - tp)],
                True,
            ),
        ],
        axis=1,
    )
    grads = jnp.concatenate([query_grad, key_grad, value_half], axis=1)
    kv_part = over_rows([normed_one], [grads[:, half:]], True)
    last = {}
    hidden_half = w_gate.shape[1]

    def finish(step, parts):
        if step == 0:
            parts, held, ready = lax.optimization_barrier((parts, grads, scattered))
            last["spread"] = lax.all_gather(ready, CTX, axis=0, tiled=True)
            theirs = times_rows_turned([rows_of(held, 1 - tp)], [weight_qkv]).astype(BF16)
            theirs = flip(theirs, "tp")
            last["own"] = times_rows_turned([rows_of(held, tp)], [weight_qkv])
            last["theirs"] = theirs
            last["value"] = flip(rows_of(held[:, 2 * half :], 1 - tp), "tp")
        if step == 1:
            *parts, last["own"], last["theirs"], last["value"] = lax.optimization_barrier(
                (*parts, last["own"], last["theirs"], last["value"])
            )
        if step == len(bits) + 1:
            parts, spread_out = lax.optimization_barrier((parts, last["spread"]))
            pieces = [
                spread_out[:, at * hidden_half : (at + 1) * hidden_half] for at in range(3)
            ]
            pieces[2] = lax.optimization_barrier(pieces[2].T)
            last["grads"] = [piece.astype(F32) for piece in pieces]
        return parts

    bits = list(ctx_bits())
    early, late = reduce_ctx([early_part, kv_part], [bits, bits[1:] + bits[:1]], finish)
    w_out_grad = lax.optimization_barrier(early[:, half:].T).astype(F32)
    early, late = early.astype(F32), late.astype(F32)
    w_gate_grad, w_up_grad, w_down_grad = last["grads"]
    grad_one = last["own"] + last["theirs"].astype(F32)
    input_part, gain_attn_term = jax.vjp(rms_norm, inputs, gain_attn)[1](grad_one)
    tokens_grad = grad_hidden + input_part
    first_grad = in_order(tp, rows_of(value_half, tp), last["value"], 1).astype(F32)

    small = jnp.concatenate(
        [gain_attn_term, gain_ffn_term, jnp.broadcast_to(local_error, (128,))]
    )
    small = tree_sum(small.reshape(1, -1)).reshape(-1)
    return (
        final.astype(BF16).reshape(1, own_rows, width),
        small[2 * width] / count,
        tokens_grad.reshape(1, own_rows, width),
        first_grad.reshape(1, own_rows, width),
        small[:width],
        small[width : 2 * width],
        early[:, :half],
        late[:, :half],
        late[:, half:],
        w_out_grad,
        w_gate_grad,
        w_up_grad,
        w_down_grad,
    )


def solution(mesh):
    places = dict(mesh.shape)
    devices = mesh.devices.reshape(places["shard"], places["ctx"] // 2, 2, places["tp"])
    rows = P("shard", (*CTX, "tp"), None)
    wide, tall = P("shard", "tp"), P("tp", "shard")
    return jax.shard_map(
        on_device,
        mesh=jax.sharding.Mesh(devices, ("shard", *CTX, "tp")),
        in_specs=(
            rows,
            rows,
            rows,
            P("shard", (*CTX, "tp")),
            P("shard", None),
            P(),
            P(),
            wide,
            wide,
            wide,
            tall,
            wide,
            wide,
            tall,
        ),
        out_specs=(rows, P(), rows, rows, P(), P(), wide, wide, wide, tall, wide, wide, tall),
        check_vma=False,
    )
```
